32 devices in a mesh: dp: 16 (over z, x, core), ctx: 2 (over y).
Axes of the slice: x: 2, y: 2, z: 4, core: 2. Of those that a mesh axis runs over, the one named last changes fastest.
Arguments:
- tokens: bfloat16 [16, 1024, 768], P('dp', 'ctx'), may hold values from -6 to 6
- block_table: int32 [4], replicated, may hold values from 0 to 3, as said below
- ln1_gain: bfloat16 [768], P('dp'), may hold values from 0.099609375 to 1.8984375
- ln1_bias: bfloat16 [768], P('dp'), may hold values from -3 to 3
- w_qkv: bfloat16 [768, 2304], P('dp'), may hold values from -0.21875 to 0.21875
- bias_query: bfloat16 [768], P('dp'), may hold values from -3 to 3
- bias_value: bfloat16 [768], P('dp'), may hold values from -3 to 3
- w_out: bfloat16 [768, 768], P('dp'), may hold values from -6 to 6
- bias_out: bfloat16 [768], P('dp'), may hold values from -3 to 3
- ln2_gain: bfloat16 [768], P('dp'), may hold values from 0.099609375 to 1.8984375
- ln2_bias: bfloat16 [768], P('dp'), may hold values from -3 to 3
- w_up: bfloat16 [768, 3072], P('dp'), may hold values from -0.21875 to 0.21875
- bias_up: bfloat16 [3072], P('dp'), may hold values from -3 to 3
- w_down: bfloat16 [3072, 768], P('dp'), may hold values from -0.109375 to 0.109375
- bias_down: bfloat16 [768], P('dp'), may hold values from -3 to 3
- cotangent: bfloat16 [16, 1024, 768], P('dp', 'ctx'), may hold values from -6 to 6
Outputs:
- output: bfloat16 [16, 1024, 768], P('dp', 'ctx')
- grad_tokens: bfloat16 [16, 1024, 768], P('dp', 'ctx')
- grad_ln1_gain: float32 [768], P('dp')
- grad_ln1_bias: float32 [768], P('dp')
- grad_w_qkv: float32 [768, 2304], P('dp')
- grad_bias_query: float32 [768], P('dp')
- grad_bias_value: float32 [768], P('dp')
- grad_w_out: float32 [768, 768], P('dp')
- grad_bias_out: float32 [768], P('dp')
- grad_ln2_gain: float32 [768], P('dp')
- grad_ln2_bias: float32 [768], P('dp')
- grad_w_up: float32 [768, 3072], P('dp')
- grad_bias_up: float32 [3072], P('dp')
- grad_w_down: float32 [3072, 768], P('dp')
- grad_bias_down: float32 [768], P('dp')
The draws below stay inside these ranges and needn't reach their ends.
Inputs may be any that keep to these rules, and one draw needn't show every extreme that they name: block_table holds every block index of a sequence once; entries 2 i and 2 i + 1 are a mirrored pair b and 3 - b.
All inputs are finite; a program needn't handle non-finite values.
Results may differ from the reference program's by a relative error of at most 0.018.
Values may be sent and summed in bfloat16 or wider, within the bound.
A program may use at most 256 MiB of HBM per device.

```python
import jax
import jax.numpy as jnp
from jax import lax

D = 768
HEADS = 12
HD = 64
FF = 3072
BLK = 256
SEQ = 1024
NBLK = 4
SEQS = 16


def draw_block_table(key, part):
    half_count = NBLK // 2
    pair_order = jax.random.permutation(jax.random.fold_in(key, 11), half_count).astype(jnp.int32)
    flipped = jax.random.randint(jax.random.fold_in(key, 12), (half_count,), 0, 2).astype(jnp.int32)
    first_block = jnp.where(flipped == 1, pair_order, NBLK - 1 - pair_order).astype(jnp.int32)
    second_block = (NBLK - 1 - first_block).astype(jnp.int32)
    return jnp.stack([first_block, second_block], axis=1).reshape(NBLK).astype(jnp.int32)


def steps_of(rng, dims, shards, least, high):
    loudness, own = 1.0, jax.random.fold_in(rng, 6)
    for axis_at, shards_of in shards:
        draws = jnp.exp(jax.random.uniform(jax.random.fold_in(own, axis_at), (shards_of,), jnp.float32, least / len(shards), high / len(shards)))
        loudness = loudness * jnp.repeat(draws, dims[axis_at] // shards_of).reshape([-1 if axis == axis_at else 1 for axis in range(len(dims))])
    return loudness


def gaussian(own_key, dims, deviation, reach, shards=(), dtype=jnp.bfloat16):
    entries = jax.random.normal(own_key, dims, jnp.float32) * deviation
    if len(shards) > 0:
        entries = steps_of(own_key, dims, shards, -0.22, 0.18) * entries
    return jnp.clip(entries, min=-reach, max=reach).astype(dtype)


def setup_inputs(seed: int = 0) -> dict:
    streams_of = jax.random.split(jax.random.key(seed), 17)
    tokens = gaussian(streams_of[0], (SEQS, SEQ, D), 1.0, 6.0, ((0, 16), (1, 2)))
    block_table = draw_block_table(jax.random.fold_in(streams_of[16], 71), 0)
    ln1_gain = jnp.clip(1.0 + 0.18 * jax.random.normal(streams_of[2], (D,), jnp.float32), 0.099609375, 1.8984375).astype(jnp.bfloat16)
    ln1_bias = gaussian(streams_of[3], (D,), 0.5, 3.0, ((0, 16),))
    w_qkv = gaussian(streams_of[4], (D, 3 * D), D ** -0.5, 0.21875, ((0, 16),))
    bias_query = gaussian(streams_of[5], (D,), 0.5, 3.0, ((0, 16),))
    bias_value = gaussian(streams_of[6], (D,), 0.5, 3.0, ((0, 16),))
    w_out = gaussian(streams_of[7], (D, D), (max(1, (2 * D) // SEQ)) ** -0.5, 6.0, ((0, 16),))
    bias_out = gaussian(streams_of[8], (D,), 0.5, 3.0, ((0, 16),))
    ln2_gain = jnp.clip(1.0 + 0.18 * jax.random.normal(streams_of[9], (D,), jnp.float32), 0.099609375, 1.8984375).astype(jnp.bfloat16)
    ln2_bias = gaussian(streams_of[10], (D,), 0.5, 3.0, ((0, 16),))
    w_up = gaussian(streams_of[11], (D, FF), D ** -0.5, 0.21875, ((0, 16),))
    bias_up = gaussian(streams_of[12], (FF,), 0.5, 3.0, ((0, 16),))
    w_down = gaussian(streams_of[13], (FF, D), FF ** -0.5, 0.109375, ((0, 16),))
    bias_down = gaussian(streams_of[14], (D,), 0.5, 3.0, ((0, 16),))
    cotangent = gaussian(streams_of[15], (SEQS, SEQ, D), 1.0, 6.0, ((0, 16), (1, 2)))
    return {"tokens": tokens, "block_table": block_table, "ln1_gain": ln1_gain, "ln1_bias": ln1_bias, "w_qkv": w_qkv, "bias_query": bias_query, "bias_value": bias_value, "w_out": w_out, "bias_out": bias_out, "ln2_gain": ln2_gain, "ln2_bias": ln2_bias, "w_up": w_up, "bias_up": bias_up, "w_down": w_down, "bias_down": bias_down, "cotangent": cotangent}


@jax.custom_vjp
def low(v):
    return lax.optimization_barrier(v.astype(jnp.bfloat16)).astype(jnp.float32)

@jax.custom_vjp
def low_back(v):
    return v

def low_keep(v):
    return (low(v), None)

def low_pass(kept, grad):
    return (grad,)

def back_keep(v):
    return (v, None)

def back_low(kept, grad):
    return (low(grad),)
low.defvjp(low_keep, low_pass)
low_back.defvjp(back_keep, back_low)

def layer_norm(values, gain, shift):
    centred = values - lax.optimization_barrier(jnp.mean(values, axis=-1, keepdims=True))
    spread_sq = lax.optimization_barrier(jnp.mean(centred * centred, axis=-1, keepdims=True))
    return centred * lax.rsqrt(spread_sq + 1e-05) * gain + shift

def reference(tokens, block_table, ln1_gain, ln1_bias, w_qkv, bias_query, bias_value, w_out, bias_out, ln2_gain, ln2_bias, w_up, bias_up, w_down, bias_down, cotangent):
    params = tuple((argument.astype(jnp.float32) for argument in (ln1_gain, ln1_bias, w_qkv, bias_query, bias_value, w_out, bias_out, ln2_gain, ln2_bias, w_up, bias_up, w_down, bias_down)))
    row_blocks = jnp.repeat(block_table, BLK, total_repeat_length=SEQ)
    allowed = row_blocks[None, :] <= row_blocks[:, None]
    scale = HD ** (-0.5)
    highest = lax.Precision.HIGHEST

    def forward_sequence(weights, inputs):
        gain_one, shift_one, qkv_w, query_b, value_b, out_w, out_b, gain_two, shift_two, up_w, up_b, down_w, down_b = weights
        model_width = inputs.shape[1]
        normed_one = low(layer_norm(inputs, gain_one, shift_one))
        bias_cat = jnp.concatenate([query_b, jnp.zeros((model_width,), jnp.float32), value_b])
        projected = low(low_back(jnp.dot(normed_one, qkv_w, precision=highest) + bias_cat))

        def one_head(head_index):
            query_part = lax.dynamic_slice_in_dim(projected, head_index * HD, HD, 1)
            key_part = lax.dynamic_slice_in_dim(projected, model_width + head_index * HD, HD, 1)
            value_part = lax.dynamic_slice_in_dim(projected, 2 * model_width + head_index * HD, HD, 1)
            scores = low_back(jnp.dot(query_part, key_part.T, precision=highest)) * scale
            scores = jnp.where(allowed, scores, -1e+30)
            probs = low(jax.nn.softmax(scores, axis=-1))
            return jnp.dot(probs, value_part, precision=highest)
        heads_out = lax.map(jax.checkpoint(one_head), jnp.arange(HEADS))
        attended = low(low_back(jnp.transpose(heads_out, (1, 0, 2)).reshape(-1, model_width)))
        branch = low_back(jnp.dot(attended, out_w, precision=highest) + out_b)
        middle = inputs + branch
        normed_two = low(layer_norm(middle, gain_two, shift_two))
        hidden_pre = low_back(jnp.dot(normed_two, up_w, precision=highest) + up_b)
        active = low(jax.nn.gelu(hidden_pre, approximate=True))
        return middle + (jnp.dot(active, down_w, precision=highest) + down_b)

    def one_sequence(totals, pair_in):
        seq_in, seq_cot = pair_in
        result, pullback = jax.vjp(forward_sequence, params, seq_in)
        grad_params, grad_in = pullback(seq_cot)
        totals = jax.tree.map(jnp.add, totals, grad_params)
        return (totals, (result.astype(jnp.bfloat16), grad_in.astype(jnp.bfloat16)))
    zeros_start = tuple((jnp.zeros_like(argument) for argument in params))
    grads, (outputs, grad_inputs) = lax.scan(one_sequence, zeros_start, (tokens.astype(jnp.float32), cotangent.astype(jnp.float32)))
    return (outputs, grad_inputs, grads[0], grads[1], grads[2], grads[3], grads[4], grads[5], grads[6], grads[7], grads[8], grads[9], grads[10], grads[11], grads[12])
```

```python
import functools
import jax
import jax.numpy as jnp
from jax import lax
from jax.experimental import pallas as pl
from jax.experimental.pallas import tpu as pltpu
from jax.sharding import PartitionSpec as P

ANY = pl.BlockSpec(memory_space=pl.ANY)
VM = pl.BlockSpec(memory_space=pltpu.VMEM)
DMA = pltpu.SemaphoreType.DMA


def near_first(count):
    order = []
    for step in range(1, count):
        order.append((step + 1) // 2 if step % 2 else count - step // 2)
    return order


class Spot:
    def __init__(self, dp, ctx):
        self.dp, self.ctx = dp, ctx
        self.lines = dp // 4
        me = lax.axis_index("dp")
        self.y = lax.axis_index("ctx")
        self.z = me // 4
        self.x = (me // 2) % 2
        self.c = me % 2
        self.me = me

    def dp_at(self, z, x, c):
        return (z * 2 + x) * 2 + c

    def z_at(self, k):
        return lax.rem(self.z + k, self.lines)

    def y_at(self, k):
        return lax.rem(self.y + k, self.ctx)

    def barrier(self):
        sem = pltpu.get_barrier_semaphore()
        peers = [{"dp": self.dp_at(self.z_at(k), self.x, self.c)} for k in range(1, self.lines)]
        peers.append({"dp": self.dp_at(self.z, 1 - self.x, self.c)})
        peers.append({"dp": self.dp_at(self.z, self.x, 1 - self.c)})
        peers += [{"ctx": self.y_at(k)} for k in range(1, self.ctx)]
        for peer in peers:
            pl.semaphore_signal(sem, inc=1, device_id=peer, device_id_type=pl.DeviceIdType.MESH)
        pl.semaphore_wait(sem, len(peers))


def remote(src, dst, ssem, rsem, device):
    return pltpu.make_async_remote_copy(
        src_ref=src, dst_ref=dst, send_sem=ssem, recv_sem=rsem,
        device_id=device, device_id_type=pl.DeviceIdType.MESH,
    )


def gather_kernel(dp, ctx, head, third, tok_ref, cat_ref, tok_all, wall,
                  loc, st, rt, sz, rz, sx, rx, sy, ry, sc, rc):
    at = Spot(dp, ctx)
    lines = at.lines
    ky = at.y % 2
    mine = pl.multiple_of(head + third + ky * third, 128)
    other = pl.multiple_of(head + third + (1 - ky) * third, 128)
    cols = {"q": pl.ds(0, head), "m": pl.ds(mine, third), "t": pl.ds(head, third), "o": pl.ds(other, third)}
    num = {"q": 0, "m": 1, "t": 2, "o": 3}
    own = at.me
    mate = {"dp": at.dp_at(at.z, at.x, 1 - at.c)}
    across = {"dp": at.dp_at(at.z, 1 - at.x, at.c)}
    pair = {"ctx": at.y + 1 - 2 * ky}
    at.barrier()
    copies = []

    def go(copy):
        copy.start()
        copies.append(copy)

    local = [pltpu.make_async_copy(cat_ref, wall.at[own], loc.at[0]),
             pltpu.make_async_copy(tok_ref, tok_all.at[at.y], loc.at[1])]
    for copy in local:
        copy.start()

    def block(b, z, x, c):
        return wall.at[at.dp_at(z, x, c), :, cols[b]]

    def own_block(b):
        return cat_ref.at[:, cols[b]]

    def send_z(b):
        for k in near_first(lines):
            go(remote(own_block(b), block(b, at.z, at.x, at.c), sz.at[num[b], k], rz.at[num[b], at.z],
                      {"dp": at.dp_at(at.z_at(k), at.x, at.c)}))

    def send_x(b, z, k, src):
        go(remote(src, block(b, z, at.x, at.c), sx.at[num[b], k], rx.at[num[b], z], across))

    def send_c(b, z, x, k, kx, src):
        go(remote(src, block(b, z, x, at.c), sc.at[num[b], k, kx], rc.at[num[b], z, x], mate))

    def send_y(z, x, k, kx, src):
        go(remote(src, block("m", z, x, at.c), sy.at[k, kx], ry.at[z, x], pair))

    def got_z(b, k):
        z = at.z_at(k)
        remote(own_block(b), block(b, z, at.x, at.c), sz.at[num[b], 0], rz.at[num[b], z], across).wait_recv()

    def got_x(b, k):
        z = at.z_at(k)
        remote(own_block(b), block(b, z, 1 - at.x, at.c), sz.at[num[b], 0], rx.at[num[b], z], across).wait_recv()

    def got_y(k, kx):
        z, x = at.z_at(k), (at.x + kx) % 2
        remote(own_block("o"), block("o", z, x, at.c), sz.at[0, 0], ry.at[z, x], across).wait_recv()

    def got_c(b, k, kx):
        z, x = at.z_at(k), (at.x + kx) % 2
        remote(own_block(b), block(b, z, x, 1 - at.c), sz.at[0, 0], rc.at[num[b], z, x], across).wait_recv()

    order = [0] + near_first(lines)
    for k in range(1, ctx):
        go(remote(tok_ref, tok_all.at[at.y], st.at[k], rt.at[at.y], {"ctx": at.y_at(k)}))
    for b in ("q", "m", "t"):
        send_z(b)
    for b in ("q", "m", "t"):
        send_x(b, at.z, 0, own_block(b))
        send_c(b, at.z, at.x, 0, 0, own_block(b))
        for k in order[1:]:
            got_z(b, k)
            z = at.z_at(k)
            src = block(b, z, at.x, at.c)
            send_x(b, z, k, src)
            if b == "m":
                send_y(z, at.x, k, 0, src)
            send_c(b, z, at.x, k, 0, src)
        for k in order:
            got_x(b, k)
            z = at.z_at(k)
            src = block(b, z, 1 - at.x, at.c)
            if b == "m":
                send_y(z, 1 - at.x, k, 1, src)
            send_c(b, z, 1 - at.x, k, 1, src)
    send_c("o", at.z, at.x, 0, 0, own_block("o"))
    for kx in range(2):
        for k in order:
            if k == 0 and kx == 0:
                continue
            got_y(k, kx)
            z, x = at.z_at(k), (at.x + kx) % 2
            send_c("o", z, x, k, kx, block("o", z, x, at.c))
    for b in ("q", "m", "t", "o"):
        for kx in range(2):
            for k in order:
                got_c(b, k, kx)
    for k in range(1, ctx):
        y = at.y_at(k)
        remote(tok_ref, tok_all.at[y], st.at[0], rt.at[y], across).wait_recv()
    for copy in copies:
        copy.wait_send()
    for copy in local:
        copy.wait()


def gather(tok, cat, dp, ctx, head, third):
    lines = dp // 4
    rows, width = cat.shape
    return pl.pallas_call(
        functools.partial(gather_kernel, dp, ctx, head, third),
        out_shape=(jax.ShapeDtypeStruct((ctx, *tok.shape), tok.dtype),
                   jax.ShapeDtypeStruct((dp, rows, width), cat.dtype)),
        in_specs=[VM, VM], out_specs=(ANY, ANY),
        scratch_shapes=[DMA((2,)), DMA((ctx,)), DMA((ctx,)),
                        DMA((3, lines)), DMA((3, lines)), DMA((3, lines)), DMA((3, lines)),
                        DMA((lines, 2)), DMA((lines, 2)), DMA((4, lines, 2)), DMA((4, lines, 2))],
        compiler_params=pltpu.CompilerParams(collective_id=0, has_side_effects=True, vmem_limit_bytes=32 * 2**20),
    )(tok, cat)


def scatter_kernel(dp, ctx, head, third, gq, gt, out, a_core, a_pair, a_x, a_z, a_y, stage, total,
                   loc, s1, r1, s2, r2, s3, r3, s4, r4, s5, r5):
    at = Spot(dp, ctx)
    lines = at.lines
    rows = gq.shape[1]
    ky = at.y % 2
    mine = pl.multiple_of(head + third + ky * third, 128)
    other = pl.multiple_of(head + third + (1 - ky) * third, 128)
    cols = {"q": pl.ds(0, head), "m": pl.ds(mine, third), "t": pl.ds(head, third), "o": pl.ds(other, third)}
    size = {"q": head, "m": third, "t": third, "o": third}
    num = {"q": 0, "m": 1, "t": 2, "o": 3}
    mate = {"dp": at.dp_at(at.z, at.x, 1 - at.c)}
    across = {"dp": at.dp_at(at.z, 1 - at.x, at.c)}
    pair = {"ctx": at.y + 1 - 2 * ky}
    at.barrier()
    copies = []

    def go(copy):
        copy.start()
        copies.append(copy)

    first = {"m": pl.multiple_of(third + ky * third, 128), "o": pl.multiple_of(third + (1 - ky) * third, 128), "t": 0}

    def full(b, at_dp):
        if b == "q":
            return gq.at[at_dp]
        return gt.at[at_dp, :, pl.ds(first[b], third)]

    order = [0] + near_first(lines)
    order = order[::-1]
    spots = [(k, kx) for kx in (1, 0) for k in order]

    def where(k, kx):
        return at.z_at(k), (at.x + kx) % 2

    def land(ref, b, *idx):
        return ref.at[(num[b], *idx, slice(None), pl.ds(0, size[b]))]

    blocks = ("o", "m", "t", "q")
    for b in blocks:
        for k, kx in spots:
            z, x = where(k, kx)
            go(remote(full(b, at.dp_at(z, x, 1 - at.c)), land(a_core, b, z, x),
                      s1.at[num[b], k, kx], r1.at[num[b], z, x], mate))
    def fetch(b, k, kx):
        z, x = where(k, kx)
        return pltpu.make_async_copy(full(b, at.dp_at(z, x, at.c)), land(stage, b, z, x),
                                     loc.at[num[b], k, kx])
    for b in blocks:
        for k, kx in spots:
            fetch(b, k, kx).start()

    def take(sem, dst):
        remote(dst, dst, s1.at[0, 0, 0], sem, across).wait_recv()

    def added(b, k, kx):
        z, x = where(k, kx)
        fetch(b, k, kx).wait()
        here = land(a_core, b, z, x)
        take(r1.at[num[b], z, x], here)
        here[...] = here[...] + land(stage, b, z, x)[...]
        return here

    for b in blocks:
        if b == "o":
            for k, kx in spots:
                z, x = where(k, kx)
                go(remote(added(b, k, kx), a_pair.at[z, x], s2.at[k, kx], r2.at[z, x], pair))
            continue
        for k, kx in spots:
            z, x = where(k, kx)
            here = added(b, k, kx)
            if b == "m":
                take(r2.at[z, x], a_pair.at[z, x])
                here[...] = here[...] + a_pair[z, x]
            if kx == 1:
                go(remote(here, land(a_x, b, z), s3.at[num[b], k], r3.at[num[b], z], across))
        for k in order:
            z = at.z_at(k)
            here = land(a_core, b, z, at.x)
            take(r3.at[num[b], z], land(a_x, b, z))
            here[...] = here[...] + land(a_x, b, z)[...]
            if k:
                go(remote(here, land(a_z, b, at.z), s4.at[num[b], k], r4.at[num[b], at.z],
                          {"dp": at.dp_at(z, at.x, at.c)}))
    for b in ("m", "t", "q"):
        acc = land(a_core, b, at.z, at.x)[...].astype(jnp.float32)
        for k in near_first(lines):
            z = at.z_at(k)
            take(r4.at[num[b], z], land(a_z, b, z))
            acc = acc + land(a_z, b, z)[...].astype(jnp.float32)
        land(total, b)[...] = acc
        land(a_core, b, at.z, at.x)[...] = acc.astype(jnp.bfloat16)
        for k in range(1, ctx):
            go(remote(land(a_core, b, at.z, at.x), land(a_y, b, at.y), s5.at[num[b], k], r5.at[num[b], at.y],
                      {"ctx": at.y_at(k)}))
    outs = []
    for b in ("t", "q", "m", "o"):
        if b == "m":
            acc = land(total, b)[...]
        elif b == "o":
            acc = jnp.zeros((rows, third), jnp.float32)
        else:
            acc = land(total, b)[...]
        for k in range(1, ctx):
            y = at.y_at(k)
            if b in ("t", "q") or (b == "m" and k % 2 == 0):
                take(r5.at[num[b], y], land(a_y, b, y))
                acc = acc + land(a_y, b, y)[...].astype(jnp.float32)
            elif b == "o" and k % 2 == 1:
                here = a_y.at[1, y, :, pl.ds(0, third)]
                take(r5.at[1, y], here)
                acc = acc + here[...].astype(jnp.float32)
        land(total, b)[...] = acc
        copy = pltpu.make_async_copy(land(total, b), out.at[:, cols[b]], loc.at[num[b], 0, 0])
        copy.start()
        outs.append(copy)
    for copy in copies:
        copy.wait_send()
    for copy in outs:
        copy.wait()


def scatter(gq, gt, dp, ctx, head, third):
    lines = dp // 4
    _, rows, width = gq.shape[0], gq.shape[1], gq.shape[2] + gt.shape[2]
    bf, f32 = jnp.bfloat16, jnp.float32
    return pl.pallas_call(
        functools.partial(scatter_kernel, dp, ctx, head, third),
        out_shape=jax.ShapeDtypeStruct((rows, width), f32),
        in_specs=[ANY, ANY], out_specs=ANY,
        scratch_shapes=[pltpu.VMEM((4, lines, 2, rows, head), bf), pltpu.VMEM((lines, 2, rows, third), bf),
                        pltpu.VMEM((3, lines, rows, head), bf), pltpu.VMEM((3, lines, rows, head), bf),
                        pltpu.VMEM((3, ctx, rows, head), bf), pltpu.VMEM((4, lines, 2, rows, head), bf),
                        pltpu.VMEM((4, rows, head), f32),
                        DMA((4, lines, 2)), DMA((4, lines, 2)), DMA((4, lines, 2)),
                        DMA((lines, 2)), DMA((lines, 2)),
                        DMA((3, lines)), DMA((3, lines)), DMA((3, lines)), DMA((3, lines)),
                        DMA((3, ctx)), DMA((3, ctx))],
        compiler_params=pltpu.CompilerParams(collective_id=1, has_side_effects=True, vmem_limit_bytes=60 * 2**20),
    )(gq, gt)


F32, BF = jnp.float32, jnp.bfloat16
HEADS, HD, BLK = 12, 64, 256
PAIRS, LANES = HEADS // 2, 2 * HD


def dot(a, b):
    return jnp.dot(a, b, preferred_element_type=F32)


def dot_t(a, b):
    return lax.dot_general(a, b, (((1,), (1,)), ((), ())), preferred_element_type=F32)


def dot_l(a, b):
    return lax.dot_general(a, b, (((0,), (0,)), ((), ())), preferred_element_type=F32)


def normed(x):
    centred = x - jnp.mean(x, axis=-1, keepdims=True)
    inv = lax.rsqrt(jnp.mean(centred * centred, axis=-1, keepdims=True) + 1e-05)
    return centred * inv, inv


def norm_back(dy, unit, inv, gain):
    dn = dy * gain
    return inv * (dn - jnp.mean(dn, axis=-1, keepdims=True) - unit * jnp.mean(dn * unit, axis=-1, keepdims=True))


class Table:
    def __init__(self, tbl, nb, y):
        self.nb, self.half = nb, nb // 2
        self.own = [tbl[2 * y], tbl[2 * y + 1]]
        first_high = (self.own[0] >= self.half).astype(jnp.int32)
        self.row_of = [first_high, 1 - first_high]
        self.slot_of = [first_high, 1 - first_high]
        self.block = [jnp.minimum(self.own[0], self.own[1]), jnp.maximum(self.own[0], self.own[1])]
        self.pos = []
        for j in range(nb):
            at = jnp.int32(0)
            for p in range(nb):
                at = at + jnp.where(tbl[p] == j, p, 0)
            self.pos.append(at)
        self.tbl = tbl

    def keys(self, slot):
        return self.half if slot == 0 else self.nb

    def masked(self, slot, j):
        return j >= 1 if slot == 0 else j > self.half


def rows_of(ref, *idx):
    value = ref[idx]
    return value.reshape(value.shape[0] * value.shape[1], value.shape[2])


def lane_masks(rows):
    lane = lax.broadcasted_iota(jnp.int32, (rows, LANES), 1)
    return [lane < HD, lane >= HD]


def project(ctx, tok, wall, h1, q, kv, vec, y):
    gain, shift = vec[0:1], vec[1:2]
    width = tok.shape[2]
    zero = jnp.zeros((1, width), F32)
    kv_bias = jnp.concatenate([zero, vec[3:4]], axis=1)
    w_kv = rows_of(wall, slice(None), slice(None), slice(128 + width, 128 + 3 * width))

    def rows(r, carry):
        x = tok[r // 2, pl.ds(pl.multiple_of((r % 2) * BLK, BLK), BLK)].astype(F32)
        low = (normed(x)[0] * gain + shift).astype(BF)
        kv[pl.ds(pl.multiple_of(r * BLK, BLK), BLK)] = (dot(low, w_kv) + kv_bias).astype(BF)
        return carry

    lax.fori_loop(0, 2 * ctx, rows, 0)
    w_q = rows_of(wall, slice(None), slice(None), slice(128, 128 + width))

    def own(i, carry):
        at = pl.ds(pl.multiple_of(i * BLK, BLK), BLK)
        low = (normed(tok[y, at].astype(F32))[0] * gain + shift).astype(BF)
        h1[at] = low
        q[at] = ((dot(low, w_q) + vec[2:3]).astype(BF).astype(F32) * HD ** (-0.5)).astype(BF)
        return carry

    lax.fori_loop(0, 2, own, 0)


def attend_pair(hp, table, q, kv, att, lse_acc, width):
    lanes = pl.ds(pl.multiple_of(hp * LANES, LANES), LANES)
    v_lanes = pl.ds(pl.multiple_of(width + hp * LANES, LANES), LANES)
    masks = lane_masks(BLK)
    lane = lax.broadcasted_iota(jnp.int32, (BLK, LANES), 1)
    for slot in range(2):
        q2 = q[pl.ds(pl.multiple_of(table.row_of[slot] * BLK, BLK), BLK), lanes]
        spots = [pl.ds(pl.multiple_of(table.pos[j] * BLK, BLK), BLK) for j in range(table.keys(slot))]
        mixed = []
        for h in range(2):
            qm = jnp.where(masks[h], q2, jnp.zeros_like(q2))
            scores = []
            for j, at in enumerate(spots):
                s = dot_t(qm, kv[at, lanes])
                if table.masked(slot, j):
                    s = jnp.where(j <= table.block[slot], s, -1e30)
                scores.append(s)
            largest = functools.reduce(jnp.maximum, scores)
            largest = jnp.max(largest, axis=-1, keepdims=True)
            exps = [jnp.exp(s - largest) for s in scores]
            total = jnp.sum(functools.reduce(jnp.add, exps), axis=-1, keepdims=True)
            out = functools.reduce(jnp.add, [dot(e.astype(BF), kv[at, v_lanes]) for e, at in zip(exps, spots)])
            mixed.append(out / total)
            lse_acc[slot] = jnp.where(lane == 2 * hp + h, largest + jnp.log(total), lse_acc[slot])
        att[slot, :, lanes] = jnp.where(masks[0], mixed[0], mixed[1]).astype(BF)


def attend_back_pair(hp, table, q, kv, da, lse, delta, dq, dk_acc, dv_acc, width):
    lanes = pl.ds(pl.multiple_of(hp * LANES, LANES), LANES)
    v_lanes = pl.ds(pl.multiple_of(width + hp * LANES, LANES), LANES)
    masks = lane_masks(BLK)
    for slot in (1, 0):
        row = pl.ds(pl.multiple_of(table.row_of[slot] * BLK, BLK), BLK)
        q2, da2 = q[row, lanes], da[row, lanes]
        dq_acc = None
        for h in range(2):
            qm = jnp.where(masks[h], q2, jnp.zeros_like(q2))
            dam = jnp.where(masks[h], da2, jnp.zeros_like(da2))
            lse_row = lse[slot, pl.ds(2 * hp + h, 1), :]
            delta_row = delta[table.row_of[slot], pl.ds(2 * hp + h, 1), :]
            for j in range(table.keys(slot)):
                at = pl.ds(pl.multiple_of(table.pos[j] * BLK, BLK), BLK)
                k2, v2 = kv[at, lanes], kv[at, v_lanes]
                st = dot_t(k2, qm)
                if table.masked(slot, j):
                    st = jnp.where(j <= table.block[slot], st, -1e30)
                pt = jnp.exp(st - lse_row)
                dst = (pt * (dot_t(v2, dam) - delta_row)).astype(BF)
                dv, dk = dot(pt.astype(BF), dam), dot(dst, qm)
                if slot == 1 and h == 0:
                    dv_acc[j], dk_acc[j] = dv, dk
                else:
                    dv_acc[j] += dv
                    dk_acc[j] += dk
                part = dot_l(dst, jnp.where(masks[h], k2, jnp.zeros_like(k2)))
                dq_acc = part if dq_acc is None else dq_acc + part
        dq[slot, :, lanes] = (dq_acc * HD ** (-0.5)).astype(BF)


def feed(nd, off_up, off_down, table, tok, att, wall, cot, vec, bup, out, gt, da, dx1, delta, gvec, gup,
         x1, h2, acc, dh2):
    rows, width = cot.shape
    dp, r = wall.shape[0], wall.shape[1]
    chunk = 4 * nd * r
    w_out = rows_of(wall, slice(None), slice(None), slice(off_up - width, off_up))
    for i in range(2):
        at = pl.ds(i * BLK, BLK)
        mid = tok[at].astype(F32) + (dot(att[table.slot_of[i]], w_out) + vec[4:5])
        x1[at] = mid
        h2[at] = (normed(mid)[0] * vec[5:6] + vec[6:7]).astype(BF)
        acc[at] = mid + vec[7:8]
    dh2[...] = jnp.zeros_like(dh2)
    g = cot[...]

    def part(f, carry):
        cols = pl.ds(pl.multiple_of(off_up + f * chunk, 128), chunk)
        w_up = rows_of(wall, slice(None), slice(None), cols)
        w_down = jnp.concatenate(
            [wall[f * nd + d, :, pl.ds(off_down + j * width, width)] for d in range(nd) for j in range(4)], axis=0)
        low = h2[...]
        u = dot(low, w_up) + bup[:, pl.ds(pl.multiple_of(f * chunk, 128), chunk)]
        sq = u * u
        t = jnp.tanh(u * (0.7978845608028654 + 0.03567740813636141 * sq))
        act = (0.5 * u * (1.0 + t)).astype(BF)
        slope = 0.5 * (1.0 + t) + 0.5 * u * (1.0 - t * t) * (0.7978845608028654 + 0.10703222440908423 * sq)
        acc[...] += dot(act, w_down)
        du = slope * dot_t(g, w_down)
        dul = du.astype(BF)
        gup[:, pl.ds(pl.multiple_of(f * chunk, 128), chunk)] = jnp.sum(dul.astype(F32), axis=0, keepdims=True)
        dh2[...] += dot_t(dul, w_up)
        g_up = dot_l(low, dul).astype(BF)
        gt[:, :, pl.ds(pl.multiple_of(width + f * chunk, 128), chunk)] = g_up.reshape(dp, r, chunk)
        g_down = dot_l(act, g).astype(BF)
        for d in range(nd):
            for j in range(4):
                piece = g_down[(4 * d + j) * r:(4 * d + j + 1) * r]
                gt[f * nd + d, :, pl.ds(width + off_down - off_up + j * width, width)] = piece
        return carry

    lax.fori_loop(0, dp // nd, part, 0)
    out[...] = acc[...].astype(BF)
    gf = g.astype(F32)
    unit, inv = normed(x1[...])
    dy = dh2[...]
    mid_grad = gf + norm_back(dy, unit, inv, vec[5:6])
    dx1[...] = mid_grad
    branch = mid_grad.astype(BF)
    gvec[...] = jnp.zeros_like(gvec)
    gvec[4:5] = jnp.sum(branch.astype(F32), axis=0, keepdims=True)
    gvec[5:6] = jnp.sum(dy * unit, axis=0, keepdims=True)
    gvec[6:7] = jnp.sum(dy, axis=0, keepdims=True)
    gvec[7:8] = jnp.sum(gf, axis=0, keepdims=True)
    head = lax.broadcasted_iota(jnp.int32, (16, width), 0)
    pick = (lax.broadcasted_iota(jnp.int32, (16, width), 1) // HD == head).astype(F32)
    grad = None
    for i in range(2):
        own = att[table.slot_of[i]]
        low = branch[i * BLK:(i + 1) * BLK]
        piece = dot_l(own, low)
        grad = piece if grad is None else grad + piece
        back = dot_t(low, w_out).astype(BF)
        da[pl.ds(i * BLK, BLK)] = back
        prod = back.astype(F32) * own.astype(F32)
        delta[i] = lax.dot_general(pick, prod, (((1,), (1,)), ((), ())), precision=lax.Precision.HIGHEST,
                                   preferred_element_type=F32)
    gt[:, :, 0:width] = grad.astype(BF).reshape(dp, r, width)


def last(ctx, table, y, dq, own_kv, h1, tok, wall, dx1, vec, gvec, gq, gtok):
    width = h1.shape[1]
    dp, r = wall.shape[0], wall.shape[1]
    w_q = rows_of(wall, slice(None), slice(None), slice(128, 128 + width))
    low = h1[...]
    dq_all = jnp.concatenate([dq[table.slot_of[0]], dq[table.slot_of[1]]], axis=0)
    gq[:, :, 128:128 + width] = dot_l(low, dq_all).astype(BF).reshape(dp, r, width)
    dh1 = dot_t(dq_all, w_q)
    dkv = own_kv()
    w_kv = rows_of(wall, slice(None), slice(None), slice(128 + width, 128 + 3 * width))
    gq[:, :, 128 + width:128 + 3 * width] = dot_l(low, dkv).astype(BF).reshape(dp, r, 2 * width)
    dh1 = dh1 + dot_t(dkv, w_kv)
    unit, inv = normed(tok[...].astype(F32))
    gtok[...] = (dx1[...] + norm_back(dh1, unit, inv, vec[0:1])).astype(BF)
    sums = [jnp.sum(dh1 * unit, axis=0, keepdims=True), jnp.sum(dh1, axis=0, keepdims=True),
            jnp.sum(dq_all.astype(F32), axis=0, keepdims=True),
            jnp.sum(dkv[:, width:].astype(F32), axis=0, keepdims=True)]
    table_rows = jnp.concatenate(sums + [gvec[4:16], jnp.zeros((112, width), F32)], axis=0)
    gq[:, :, 0:128] = jnp.transpose(table_rows).astype(BF).reshape(dp, r, 128)


SM = pl.BlockSpec(memory_space=pltpu.SMEM)


def params(limit, **more):
    return pltpu.CompilerParams(vmem_limit_bytes=limit * 2**20, **more)


def shape(*dims, dtype=BF):
    return jax.ShapeDtypeStruct(dims, dtype)


def attend_kernel(ctx, tbl, tok, wall, h1, q, kv, att, lse, vec, lse_acc):
    width = tok.shape[2]
    y = lax.axis_index("ctx")
    table = Table(tbl, 2 * ctx, y)
    small = rows_of(wall, slice(None), slice(None), slice(0, 128)).astype(F32)
    vec[...] = jnp.transpose(small)[0:16]
    project(ctx, tok, wall, h1, q, kv, vec, y)
    lse_acc[...] = jnp.zeros_like(lse_acc)

    def pair(hp, carry):
        attend_pair(hp, table, q, kv, att, lse_acc, width)
        return carry

    lax.fori_loop(0, PAIRS, pair, 0)
    for slot in range(2):
        lse[slot] = jnp.transpose(lse_acc[slot])[0:16]


def attend(tbl, tok_all, wall, ctx):
    rows, width = tok_all.shape[1:]
    return pl.pallas_call(
        functools.partial(attend_kernel, ctx),
        out_shape=(shape(rows, width), shape(rows, width), shape(ctx * rows, 2 * width), shape(2, BLK, width),
                   shape(2, 16, BLK, dtype=F32), shape(16, width, dtype=F32)),
        in_specs=[SM, VM, VM], out_specs=(VM,) * 6,
        scratch_shapes=[pltpu.VMEM((2, BLK, LANES), F32)],
        compiler_params=params(62), name="attend",
    )(tbl, tok_all, wall)


def feed_kernel(ctx, nd, off_up, off_down, tbl, tok, att, wall, cot, vec, bup, *rest):
    table = Table(tbl, 2 * ctx, lax.axis_index("ctx"))
    feed(nd, off_up, off_down, table, tok, att, wall, cot, vec, bup, *rest)


def feed_call(tbl, tok, att, wall, cot, vec, bup, ctx, off_up, off_down, gt_cols):
    rows, width = cot.shape
    dp, r = wall.shape[:2]
    return pl.pallas_call(
        functools.partial(feed_kernel, ctx, dp // 4, off_up, off_down),
        out_shape=(shape(rows, width), shape(dp, r, gt_cols), shape(rows, width), shape(rows, width, dtype=F32),
                   shape(2, 16, BLK, dtype=F32), shape(16, width, dtype=F32), shape(1, bup.shape[1], dtype=F32)),
        in_specs=[SM] + [VM] * 6, out_specs=(VM,) * 7,
        scratch_shapes=[pltpu.VMEM((rows, width), F32), pltpu.VMEM((rows, width), BF),
                        pltpu.VMEM((rows, width), F32), pltpu.VMEM((rows, width), F32)],
        compiler_params=params(62), name="feed",
    )(tbl, tok, att, wall, cot, vec, bup)


def attend_back_kernel(ctx, tbl, q, kv, da, lse, delta, dq, dkv, dk_acc, dv_acc):
    width = q.shape[1]
    table = Table(tbl, 2 * ctx, lax.axis_index("ctx"))

    def pair(hp, carry):
        attend_back_pair(hp, table, q, kv, da, lse, delta, dq, dk_acc, dv_acc, width)
        for j in range(2 * ctx):
            at = pl.ds(pl.multiple_of(table.pos[j] * BLK, BLK), BLK)
            dkv[at, pl.ds(pl.multiple_of(hp * LANES, LANES), LANES)] = dk_acc[j].astype(BF)
            dkv[at, pl.ds(pl.multiple_of(width + hp * LANES, LANES), LANES)] = dv_acc[j].astype(BF)
        return carry

    lax.fori_loop(0, PAIRS, pair, 0)


def attend_back(tbl, q, kv, da, lse, delta, ctx):
    rows, width = q.shape
    return pl.pallas_call(
        functools.partial(attend_back_kernel, ctx),
        out_shape=(shape(2, BLK, width), shape(*kv.shape)),
        in_specs=[SM] + [VM] * 5, out_specs=(VM,) * 2,
        scratch_shapes=[pltpu.VMEM((2 * ctx, BLK, LANES), F32), pltpu.VMEM((2 * ctx, BLK, LANES), F32)],
        compiler_params=params(62), name="attend_back",
    )(tbl, q, kv, da, lse, delta)


def last_kernel(ctx, tbl, dq, dkv, h1, tok, wall, dx1, vec, gvec, gq, gtok, land, ssem, rsem):
    rows = h1.shape[0]
    y = lax.axis_index("ctx")
    table = Table(tbl, 2 * ctx, y)
    sem = pltpu.get_barrier_semaphore()
    peers = [lax.rem(y + k, ctx) for k in range(1, ctx)]
    for peer in peers:
        pl.semaphore_signal(sem, inc=1, device_id={"ctx": peer}, device_id_type=pl.DeviceIdType.MESH)
    pl.semaphore_wait(sem, ctx - 1)
    copies = []
    for k, peer in enumerate(peers):
        copy = remote(dkv.at[pl.ds(pl.multiple_of(peer * rows, BLK), rows)], land.at[y], ssem.at[k], rsem.at[y], {"ctx": peer})
        copy.start()
        copies.append(copy)

    def own_kv():
        total = dkv[pl.ds(pl.multiple_of(y * rows, BLK), rows)].astype(F32)
        for peer in peers:
            remote(land.at[peer], land.at[peer], ssem.at[0], rsem.at[peer], {"ctx": peer}).wait_recv()
            total = total + land[peer].astype(F32)
        return total.astype(BF)

    last(ctx, table, y, dq, own_kv, h1, tok, wall, dx1, vec, gvec, gq, gtok)
    for copy in copies:
        copy.wait_send()


def last_call(tbl, dq, dkv, h1, tok, wall, dx1, vec, gvec, ctx, head):
    rows, width = h1.shape
    dp, r = wall.shape[:2]
    return pl.pallas_call(
        functools.partial(last_kernel, ctx),
        out_shape=(shape(dp, r, head), shape(rows, width)),
        in_specs=[SM] + [VM] * 8, out_specs=(VM,) * 2,
        scratch_shapes=[pltpu.VMEM((ctx, rows, 2 * width), BF), DMA((ctx,)), DMA((ctx,))],
        compiler_params=params(62, collective_id=2, has_side_effects=True), name="last",
    )(tbl, dq, dkv, h1, tok, wall, dx1, vec, gvec)


def shards(tokens, block_table, ln1_gain, ln1_bias, w_qkv, bias_query, bias_value, w_out, bias_out,
           ln2_gain, ln2_bias, w_up, bias_up, w_down, bias_down, cotangent):
    dp, ctx = lax.axis_size("dp"), lax.axis_size("ctx")
    width, hidden = tokens.shape[2], w_up.shape[1]
    r = w_qkv.shape[0]
    head = 128 + 3 * width
    third = (width + 2 * hidden) // 3
    off_up = head + width
    off_down = off_up + hidden
    small = jnp.concatenate([jnp.stack([ln1_gain, ln1_bias, bias_query, bias_value, bias_out, ln2_gain, ln2_bias,
                                        bias_down]), bias_up.reshape(4, r), jnp.zeros((116, r), BF)]).T
    cat = jnp.concatenate([small, w_qkv, w_out, w_up] + [w_down[j * r:(j + 1) * r] for j in range(4)], axis=1)
    tok_all, wall = gather(tokens[0], cat, dp, ctx, head, third)
    h1, q, kv, att, lse, vec = attend(block_table, tok_all, wall, ctx)
    bup = vec[8:12].reshape(4, dp, r).transpose(1, 0, 2).reshape(1, hidden)
    out, gt, da, dx1, delta, gvec, gup = feed_call(block_table, tokens[0], att, wall, cotangent[0], vec, bup,
                                                   ctx, off_up, off_down, 3 * third)
    dq, dkv = attend_back(block_table, q, kv, da, lse, delta, ctx)
    gvec = gvec.at[8:12].set(gup.reshape(dp, 4, r).transpose(1, 0, 2).reshape(4, width))
    gq, gtok = last_call(block_table, dq, dkv, h1, tokens[0], wall, dx1, vec, gvec, ctx, head)
    total = scatter(gq, gt, dp, ctx, head, third)
    rows = total[:, 0:128].T
    g_down = jnp.concatenate([total[:, off_down + j * width:off_down + (j + 1) * width] for j in range(4)], axis=0)
    return (out[None], gtok[None], rows[0], rows[1], total[:, 128:head], rows[2], rows[3],
            total[:, head:off_up], rows[4], rows[5], rows[6], total[:, off_up:off_down],
            rows[8:12].reshape(4 * r), g_down, rows[7])


def solution(mesh):
    row, mat = P("dp"), P("dp", None)
    act = P("dp", "ctx", None)
    in_specs = (act, P(), row, row, mat, row, row, mat, row, row, row, mat, row, mat, row, act)
    out_specs = (act, act, row, row, mat, row, row, mat, row, row, row, mat, row, mat, row)
    return jax.shard_map(shards, mesh=mesh, in_specs=in_specs, out_specs=out_specs, check_vma=False)
```

```python
import functools
import jax
import jax.numpy as jnp
from jax import lax
from jax.experimental import pallas as pl
from jax.experimental.pallas import tpu as pltpu
from jax.sharding import PartitionSpec as P

ANY = pl.BlockSpec(memory_space=pl.ANY)
VM = pl.BlockSpec(memory_space=pltpu.VMEM)
DMA = pltpu.SemaphoreType.DMA


def near_first(count):
    order = []
    for step in range(1, count):
        order.append((step + 1) // 2 if step % 2 else count - step // 2)
    return order


class Spot:
    def __init__(self, dp, ctx):
        self.dp, self.ctx = dp, ctx
        self.lines = dp // 4
        me = lax.axis_index("dp")
        self.y = lax.axis_index("ctx")
        self.z = me // 4
        self.x = (me // 2) % 2
        self.c = me % 2
        self.me = me

    def dp_at(self, z, x, c):
        return (z * 2 + x) * 2 + c

    def z_at(self, k):
        return lax.rem(self.z + k, self.lines)

    def y_at(self, k):
        return lax.rem(self.y + k, self.ctx)

    def barrier(self):
        sem = pltpu.get_barrier_semaphore()
        peers = [{"dp": self.dp_at(self.z_at(k), self.x, self.c)} for k in range(1, self.lines)]
        peers.append({"dp": self.dp_at(self.z, 1 - self.x, self.c)})
        peers.append({"dp": self.dp_at(self.z, self.x, 1 - self.c)})
        peers += [{"ctx": self.y_at(k)} for k in range(1, self.ctx)]
        for peer in peers:
            pl.semaphore_signal(sem, inc=1, device_id=peer, device_id_type=pl.DeviceIdType.MESH)
        pl.semaphore_wait(sem, len(peers))


def remote(src, dst, ssem, rsem, device):
    return pltpu.make_async_remote_copy(
        src_ref=src, dst_ref=dst, send_sem=ssem, recv_sem=rsem,
        device_id=device, device_id_type=pl.DeviceIdType.MESH,
    )


def gather_kernel(dp, ctx, head, third, tok_ref, cat_ref, tok_all, wall,
                  loc, st, rt, sz, rz, sx, rx, sy, ry, sc, rc):
    at = Spot(dp, ctx)
    lines = at.lines
    ky = at.y % 2
    mine = pl.multiple_of(head + third + ky * third, 128)
    other = pl.multiple_of(head + third + (1 - ky) * third, 128)
    cols = {"q": pl.ds(0, head), "m": pl.ds(mine, third), "t": pl.ds(head, third), "o": pl.ds(other, third)}
    num = {"q": 0, "m": 1, "t": 2, "o": 3}
    own = at.me
    mate = {"dp": at.dp_at(at.z, at.x, 1 - at.c)}
    across = {"dp": at.dp_at(at.z, 1 - at.x, at.c)}
    pair = {"ctx": at.y + 1 - 2 * ky}
    at.barrier()
    copies = []

    def go(copy):
        copy.start()
        copies.append(copy)

    local = [pltpu.make_async_copy(cat_ref, wall.at[own], loc.at[0]),
             pltpu.make_async_copy(tok_ref, tok_all.at[at.y], loc.at[1])]
    for copy in local:
        copy.start()

    def block(b, z, x, c):
        return wall.at[at.dp_at(z, x, c), :, cols[b]]

    def own_block(b):
        return cat_ref.at[:, cols[b]]

    def send_z(b):
        for k in near_first(lines):
            go(remote(own_block(b), block(b, at.z, at.x, at.c), sz.at[num[b], k], rz.at[num[b], at.z],
                      {"dp": at.dp_at(at.z_at(k), at.x, at.c)}))

    def send_x(b, z, k, src):
        go(remote(src, block(b, z, at.x, at.c), sx.at[num[b], k], rx.at[num[b], z], across))

    def send_c(b, z, x, k, kx, src):
        go(remote(src, block(b, z, x, at.c), sc.at[num[b], k, kx], rc.at[num[b], z, x], mate))

    def send_y(z, x, k, kx, src):
        go(remote(src, block("m", z, x, at.c), sy.at[k, kx], ry.at[z, x], pair))

    def got_z(b, k):
        z = at.z_at(k)
        remote(own_block(b), block(b, z, at.x, at.c), sz.at[num[b], 0], rz.at[num[b], z], across).wait_recv()

    def got_x(b, k):
        z = at.z_at(k)
        remote(own_block(b), block(b, z, 1 - at.x, at.c), sz.at[num[b], 0], rx.at[num[b], z], across).wait_recv()

    def got_y(k, kx):
        z, x = at.z_at(k), (at.x + kx) % 2
        remote(own_block("o"), block("o", z, x, at.c), sz.at[0, 0], ry.at[z, x], across).wait_recv()

    def got_c(b, k, kx):
        z, x = at.z_at(k), (at.x + kx) % 2
        remote(own_block(b), block(b, z, x, 1 - at.c), sz.at[0, 0], rc.at[num[b], z, x], across).wait_recv()

    order = [0] + near_first(lines)
    for k in range(1, ctx):
        go(remote(tok_ref, tok_all.at[at.y], st.at[k], rt.at[at.y], {"ctx": at.y_at(k)}))
    for b in ("q", "m", "t"):
        send_z(b)
    for b in ("q", "m", "t"):
        send_x(b, at.z, 0, own_block(b))
        send_c(b, at.z, at.x, 0, 0, own_block(b))
        for k in order[1:]:
            got_z(b, k)
            z = at.z_at(k)
            src = block(b, z, at.x, at.c)
            send_x(b, z, k, src)
            if b == "m":
                send_y(z, at.x, k, 0, src)
            send_c(b, z, at.x, k, 0, src)
        for k in order:
            got_x(b, k)
            z = at.z_at(k)
            src = block(b, z, 1 - at.x, at.c)
            if b == "m":
                send_y(z, 1 - at.x, k, 1, src)
            send_c(b, z, 1 - at.x, k, 1, src)
    send_c("o", at.z, at.x, 0, 0, own_block("o"))
    for kx in range(2):
        for k in order:
            if k == 0 and kx == 0:
                continue
            got_y(k, kx)
            z, x = at.z_at(k), (at.x + kx) % 2
            send_c("o", z, x, k, kx, block("o", z, x, at.c))
    for b in ("q", "m", "t", "o"):
        for kx in range(2):
            for k in order:
                got_c(b, k, kx)
    for k in range(1, ctx):
        y = at.y_at(k)
        remote(tok_ref, tok_all.at[y], st.at[0], rt.at[y], across).wait_recv()
    for copy in copies:
        copy.wait_send()
    for copy in local:
        copy.wait()


def gather(tok, cat, dp, ctx, head, third):
    lines = dp // 4
    rows, width = cat.shape
    return pl.pallas_call(
        functools.partial(gather_kernel, dp, ctx, head, third),
        out_shape=(jax.ShapeDtypeStruct((ctx, *tok.shape), tok.dtype),
                   jax.ShapeDtypeStruct((dp, rows, width), cat.dtype)),
        in_specs=[VM, VM], out_specs=(ANY, ANY),
        scratch_shapes=[DMA((2,)), DMA((ctx,)), DMA((ctx,)),
                        DMA((3, lines)), DMA((3, lines)), DMA((3, lines)), DMA((3, lines)),
                        DMA((lines, 2)), DMA((lines, 2)), DMA((4, lines, 2)), DMA((4, lines, 2))],
        compiler_params=pltpu.CompilerParams(collective_id=0, has_side_effects=True, vmem_limit_bytes=32 * 2**20),
    )(tok, cat)


def scatter_kernel(dp, ctx, head, third, gq, gt, out, a_core, a_pair, a_x, a_z, a_y, stage, total,
                   loc, s1, r1, s2, r2, s3, r3, s4, r4, s5, r5):
    at = Spot(dp, ctx)
    lines = at.lines
    rows = gq.shape[1]
    ky = at.y % 2
    mine = pl.multiple_of(head + third + ky * third, 128)
    other = pl.multiple_of(head + third + (1 - ky) * third, 128)
    cols = {"q": pl.ds(0, head), "m": pl.ds(mine, third), "t": pl.ds(head, third), "o": pl.ds(other, third)}
    size = {"q": head, "m": third, "t": third, "o": third}
    num = {"q": 0, "m": 1, "t": 2, "o": 3}
    mate = {"dp": at.dp_at(at.z, at.x, 1 - at.c)}
    across = {"dp": at.dp_at(at.z, 1 - at.x, at.c)}
    pair = {"ctx": at.y + 1 - 2 * ky}
    at.barrier()
    copies = []

    def go(copy):
        copy.start()
        copies.append(copy)

    first = {"m": pl.multiple_of(third + ky * third, 128), "o": pl.multiple_of(third + (1 - ky) * third, 128), "t": 0}

    def full(b, at_dp):
        if b == "q":
            return gq.at[at_dp]
        return gt.at[at_dp, :, pl.ds(first[b], third)]

    order = [0] + near_first(lines)
    order = order[::-1]
    spots = [(k, kx) for kx in (1, 0) for k in order]

    def where(k, kx):
        return at.z_at(k), (at.x + kx) % 2

    def land(ref, b, *idx):
        return ref.at[(num[b], *idx, slice(None), pl.ds(0, size[b]))]

    blocks = ("o", "m", "t", "q")
    for b in blocks:
        for k, kx in spots:
            z, x = where(k, kx)
            go(remote(full(b, at.dp_at(z, x, 1 - at.c)), land(a_core, b, z, x),
                      s1.at[num[b], k, kx], r1.at[num[b], z, x], mate))
    def fetch(b, k, kx):
        z, x = where(k, kx)
        return pltpu.make_async_copy(full(b, at.dp_at(z, x, at.c)), land(stage, b, z, x),
                                     loc.at[num[b], k, kx])
    for b in blocks:
        for k, kx in spots:
            fetch(b, k, kx).start()

    def take(sem, dst):
        remote(dst, dst, s1.at[0, 0, 0], sem, across).wait_recv()

    def added(b, k, kx):
        z, x = where(k, kx)
        fetch(b, k, kx).wait()
        here = land(a_core, b, z, x)
        take(r1.at[num[b], z, x], here)
        here[...] = here[...] + land(stage, b, z, x)[...]
        return here

    for b in blocks:
        if b == "o":
            for k, kx in spots:
                z, x = where(k, kx)
                go(remote(added(b, k, kx), a_pair.at[z, x], s2.at[k, kx], r2.at[z, x], pair))
            continue
        for k, kx in spots:
            z, x = where(k, kx)
            here = added(b, k, kx)
            if b == "m":
                take(r2.at[z, x], a_pair.at[z, x])
                here[...] = here[...] + a_pair[z, x]
            if kx == 1:
                go(remote(here, land(a_x, b, z), s3.at[num[b], k], r3.at[num[b], z], across))
        for k in order:
            z = at.z_at(k)
            here = land(a_core, b, z, at.x)
            take(r3.at[num[b], z], land(a_x, b, z))
            here[...] = here[...] + land(a_x, b, z)[...]
            if k:
                go(remote(here, land(a_z, b, at.z), s4.at[num[b], k], r4.at[num[b], at.z],
                          {"dp": at.dp_at(z, at.x, at.c)}))
    for b in ("m", "t", "q"):
        acc = land(a_core, b, at.z, at.x)[...].astype(jnp.float32)
        for k in near_first(lines):
            z = at.z_at(k)
            take(r4.at[num[b], z], land(a_z, b, z))
            acc = acc + land(a_z, b, z)[...].astype(jnp.float32)
        land(total, b)[...] = acc
        land(a_core, b, at.z, at.x)[...] = acc.astype(jnp.bfloat16)
        for k in range(1, ctx):
            go(remote(land(a_core, b, at.z, at.x), land(a_y, b, at.y), s5.at[num[b], k], r5.at[num[b], at.y],
                      {"ctx": at.y_at(k)}))
    outs = []
    for b in ("t", "q", "m", "o"):
        if b == "m":
            acc = land(total, b)[...]
        elif b == "o":
            acc = jnp.zeros((rows, third), jnp.float32)
        else:
            acc = land(total, b)[...]
        for k in range(1, ctx):
            y = at.y_at(k)
            if b in ("t", "q") or (b == "m" and k % 2 == 0):
                take(r5.at[num[b], y], land(a_y, b, y))
                acc = acc + land(a_y, b, y)[...].astype(jnp.float32)
            elif b == "o" and k % 2 == 1:
                here = a_y.at[1, y, :, pl.ds(0, third)]
                take(r5.at[1, y], here)
                acc = acc + here[...].astype(jnp.float32)
        land(total, b)[...] = acc
        copy = pltpu.make_async_copy(land(total, b), out.at[:, cols[b]], loc.at[num[b], 0, 0])
        copy.start()
        outs.append(copy)
    for copy in copies:
        copy.wait_send()
    for copy in outs:
        copy.wait()


def scatter(gq, gt, dp, ctx, head, third):
    lines = dp // 4
    _, rows, width = gq.shape[0], gq.shape[1], gq.shape[2] + gt.shape[2]
    bf, f32 = jnp.bfloat16, jnp.float32
    return pl.pallas_call(
        functools.partial(scatter_kernel, dp, ctx, head, third),
        out_shape=jax.ShapeDtypeStruct((rows, width), f32),
        in_specs=[ANY, ANY], out_specs=ANY,
        scratch_shapes=[pltpu.VMEM((4, lines, 2, rows, head), bf), pltpu.VMEM((lines, 2, rows, third), bf),
                        pltpu.VMEM((3, lines, rows, head), bf), pltpu.VMEM((3, lines, rows, head), bf),
                        pltpu.VMEM((3, ctx, rows, head), bf), pltpu.VMEM((4, lines, 2, rows, head), bf),
                        pltpu.VMEM((4, rows, head), f32),
                        DMA((4, lines, 2)), DMA((4, lines, 2)), DMA((4, lines, 2)),
                        DMA((lines, 2)), DMA((lines, 2)),
                        DMA((3, lines)), DMA((3, lines)), DMA((3, lines)), DMA((3, lines)),
                        DMA((3, ctx)), DMA((3, ctx))],
        compiler_params=pltpu.CompilerParams(collective_id=1, has_side_effects=True, vmem_limit_bytes=60 * 2**20),
    )(gq, gt)


F32, BF = jnp.float32, jnp.bfloat16
HEADS, HD, BLK = 12, 64, 256
PAIRS, LANES = HEADS // 2, 2 * HD


def dot(a, b):
    return jnp.dot(a, b, preferred_element_type=F32)


def dot_t(a, b):
    return lax.dot_general(a, b, (((1,), (1,)), ((), ())), preferred_element_type=F32)


def dot_l(a, b):
    return lax.dot_general(a, b, (((0,), (0,)), ((), ())), preferred_element_type=F32)


def normed(x):
    centred = x - jnp.mean(x, axis=-1, keepdims=True)
    inv = lax.rsqrt(jnp.mean(centred * centred, axis=-1, keepdims=True) + 1e-05)
    return centred * inv, inv


def norm_back(dy, unit, inv, gain):
    dn = dy * gain
    return inv * (dn - jnp.mean(dn, axis=-1, keepdims=True) - unit * jnp.mean(dn * unit, axis=-1, keepdims=True))


class Table:
    def __init__(self, tbl, nb, y, ordered=False):
        self.nb, self.half = nb, nb // 2
        self.own = [tbl[2 * y], tbl[2 * y + 1]]
        self.turned = self.own[0] >= self.half
        first_high = self.turned.astype(jnp.int32)
        self.place = [first_high, 1 - first_high]
        self.row_of = [first_high, 1 - first_high]
        self.slot_of = [first_high, 1 - first_high]
        self.block = [jnp.minimum(self.own[0], self.own[1]), jnp.maximum(self.own[0], self.own[1])]
        self.tbl = tbl
        if ordered:
            self.row_of, self.slot_of, self.pos = [0, 1], [0, 1], list(range(nb))
            return
        self.pos = []
        for j in range(nb):
            at = jnp.int32(0)
            for p in range(nb):
                at = at + jnp.where(tbl[p] == j, p, 0)
            self.pos.append(at)

    def keys(self, slot):
        return self.half if slot == 0 else self.nb

    def masked(self, slot, j):
        return j >= 1 if slot == 0 else j > self.half


def rows_of(ref, *idx):
    value = ref[idx]
    return value.reshape(value.shape[0] * value.shape[1], value.shape[2])


def block_rows(i):
    return pl.ds(i * BLK if isinstance(i, int) else pl.multiple_of(i * BLK, BLK), BLK)


def lane_masks(rows):
    lane = lax.broadcasted_iota(jnp.int32, (rows, LANES), 1)
    return [lane < HD, lane >= HD]


def project(ctx, table, tok, wall, h1, q, kv, vec, y, ordered=None):
    gain, shift = vec[0:1], vec[1:2]
    width = tok.shape[2]
    zero = jnp.zeros((1, width), F32)
    kv_bias = jnp.concatenate([zero, vec[3:4]], axis=1)
    w_kv = rows_of(wall, slice(None), slice(None), slice(128 + width, 128 + 3 * width))

    def rows(r, carry):
        x = tok[r // 2, pl.ds(pl.multiple_of((r % 2) * BLK, BLK), BLK)].astype(F32)
        low = (normed(x)[0] * gain + shift).astype(BF)
        kv[block_rows(r if ordered is None else table.tbl[r])] = (dot(low, w_kv) + kv_bias).astype(BF)
        return carry

    lax.fori_loop(0, 2 * ctx, rows, 0)
    w_q = rows_of(wall, slice(None), slice(None), slice(128, 128 + width))

    def own(i, carry):
        at = pl.ds(pl.multiple_of(i * BLK, BLK), BLK)
        low = (normed(tok[y, at].astype(F32))[0] * gain + shift).astype(BF)
        if ordered is None:
            h1[at] = low
        else:
            cot, tok_slots, cot_slots = ordered
            at, stored = block_rows(jnp.where(i == 0, table.place[0], table.place[1])), at
            h1[:, at] = jnp.transpose(low)
            tok_slots[at] = tok[y, stored]
            cot_slots[at] = cot[stored]
        q[at] = ((dot(low, w_q) + vec[2:3]).astype(BF).astype(F32) * HD ** (-0.5)).astype(BF)
        return carry

    lax.fori_loop(0, 2, own, 0)


def attend_pair(hp, table, q, kv, att, lse_acc, width):
    lanes = pl.ds(pl.multiple_of(hp * LANES, LANES), LANES)
    v_lanes = pl.ds(pl.multiple_of(width + hp * LANES, LANES), LANES)
    masks = lane_masks(BLK)
    lane = lax.broadcasted_iota(jnp.int32, (BLK, LANES), 1)
    for slot in range(2):
        q2 = q[block_rows(table.row_of[slot]), lanes]
        spots = [block_rows(table.pos[j]) for j in range(table.keys(slot))]
        mixed = []
        for h in range(2):
            qm = jnp.where(masks[h], q2, jnp.zeros_like(q2))
            scores = []
            for j, at in enumerate(spots):
                s = dot_t(qm, kv[at, lanes])
                if table.masked(slot, j):
                    s = jnp.where(j <= table.block[slot], s, -1e30)
                scores.append(s)
            largest = functools.reduce(jnp.maximum, scores)
            largest = jnp.max(largest, axis=-1, keepdims=True)
            exps = [jnp.exp(s - largest) for s in scores]
            total = jnp.sum(functools.reduce(jnp.add, exps), axis=-1, keepdims=True)
            out = functools.reduce(jnp.add, [dot(e.astype(BF), kv[at, v_lanes]) for e, at in zip(exps, spots)])
            mixed.append(out / total)
            lse_acc[slot] = jnp.where(lane == 2 * hp + h, largest + jnp.log(total), lse_acc[slot])
        att[slot, :, lanes] = jnp.where(masks[0], mixed[0], mixed[1]).astype(BF)


def attend_back_pair(hp, table, q, kv, da, lse, delta, put_dq, dk_acc, dv_acc, width):
    lanes = pl.ds(pl.multiple_of(hp * LANES, LANES), LANES)
    v_lanes = pl.ds(pl.multiple_of(width + hp * LANES, LANES), LANES)
    masks = lane_masks(BLK)
    for slot in (1, 0):
        row = block_rows(table.row_of[slot])
        q2, da2 = q[row, lanes], da[row, lanes]
        dq_acc = None
        for h in range(2):
            qm = jnp.where(masks[h], q2, jnp.zeros_like(q2))
            dam = jnp.where(masks[h], da2, jnp.zeros_like(da2))
            lse_row = lse[slot, pl.ds(2 * hp + h, 1), :]
            delta_row = delta[table.row_of[slot], pl.ds(2 * hp + h, 1), :]
            for j in range(table.keys(slot)):
                at = block_rows(table.pos[j])
                k2, v2 = kv[at, lanes], kv[at, v_lanes]
                st = dot_t(k2, qm)
                if table.masked(slot, j):
                    st = jnp.where(j <= table.block[slot], st, -1e30)
                pt = jnp.exp(st - lse_row)
                dst = (pt * (dot_t(v2, dam) - delta_row)).astype(BF)
                dv, dk = dot(pt.astype(BF), dam), dot(dst, qm)
                if slot == 1 and h == 0:
                    dv_acc[j], dk_acc[j] = dv, dk
                else:
                    dv_acc[j] += dv
                    dk_acc[j] += dk
                part = dot_l(dst, jnp.where(masks[h], k2, jnp.zeros_like(k2)))
                dq_acc = part if dq_acc is None else dq_acc + part
        put_dq(slot, (dq_acc * HD ** (-0.5)).astype(BF))


def feed(nd, off_up, off_down, table, tok, att, wall, cot, vec, bup, out, gt, da, dx1, delta, gvec, gup,
         x1, h2, acc, dh2):
    rows, width = cot.shape
    dp, r = wall.shape[0], wall.shape[1]
    chunk = 4 * nd * r
    w_out = rows_of(wall, slice(None), slice(None), slice(off_up - width, off_up))
    for i in range(2):
        at = pl.ds(i * BLK, BLK)
        mid = tok[at].astype(F32) + (dot(att[table.slot_of[i]], w_out) + vec[4:5])
        x1[at] = mid
        h2[at] = (normed(mid)[0] * vec[5:6] + vec[6:7]).astype(BF)
        acc[at] = mid + vec[7:8]
    dh2[...] = jnp.zeros_like(dh2)
    g = cot[...]

    def part(f, carry):
        cols = pl.ds(pl.multiple_of(off_up + f * chunk, 128), chunk)
        w_up = rows_of(wall, slice(None), slice(None), cols)
        w_down = jnp.concatenate(
            [wall[f * nd + d, :, pl.ds(off_down + j * width, width)] for d in range(nd) for j in range(4)], axis=0)
        low = h2[...]
        u = dot(low, w_up) + bup[:, pl.ds(pl.multiple_of(f * chunk, 128), chunk)]
        sq = u * u
        t = jnp.tanh(u * (0.7978845608028654 + 0.03567740813636141 * sq))
        act = (0.5 * u * (1.0 + t)).astype(BF)
        slope = 0.5 * (1.0 + t) + 0.5 * u * (1.0 - t * t) * (0.7978845608028654 + 0.10703222440908423 * sq)
        acc[...] += dot(act, w_down)
        du = slope * dot_t(g, w_down)
        dul = du.astype(BF)
        gup[:, pl.ds(pl.multiple_of(f * chunk, 128), chunk)] = jnp.sum(dul.astype(F32), axis=0, keepdims=True)
        dh2[...] += dot_t(dul, w_up)
        g_up = dot_l(low, dul).astype(BF)
        gt[:, :, pl.ds(pl.multiple_of(width + f * chunk, 128), chunk)] = g_up.reshape(dp, r, chunk)
        g_down = dot_l(act, g).astype(BF)
        for d in range(nd):
            for j in range(4):
                piece = g_down[(4 * d + j) * r:(4 * d + j + 1) * r]
                gt[f * nd + d, :, pl.ds(width + off_down - off_up + j * width, width)] = piece
        return carry

    lax.fori_loop(0, dp // nd, part, 0)
    out[...] = acc[...].astype(BF)
    gf = g.astype(F32)
    unit, inv = normed(x1[...])
    dy = dh2[...]
    mid_grad = gf + norm_back(dy, unit, inv, vec[5:6])
    dx1[...] = mid_grad
    branch = mid_grad.astype(BF)
    gvec[...] = jnp.zeros_like(gvec)
    gvec[4:5] = jnp.sum(branch.astype(F32), axis=0, keepdims=True)
    gvec[5:6] = jnp.sum(dy * unit, axis=0, keepdims=True)
    gvec[6:7] = jnp.sum(dy, axis=0, keepdims=True)
    gvec[7:8] = jnp.sum(gf, axis=0, keepdims=True)
    head = lax.broadcasted_iota(jnp.int32, (16, width), 0)
    pick = (lax.broadcasted_iota(jnp.int32, (16, width), 1) // HD == head).astype(F32)
    grad = None
    for i in range(2):
        own = att[table.slot_of[i]]
        low = branch[i * BLK:(i + 1) * BLK]
        piece = dot_l(own, low)
        grad = piece if grad is None else grad + piece
        back = dot_t(low, w_out).astype(BF)
        da[pl.ds(i * BLK, BLK)] = back
        prod = back.astype(F32) * own.astype(F32)
        delta[i] = lax.dot_general(pick, prod, (((1,), (1,)), ((), ())), precision=lax.Precision.HIGHEST,
                                   preferred_element_type=F32)
    gt[:, :, 0:width] = grad.astype(BF).reshape(dp, r, width)


def last(ctx, table, y, dq, own_kv, h1, tok, wall, dx1, vec, gvec, gq, gtok):
    width = h1.shape[1]
    dp, r = wall.shape[0], wall.shape[1]
    w_q = rows_of(wall, slice(None), slice(None), slice(128, 128 + width))
    low = h1[...]
    dq_all = jnp.concatenate([dq[table.slot_of[0]], dq[table.slot_of[1]]], axis=0)
    gq[:, :, 128:128 + width] = dot_l(low, dq_all).astype(BF).reshape(dp, r, width)
    dh1 = dot_t(dq_all, w_q)
    dkv = own_kv()
    w_kv = rows_of(wall, slice(None), slice(None), slice(128 + width, 128 + 3 * width))
    gq[:, :, 128 + width:128 + 3 * width] = dot_l(low, dkv).astype(BF).reshape(dp, r, 2 * width)
    dh1 = dh1 + dot_t(dkv, w_kv)
    unit, inv = normed(tok[...].astype(F32))
    gtok[...] = (dx1[...] + norm_back(dh1, unit, inv, vec[0:1])).astype(BF)
    sums = [jnp.sum(dh1 * unit, axis=0, keepdims=True), jnp.sum(dh1, axis=0, keepdims=True),
            jnp.sum(dq_all.astype(F32), axis=0, keepdims=True),
            jnp.sum(dkv[:, width:].astype(F32), axis=0, keepdims=True)]
    table_rows = jnp.concatenate(sums + [gvec[4:16], jnp.zeros((112, width), F32)], axis=0)
    gq[:, :, 0:128] = jnp.transpose(table_rows).astype(BF).reshape(dp, r, 128)


SM = pl.BlockSpec(memory_space=pltpu.SMEM)


def params(limit, **more):
    return pltpu.CompilerParams(vmem_limit_bytes=limit * 2**20, **more)


def shape(*dims, dtype=BF):
    return jax.ShapeDtypeStruct(dims, dtype)


def attend_kernel(ctx, ordered, tbl, tok, wall, *rest):
    width = tok.shape[2]
    y = lax.axis_index("ctx")
    table = Table(tbl, 2 * ctx, y, ordered)
    extra = None
    if ordered:
        extra, rest = (rest[0], *rest[1:3]), rest[3:]
    h1, q, kv, att, lse, vec, lse_acc = rest
    small = rows_of(wall, slice(None), slice(None), slice(0, 128)).astype(F32)
    vec[...] = jnp.transpose(small)[0:16]
    project(ctx, table, tok, wall, h1, q, kv, vec, y, extra)
    lse_acc[...] = jnp.zeros_like(lse_acc)

    def pair(hp, carry):
        attend_pair(hp, table, q, kv, att, lse_acc, width)
        return carry

    lax.fori_loop(0, PAIRS, pair, 0)
    for slot in range(2):
        lse[slot] = jnp.transpose(lse_acc[slot])[0:16]


def attend(tbl, tok_all, wall, ctx, cot=None):
    rows, width = tok_all.shape[1:]
    ordered = cot is not None
    slots = (shape(rows, width), shape(rows, width), shape(width, rows)) if ordered else (shape(rows, width),)
    outs = slots + (shape(rows, width), shape(ctx * rows, 2 * width), shape(2, BLK, width),
                    shape(2, 16, BLK, dtype=F32), shape(16, width, dtype=F32))
    args = (tbl, tok_all, wall) + ((cot,) if ordered else ())
    return pl.pallas_call(
        functools.partial(attend_kernel, ctx, ordered),
        out_shape=outs, in_specs=[SM] + [VM] * (len(args) - 1), out_specs=(VM,) * len(outs),
        scratch_shapes=[pltpu.VMEM((2, BLK, LANES), F32)],
        compiler_params=params(62), name="attend",
    )(*args)


def feed_kernel(ctx, nd, off_up, off_down, tbl, tok, att, wall, cot, vec, bup, *rest):
    table = Table(tbl, 2 * ctx, lax.axis_index("ctx"))
    feed(nd, off_up, off_down, table, tok, att, wall, cot, vec, bup, *rest)


def feed_call(tbl, tok, att, wall, cot, vec, bup, ctx, off_up, off_down, gt_cols):
    rows, width = cot.shape
    dp, r = wall.shape[:2]
    return pl.pallas_call(
        functools.partial(feed_kernel, ctx, dp // 4, off_up, off_down),
        out_shape=(shape(rows, width), shape(dp, r, gt_cols), shape(rows, width), shape(rows, width, dtype=F32),
                   shape(2, 16, BLK, dtype=F32), shape(16, width, dtype=F32), shape(1, bup.shape[1], dtype=F32)),
        in_specs=[SM] + [VM] * 6, out_specs=(VM,) * 7,
        scratch_shapes=[pltpu.VMEM((rows, width), F32), pltpu.VMEM((rows, width), BF),
                        pltpu.VMEM((rows, width), F32), pltpu.VMEM((rows, width), F32)],
        compiler_params=params(62), name="feed",
    )(tbl, tok, att, wall, cot, vec, bup)


def attend_back_kernel(ctx, tbl, q, kv, da, lse, delta, dq, dkv, dk_acc, dv_acc):
    width = q.shape[1]
    table = Table(tbl, 2 * ctx, lax.axis_index("ctx"))

    def pair(hp, carry):
        def put_dq(slot, value):
            dq[slot, :, pl.ds(pl.multiple_of(hp * LANES, LANES), LANES)] = value

        attend_back_pair(hp, table, q, kv, da, lse, delta, put_dq, dk_acc, dv_acc, width)
        for j in range(2 * ctx):
            at = pl.ds(pl.multiple_of(table.pos[j] * BLK, BLK), BLK)
            dkv[at, pl.ds(pl.multiple_of(hp * LANES, LANES), LANES)] = dk_acc[j].astype(BF)
            dkv[at, pl.ds(pl.multiple_of(width + hp * LANES, LANES), LANES)] = dv_acc[j].astype(BF)
        return carry

    lax.fori_loop(0, PAIRS, pair, 0)


def attend_back(tbl, q, kv, da, lse, delta, ctx):
    rows, width = q.shape
    return pl.pallas_call(
        functools.partial(attend_back_kernel, ctx),
        out_shape=(shape(2, BLK, width), shape(*kv.shape)),
        in_specs=[SM] + [VM] * 5, out_specs=(VM,) * 2,
        scratch_shapes=[pltpu.VMEM((2 * ctx, BLK, LANES), F32), pltpu.VMEM((2 * ctx, BLK, LANES), F32)],
        compiler_params=params(62), name="attend_back",
    )(tbl, q, kv, da, lse, delta)


def last_kernel(ctx, tbl, dq, dkv, h1, tok, wall, dx1, vec, gvec, gq, gtok, land, ssem, rsem):
    rows = h1.shape[0]
    y = lax.axis_index("ctx")
    table = Table(tbl, 2 * ctx, y)
    sem = pltpu.get_barrier_semaphore()
    peers = [lax.rem(y + k, ctx) for k in range(1, ctx)]
    for peer in peers:
        pl.semaphore_signal(sem, inc=1, device_id={"ctx": peer}, device_id_type=pl.DeviceIdType.MESH)
    pl.semaphore_wait(sem, ctx - 1)
    copies = []
    for k, peer in enumerate(peers):
        copy = remote(dkv.at[pl.ds(pl.multiple_of(peer * rows, BLK), rows)], land.at[y], ssem.at[k], rsem.at[y], {"ctx": peer})
        copy.start()
        copies.append(copy)

    def own_kv():
        total = dkv[pl.ds(pl.multiple_of(y * rows, BLK), rows)].astype(F32)
        for peer in peers:
            remote(land.at[peer], land.at[peer], ssem.at[0], rsem.at[peer], {"ctx": peer}).wait_recv()
            total = total + land[peer].astype(F32)
        return total.astype(BF)

    last(ctx, table, y, dq, own_kv, h1, tok, wall, dx1, vec, gvec, gq, gtok)
    for copy in copies:
        copy.wait_send()


def last_call(tbl, dq, dkv, h1, tok, wall, dx1, vec, gvec, ctx, head):
    rows, width = h1.shape
    dp, r = wall.shape[:2]
    return pl.pallas_call(
        functools.partial(last_kernel, ctx),
        out_shape=(shape(dp, r, head), shape(rows, width)),
        in_specs=[SM] + [VM] * 8, out_specs=(VM,) * 2,
        scratch_shapes=[pltpu.VMEM((ctx, rows, 2 * width), BF), DMA((ctx,)), DMA((ctx,))],
        compiler_params=params(62, collective_id=2, has_side_effects=True), name="last",
    )(tbl, dq, dkv, h1, tok, wall, dx1, vec, gvec)


class Reduce:
    def __init__(self, at, g, a_core, a_x, a_z, a_y, sems):
        self.at, self.g = at, g
        self.a_core, self.a_x, self.a_z, self.a_y = a_core, a_x, a_z, a_y
        self.s1, self.r1, self.s2, self.r2, self.s3, self.r3, self.s4, self.r4 = sems
        self.mate = {"dp": at.dp_at(at.z, at.x, 1 - at.c)}
        self.across = {"dp": at.dp_at(at.z, 1 - at.x, at.c)}

    def to_core(self, p, cols, held=None):
        return remote(self.g.at[:, :, 1 - self.at.c, :, cols if held is None else held], self.a_core.at[:, :, :, cols],
                      self.s1.at[p], self.r1.at[p], self.mate)

    def to_x(self, p, cols):
        return remote(self.a_core.at[:, 1 - self.at.x, :, cols], self.a_x.at[:, :, cols],
                      self.s2.at[p], self.r2.at[p], self.across)

    def to_z(self, p, cols, k):
        at = self.at
        return remote(self.a_core.at[at.z_at(k), at.x, :, cols], self.a_z.at[k - 1, :, cols],
                      self.s3.at[p, k - 1], self.r3.at[p, k - 1], {"dp": at.dp_at(at.z_at(k), at.x, at.c)})

    def to_y(self, p, cols, k):
        at = self.at
        return remote(self.a_core.at[at.z, at.x, :, cols], self.a_y.at[k - 1, :, cols],
                      self.s4.at[p, k - 1], self.r4.at[p, k - 1], {"ctx": at.y_at(k)})

    def level1(self, p, cols, held=None):
        self.to_core(p, cols, held).start()

    def level2(self, p, cols, held=None):
        self.to_core(p, cols, held).wait_recv()
        own = self.g[:, :, self.at.c, :, cols if held is None else held]
        self.a_core[:, :, :, cols] = self.a_core[:, :, :, cols] + own
        self.to_x(p, cols).start()

    def level3(self, p, cols):
        at = self.at
        self.to_x(p, cols).wait_recv()
        self.a_core[:, at.x, :, cols] = self.a_core[:, at.x, :, cols] + self.a_x[:, :, cols]
        for k in near_first(at.lines):
            self.to_z(p, cols, k).start()

    def level4(self, p, cols):
        at = self.at
        total = self.a_core[at.z, at.x, :, cols].astype(F32)
        for k in near_first(at.lines):
            self.to_z(p, cols, k).wait_recv()
            total = total + self.a_z[k - 1, :, cols].astype(F32)
        self.a_core[at.z, at.x, :, cols] = total.astype(BF)
        for k in range(1, at.ctx):
            self.to_y(p, cols, k).start()

    def level5(self, p, cols):
        at = self.at
        total = self.a_core[at.z, at.x, :, cols].astype(F32)
        for k in range(1, at.ctx):
            self.to_y(p, cols, k).wait_recv()
            total = total + self.a_y[k - 1, :, cols].astype(F32)
        return total

    def finish(self, p, cols, core=True, held=None):
        at = self.at
        if core:
            self.to_core(p, cols, held).wait_send()
        self.to_x(p, cols).wait_send()
        for k in range(1, at.lines):
            self.to_z(p, cols, k).wait_send()
        for k in range(1, at.ctx):
            self.to_y(p, cols, k).wait_send()


def backward_kernel(dp, ctx, tbl, tok, att, cot, q, kv, h1t, lse, vec, bup, wall,
                    out, gtok, o_small, o_qkv, o_out, o_up, o_down,
                    x1, acc, dh2, da, delta, dq, dk_acc, dv_acc, send, recv, dqkv, gup, rows,
                    wub, wdb, g, a_core, a_x, a_z, a_y, wsem, ys, yr, *sems):
    at = Spot(dp, ctx)
    width = tok.shape[1]
    r = wall.shape[1]
    nd = dp // 4
    chunk = 4 * nd * r
    off_out = 128 + 3 * width
    off_up = off_out + width
    off_down = off_up + 4 * chunk
    table = Table(tbl, 2 * ctx, at.y, True)
    red = Reduce(at, g, a_core, a_x, a_z, a_y, sems)
    lines = at.lines
    last_t = 9
    actb, dub, h2 = dqkv.at[0], dqkv.at[1], dqkv.at[2]

    def cols_of(p):
        return pl.ds(pl.multiple_of(p * width, 128), width)

    def cols_q(hp):
        return pl.ds(pl.multiple_of(last_t * width + hp * 3 * LANES, 128), 3 * LANES)

    def held_q(hp):
        return pl.ds(pl.multiple_of(last_t * width + 128 + lax.rem(hp, 3) * 3 * LANES, 128), 3 * LANES)

    cols_small = pl.ds(last_t * width + 3 * width, 128)
    held_small = pl.ds(last_t * width, 128)

    def up_copy(f, slot):
        return pltpu.make_async_copy(wall.at[:, :, pl.ds(pl.multiple_of(off_up + f * chunk, 128), chunk)],
                                     wub.at[slot], wsem.at[0, slot])

    def down_copy(f, slot, j):
        return pltpu.make_async_copy(wall.at[pl.ds(f * nd, nd), :, pl.ds(off_down + j * width, width)],
                                     wdb.at[slot, :, j], wsem.at[1 + j, slot])

    def plain_copy(i, slot):
        return pltpu.make_async_copy(wall.at[:, :, pl.ds(128 + i * width, width)], wub.at[slot], wsem.at[5, slot])

    def fetch(f, slot):
        up_copy(f, slot).start()
        for j in range(4):
            down_copy(f, slot, j).start()

    plain_copy(3, 2).start()
    fetch(0, 0)
    at.barrier()
    plain_copy(3, 2).wait()
    w_out = wub[2].reshape(width, width)
    halves = [pl.ds(i * BLK, BLK) for i in range(2)]
    for i, half in enumerate(halves):
        mid = tok[half].astype(F32) + (dot(att[table.slot_of[i]], w_out) + vec[4:5])
        x1[half] = mid
        low = (normed(mid)[0] * vec[5:6] + vec[6:7]).astype(BF)
        h2[half] = low
        acc[half] = mid + vec[7:8]
        dh2[half] = jnp.zeros((BLK, width), F32)

    def part(f, carry):
        slot = lax.rem(f, 2)

        @pl.when(f < 3)
        def _():
            fetch(f + 1, 1 - slot)

        up_copy(f, slot).wait()
        for j in range(4):
            down_copy(f, slot, j).wait()
        w_up = wub[slot].reshape(width, chunk)
        w_down = wdb[slot].reshape(chunk, width)
        hid = pl.ds(pl.multiple_of(f * chunk, 128), chunk)
        bias = bup[:, hid]
        sums = jnp.zeros((1, chunk), F32)
        for half in halves:
            u = dot(h2[half], w_up) + bias
            sq = u * u
            t = jnp.tanh(u * (0.7978845608028654 + 0.03567740813636141 * sq))
            act = (0.5 * u * (1.0 + t)).astype(BF)
            actb[half] = act
            slope = 0.5 * (1.0 + t) + 0.5 * u * (1.0 - t * t) * (0.7978845608028654 + 0.10703222440908423 * sq)
            acc[half] += dot(act, w_down)
            dul = (slope * dot_t(cot[half], w_down)).astype(BF)
            dub[half] = dul
            sums = sums + jnp.sum(dul.astype(F32), axis=0, keepdims=True)
            dh2[half] += dot_t(dul, w_up)
        gup[:, hid] = sums
        g[:, :, :, :, cols_of(f)] = dot_l(h2[...], dub[...]).astype(BF).reshape(lines, 2, 2, r, chunk)
        red.level1(f, cols_of(f))
        g_down = dot_l(actb[...], cot[...]).astype(BF).reshape(nd // 4, 2, 2, 4, r, width)
        for j in range(4):
            g[pl.ds(f * (nd // 4), nd // 4), :, :, :, pl.ds((4 + j) * width, width)] = g_down[:, :, :, j]
        for lag, level in ((1, red.level2), (2, red.level3), (3, red.level4)):
            @pl.when(f >= lag)
            def _():
                level(f - lag, cols_of(f - lag))
        return carry

    lax.fori_loop(0, 4, part, 0)
    for p in range(4, 8):
        red.level1(p, cols_of(p))
    for i, half in enumerate(halves):
        out[half] = jnp.where(table.turned, acc[halves[1 - i]], acc[half]).astype(BF)
    rows[...] = jnp.zeros_like(rows)
    lane_head = lax.broadcasted_iota(jnp.int32, (16, width), 0)
    pick = (lax.broadcasted_iota(jnp.int32, (16, width), 1) // HD == lane_head).astype(F32)
    grad = None
    w_out = wub[2].reshape(width, width)
    for i, half in enumerate(halves):
        gf = cot[half].astype(F32)
        unit, inv = normed(x1[half])
        dy = dh2[half]
        mid_grad = gf + norm_back(dy, unit, inv, vec[5:6])
        acc[half] = mid_grad
        branch = mid_grad.astype(BF)
        rows[4:5] += jnp.sum(branch.astype(F32), axis=0, keepdims=True)
        rows[5:6] += jnp.sum(dy * unit, axis=0, keepdims=True)
        rows[6:7] += jnp.sum(dy, axis=0, keepdims=True)
        rows[7:8] += jnp.sum(gf, axis=0, keepdims=True)
        own = att[table.slot_of[i]]
        piece = dot_l(own, branch)
        grad = piece if grad is None else grad + piece
        back = dot_t(branch, w_out).astype(BF)
        da[half] = back
        delta[i] = lax.dot_general(pick, back.astype(F32) * own.astype(F32), (((1,), (1,)), ((), ())),
                                   precision=lax.Precision.HIGHEST, preferred_element_type=F32)
    g[:, :, :, :, cols_of(8)] = grad.astype(BF).reshape(lines, 2, 2, r, width)
    red.level1(8, cols_of(8))
    for i in range(3):
        plain_copy(i, i).start()
    red.level2(3, cols_of(3))
    red.level3(2, cols_of(2))
    red.level4(1, cols_of(1))

    def done_t(p):
        total = red.level5(p, cols_of(p))

        @pl.when(p < 4)
        def _():
            o_up[:, pl.ds(pl.multiple_of(jnp.minimum(p, 3) * width, 128), width)] = total

        @pl.when(p >= 4)
        def _():
            o_down[pl.ds(pl.multiple_of(jnp.clip(p - 4, 0, 3) * r, 8), r), :] = total

    done_t(jnp.int32(0))
    other = lax.rem(at.y + 1, 2)
    mate_y = {"ctx": other}

    def kv_copy(hp):
        return remote(send.at[hp], recv.at[hp], ys.at[hp], yr.at[hp], mate_y)

    def q_grad(hp):
        lanes = pl.ds(pl.multiple_of(hp * LANES, LANES), LANES)
        kv_copy(hp).wait_recv()
        for i in range(2):
            dqkv[1 + i, :, lanes] = (dqkv[1 + i, :, lanes].astype(F32)
                                     + recv[hp, :, i * LANES:(i + 1) * LANES].astype(F32)).astype(BF)
        low = jnp.concatenate([dqkv[i, :, lanes] for i in range(3)], axis=1)

        @pl.when(hp >= 3)
        def _():
            red.to_core(last_t + jnp.maximum(hp - 3, 0), cols_q(0), held_q(0)).wait_send()

        g[:, :, :, :, held_q(hp)] = dot(h1t[...], low).astype(BF).reshape(lines, 2, 2, r, 3 * LANES)
        red.level1(last_t + hp, cols_q(hp), held_q(hp))

    def done_q(hp):
        total = red.level5(last_t + hp, cols_q(hp))
        for i in range(3):
            o_qkv[:, pl.ds(pl.multiple_of(i * width + hp * LANES, LANES), LANES)] = total[:, i * LANES:(i + 1) * LANES]

    def level_q(level, hp):
        if level == red.level2:
            level(last_t + hp, cols_q(hp), held_q(hp))
        else:
            level(last_t + hp, cols_q(hp))

    outermost = table.block[0] == 0

    def pair(hp, carry):
        def put_dq(slot, value):
            dq[slot] = value

        attend_back_pair(hp, table, q, kv, da, lse, delta, put_dq, dk_acc, dv_acc, width)
        lanes = pl.ds(pl.multiple_of(hp * LANES, LANES), LANES)
        for i, half in enumerate(halves):
            dqkv[0, half, lanes] = dq[i]
            outer, inner = (0, 1) if i == 0 else (3, 2)
            for n, sums in enumerate((dk_acc, dv_acc)):
                dqkv[1 + n, half, lanes] = jnp.where(outermost, sums[outer], sums[inner]).astype(BF)
                send[hp, half, n * LANES:(n + 1) * LANES] = jnp.where(outermost, sums[inner], sums[outer]).astype(BF)
        kv_copy(hp).start()

        @pl.when(hp < 5)
        def _():
            red.level2(4 + hp, cols_of(4 + hp))

        red.level3(3 + hp, cols_of(3 + hp))
        red.level4(2 + hp, cols_of(2 + hp))
        done_t(1 + hp)

        @pl.when(hp >= 2)
        def _():
            q_grad(hp - 2)

        for lag, level in ((3, red.level2), (4, red.level3), (5, red.level4)):
            @pl.when(hp >= lag)
            def _():
                level_q(level, hp - lag)
        return carry

    lax.fori_loop(0, PAIRS, pair, 0)
    for i in range(3):
        plain_copy(i, i).wait()
    red.level4(8, cols_of(8))
    done_t(jnp.int32(7))
    q_grad(jnp.int32(4))
    level_q(red.level2, 3)
    level_q(red.level3, 2)
    level_q(red.level4, 1)
    o_out[...] = red.level5(8, cols_of(8))
    done_q(0)
    q_grad(jnp.int32(5))
    level_q(red.level2, 4)
    level_q(red.level3, 3)
    level_q(red.level4, 2)
    done_q(1)
    for i in range(3):
        piece = dot_t(dqkv[i], wub[i].reshape(width, width))
        if i == 0:
            dh2[...] = piece
        else:
            dh2[...] += piece
    level_q(red.level2, 5)
    level_q(red.level3, 4)
    level_q(red.level4, 3)
    for half in halves:
        dy = dh2[half]
        unit, inv = normed(tok[half].astype(F32))
        acc[half] += norm_back(dy, unit, inv, vec[0:1])
        rows[0:1] += jnp.sum(dy * unit, axis=0, keepdims=True)
        rows[1:2] += jnp.sum(dy, axis=0, keepdims=True)
        rows[2:3] += jnp.sum(dqkv[0, half].astype(F32), axis=0, keepdims=True)
        rows[3:4] += jnp.sum(dqkv[2, half].astype(F32), axis=0, keepdims=True)
    for i, half in enumerate(halves):
        gtok[half] = jnp.where(table.turned, acc[halves[1 - i]], acc[half]).astype(BF)
    small = jnp.transpose(rows[...])
    lane = lax.broadcasted_iota(jnp.int32, small.shape, 1)
    tall = jnp.transpose(jnp.broadcast_to(gup[...], (8, 4 * chunk))).reshape(dp, 4, r, 8)
    for j in range(4):
        small = jnp.where(lane == 8 + j, tall[:, j].reshape(width, 8)[:, 0:1], small)
    g[:, :, :, :, held_small] = small.astype(BF).reshape(lines, 2, 2, r, 128)
    red.level1(last_t + 6, cols_small, held_small)
    level_q(red.level3, 5)
    red.level2(last_t + 6, cols_small, held_small)
    level_q(red.level4, 4)
    done_q(2)
    done_q(3)
    red.level3(last_t + 6, cols_small)
    level_q(red.level4, 5)
    red.level4(last_t + 6, cols_small)
    done_q(4)
    done_q(5)
    o_small[...] = red.level5(last_t + 6, cols_small)
    for p in range(last_t):
        red.finish(p, cols_of(p))
    for hp in range(PAIRS):
        red.finish(last_t + hp, cols_q(hp), hp >= 3, held_q(hp))
        kv_copy(hp).wait_send()
    red.finish(last_t + 6, cols_small, True, held_small)


def backward(tbl, tok, att, cot, q, kv, h1t, lse, vec, bup, wall, ctx):
    rows, width = tok.shape
    dp, r, full = wall.shape
    lines, nd = dp // 4, dp // 4
    chunk = 4 * nd * r
    V = pltpu.VMEM
    return pl.pallas_call(
        functools.partial(backward_kernel, dp, ctx),
        out_shape=(shape(rows, width), shape(rows, width), shape(r, 128, dtype=F32), shape(r, 3 * width, dtype=F32),
                   shape(r, width, dtype=F32), shape(r, 4 * chunk, dtype=F32), shape(4 * r, width, dtype=F32)),
        in_specs=[SM] + [VM] * 9 + [ANY], out_specs=(VM,) * 7,
        scratch_shapes=[V((rows, width), F32), V((rows, width), F32), V((rows, width), F32), V((rows, width), BF),
                        V((2, 16, BLK), F32),
                        V((2, BLK, LANES), BF), V((2 * ctx, BLK, LANES), F32), V((2 * ctx, BLK, LANES), F32),
                        V((PAIRS, rows, 2 * LANES), BF), V((PAIRS, rows, 2 * LANES), BF), V((3, rows, width), BF),
                        V((1, 4 * chunk), F32), V((128, width), F32),
                        V((3, dp, r, chunk), BF), V((2, nd, 4, r, width), BF),
                        V((lines, 2, 2, r, 9 * width + 128 + 9 * LANES), BF), V((lines, 2, r, full), BF), V((lines, r, full), BF),
                        V((lines - 1, r, full), BF), V((ctx - 1, r, full), BF),
                        DMA((6, 3)), DMA((PAIRS,)), DMA((PAIRS,)),
                        DMA((16,)), DMA((16,)), DMA((16,)), DMA((16,)), DMA((16, lines - 1)), DMA((16, lines - 1)),
                        DMA((16, ctx - 1)), DMA((16, ctx - 1))],
        compiler_params=pltpu.CompilerParams(vmem_limit_bytes=67043328, collective_id=3, has_side_effects=True),
        name="backward",
    )(tbl, tok, att, cot, q, kv, h1t, lse, vec, bup, wall)


def shards(tokens, block_table, ln1_gain, ln1_bias, w_qkv, bias_query, bias_value, w_out, bias_out,
           ln2_gain, ln2_bias, w_up, bias_up, w_down, bias_down, cotangent):
    dp, ctx = lax.axis_size("dp"), lax.axis_size("ctx")
    width, hidden = tokens.shape[2], w_up.shape[1]
    r = w_qkv.shape[0]
    head = 128 + 3 * width
    third = (width + 2 * hidden) // 3
    off_up = head + width
    off_down = off_up + hidden
    small = jnp.concatenate([jnp.stack([ln1_gain, ln1_bias, bias_query, bias_value, bias_out, ln2_gain, ln2_bias,
                                        bias_down]), bias_up.reshape(4, r), jnp.zeros((116, r), BF)]).T
    cat = jnp.concatenate([small, w_qkv, w_out, w_up] + [w_down[j * r:(j + 1) * r] for j in range(4)], axis=1)
    tok_all, wall = gather(tokens[0], cat, dp, ctx, head, third)
    fused = ctx == 2 and dp == 16
    *slots, h1, q, kv, att, lse, vec = attend(block_table, tok_all, wall, ctx, cotangent[0] if fused else None)
    bup = vec[8:12].reshape(4, dp, r).transpose(1, 0, 2).reshape(1, hidden)
    if fused:
        out, gtok, g_small, g_qkv, g_out, g_up, g_down = backward(
            block_table, slots[0], att, slots[1], q, kv, h1, lse, vec, bup, wall, ctx)
        rows = g_small.T
        return (out[None], gtok[None], rows[0], rows[1], g_qkv, rows[2], rows[3], g_out, rows[4], rows[5], rows[6],
                g_up, rows[8:12].reshape(4 * r), g_down, rows[7])
    out, gt, da, dx1, delta, gvec, gup = feed_call(block_table, tokens[0], att, wall, cotangent[0], vec, bup,
                                                   ctx, off_up, off_down, 3 * third)
    dq, dkv = attend_back(block_table, q, kv, da, lse, delta, ctx)
    gvec = gvec.at[8:12].set(gup.reshape(dp, 4, r).transpose(1, 0, 2).reshape(4, width))
    gq, gtok = last_call(block_table, dq, dkv, h1, tokens[0], wall, dx1, vec, gvec, ctx, head)
    total = scatter(gq, gt, dp, ctx, head, third)
    rows = total[:, 0:128].T
    g_down = jnp.concatenate([total[:, off_down + j * width:off_down + (j + 1) * width] for j in range(4)], axis=0)
    return (out[None], gtok[None], rows[0], rows[1], total[:, 128:head], rows[2], rows[3],
            total[:, head:off_up], rows[4], rows[5], rows[6], total[:, off_up:off_down],
            rows[8:12].reshape(4 * r), g_down, rows[7])


def solution(mesh):
    row, mat = P("dp"), P("dp", None)
    act = P("dp", "ctx", None)
    in_specs = (act, P(), row, row, mat, row, row, mat, row, row, row, mat, row, mat, row, act)
    out_specs = (act, act, row, row, mat, row, row, mat, row, row, row, mat, row, mat, row)
    return jax.shard_map(shards, mesh=mesh, in_specs=in_specs, out_specs=out_specs, check_vma=False)
```

```python
import functools
import jax
import jax.numpy as jnp
from jax import lax
from jax.experimental import pallas as pl
from jax.experimental.pallas import tpu as pltpu
from jax.sharding import PartitionSpec as P

ANY = pl.BlockSpec(memory_space=pl.ANY)
VM = pl.BlockSpec(memory_space=pltpu.VMEM)
HBM = pl.BlockSpec(memory_space=pltpu.HBM)
DMA = pltpu.SemaphoreType.DMA


def near_first(count):
    order = []
    for step in range(1, count):
        order.append((step + 1) // 2 if step % 2 else count - step // 2)
    return order


class Spot:
    def __init__(self, dp, ctx):
        self.dp, self.ctx = dp, ctx
        self.lines = dp // 4
        me = lax.axis_index("dp")
        self.y = lax.axis_index("ctx")
        self.z = me // 4
        self.x = (me // 2) % 2
        self.c = me % 2
        self.me = me

    def dp_at(self, z, x, c):
        return (z * 2 + x) * 2 + c

    def z_at(self, k):
        return lax.rem(self.z + k, self.lines)

    def y_at(self, k):
        return lax.rem(self.y + k, self.ctx)

    def barrier(self):
        sem = pltpu.get_barrier_semaphore()
        peers = [{"dp": self.dp_at(self.z_at(k), self.x, self.c)} for k in range(1, self.lines)]
        peers.append({"dp": self.dp_at(self.z, 1 - self.x, self.c)})
        peers.append({"dp": self.dp_at(self.z, self.x, 1 - self.c)})
        peers += [{"ctx": self.y_at(k)} for k in range(1, self.ctx)]
        for peer in peers:
            pl.semaphore_signal(sem, inc=1, device_id=peer, device_id_type=pl.DeviceIdType.MESH)
        pl.semaphore_wait(sem, len(peers))


def remote(src, dst, ssem, rsem, device):
    return pltpu.make_async_remote_copy(
        src_ref=src, dst_ref=dst, send_sem=ssem, recv_sem=rsem,
        device_id=device, device_id_type=pl.DeviceIdType.MESH,
    )


def gather_kernel(dp, ctx, head, third, tok_ref, cat_ref, tok_all, wall,
                  loc, st, rt, sz, rz, sx, rx, sy, ry, sc, rc):
    at = Spot(dp, ctx)
    lines = at.lines
    ky = at.y % 2
    mine = pl.multiple_of(head + third + ky * third, 128)
    other = pl.multiple_of(head + third + (1 - ky) * third, 128)
    cols = {"q": pl.ds(0, head), "m": pl.ds(mine, third), "t": pl.ds(head, third), "o": pl.ds(other, third)}
    num = {"q": 0, "m": 1, "t": 2, "o": 3}
    own = at.me
    mate = {"dp": at.dp_at(at.z, at.x, 1 - at.c)}
    across = {"dp": at.dp_at(at.z, 1 - at.x, at.c)}
    pair = {"ctx": at.y + 1 - 2 * ky}
    at.barrier()
    copies = []

    def go(copy):
        copy.start()
        copies.append(copy)

    local = [pltpu.make_async_copy(cat_ref, wall.at[own], loc.at[0]),
             pltpu.make_async_copy(tok_ref, tok_all.at[at.y], loc.at[1])]
    for copy in local:
        copy.start()

    def block(b, z, x, c):
        return wall.at[at.dp_at(z, x, c), :, cols[b]]

    def own_block(b):
        return cat_ref.at[:, cols[b]]

    def send_z(b):
        for k in near_first(lines):
            go(remote(own_block(b), block(b, at.z, at.x, at.c), sz.at[num[b], k], rz.at[num[b], at.z],
                      {"dp": at.dp_at(at.z_at(k), at.x, at.c)}))

    def send_x(b, z, k, src):
        go(remote(src, block(b, z, at.x, at.c), sx.at[num[b], k], rx.at[num[b], z], across))

    def send_c(b, z, x, k, kx, src):
        go(remote(src, block(b, z, x, at.c), sc.at[num[b], k, kx], rc.at[num[b], z, x], mate))

    def send_y(z, x, k, kx, src):
        go(remote(src, block("m", z, x, at.c), sy.at[k, kx], ry.at[z, x], pair))

    def got_z(b, k):
        z = at.z_at(k)
        remote(own_block(b), block(b, z, at.x, at.c), sz.at[num[b], 0], rz.at[num[b], z], across).wait_recv()

    def got_x(b, k):
        z = at.z_at(k)
        remote(own_block(b), block(b, z, 1 - at.x, at.c), sz.at[num[b], 0], rx.at[num[b], z], across).wait_recv()

    def got_y(k, kx):
        z, x = at.z_at(k), (at.x + kx) % 2
        remote(own_block("o"), block("o", z, x, at.c), sz.at[0, 0], ry.at[z, x], across).wait_recv()

    def got_c(b, k, kx):
        z, x = at.z_at(k), (at.x + kx) % 2
        remote(own_block(b), block(b, z, x, 1 - at.c), sz.at[0, 0], rc.at[num[b], z, x], across).wait_recv()

    order = [0] + near_first(lines)
    for k in range(1, ctx):
        go(remote(tok_ref, tok_all.at[at.y], st.at[k], rt.at[at.y], {"ctx": at.y_at(k)}))
    for b in ("q", "m", "t"):
        send_z(b)
    for b in ("q", "m", "t"):
        send_x(b, at.z, 0, own_block(b))
        send_c(b, at.z, at.x, 0, 0, own_block(b))
        for k in order[1:]:
            got_z(b, k)
            z = at.z_at(k)
            src = block(b, z, at.x, at.c)
            send_x(b, z, k, src)
            if b == "m":
                send_y(z, at.x, k, 0, src)
            send_c(b, z, at.x, k, 0, src)
        for k in order:
            got_x(b, k)
            z = at.z_at(k)
            src = block(b, z, 1 - at.x, at.c)
            if b == "m":
                send_y(z, 1 - at.x, k, 1, src)
            send_c(b, z, 1 - at.x, k, 1, src)
    send_c("o", at.z, at.x, 0, 0, own_block("o"))
    for kx in range(2):
        for k in order:
            if k == 0 and kx == 0:
                continue
            got_y(k, kx)
            z, x = at.z_at(k), (at.x + kx) % 2
            send_c("o", z, x, k, kx, block("o", z, x, at.c))
    for b in ("q", "m", "t", "o"):
        for kx in range(2):
            for k in order:
                got_c(b, k, kx)
    for k in range(1, ctx):
        y = at.y_at(k)
        remote(tok_ref, tok_all.at[y], st.at[0], rt.at[y], across).wait_recv()
    for copy in copies:
        copy.wait_send()
    for copy in local:
        copy.wait()


def gather(tok, cat, dp, ctx, head, third):
    lines = dp // 4
    rows, width = cat.shape
    return pl.pallas_call(
        functools.partial(gather_kernel, dp, ctx, head, third),
        out_shape=(jax.ShapeDtypeStruct((ctx, *tok.shape), tok.dtype),
                   jax.ShapeDtypeStruct((dp, rows, width), cat.dtype)),
        in_specs=[VM, VM], out_specs=(ANY, ANY),
        scratch_shapes=[DMA((2,)), DMA((ctx,)), DMA((ctx,)),
                        DMA((3, lines)), DMA((3, lines)), DMA((3, lines)), DMA((3, lines)),
                        DMA((lines, 2)), DMA((lines, 2)), DMA((4, lines, 2)), DMA((4, lines, 2))],
        compiler_params=pltpu.CompilerParams(collective_id=0, has_side_effects=True, vmem_limit_bytes=32 * 2**20),
    )(tok, cat)


def scatter_kernel(dp, ctx, head, third, gq, gt, out, a_core, a_pair, a_x, a_z, a_y, stage, total,
                   loc, s1, r1, s2, r2, s3, r3, s4, r4, s5, r5):
    at = Spot(dp, ctx)
    lines = at.lines
    rows = gq.shape[1]
    ky = at.y % 2
    mine = pl.multiple_of(head + third + ky * third, 128)
    other = pl.multiple_of(head + third + (1 - ky) * third, 128)
    cols = {"q": pl.ds(0, head), "m": pl.ds(mine, third), "t": pl.ds(head, third), "o": pl.ds(other, third)}
    size = {"q": head, "m": third, "t": third, "o": third}
    num = {"q": 0, "m": 1, "t": 2, "o": 3}
    mate = {"dp": at.dp_at(at.z, at.x, 1 - at.c)}
    across = {"dp": at.dp_at(at.z, 1 - at.x, at.c)}
    pair = {"ctx": at.y + 1 - 2 * ky}
    at.barrier()
    copies = []

    def go(copy):
        copy.start()
        copies.append(copy)

    first = {"m": pl.multiple_of(third + ky * third, 128), "o": pl.multiple_of(third + (1 - ky) * third, 128), "t": 0}

    def full(b, at_dp):
        if b == "q":
            return gq.at[at_dp]
        return gt.at[at_dp, :, pl.ds(first[b], third)]

    order = [0] + near_first(lines)
    order = order[::-1]
    spots = [(k, kx) for kx in (1, 0) for k in order]

    def where(k, kx):
        return at.z_at(k), (at.x + kx) % 2

    def land(ref, b, *idx):
        return ref.at[(num[b], *idx, slice(None), pl.ds(0, size[b]))]

    blocks = ("o", "m", "t", "q")
    for b in blocks:
        for k, kx in spots:
            z, x = where(k, kx)
            go(remote(full(b, at.dp_at(z, x, 1 - at.c)), land(a_core, b, z, x),
                      s1.at[num[b], k, kx], r1.at[num[b], z, x], mate))
    def fetch(b, k, kx):
        z, x = where(k, kx)
        return pltpu.make_async_copy(full(b, at.dp_at(z, x, at.c)), land(stage, b, z, x),
                                     loc.at[num[b], k, kx])
    for b in blocks:
        for k, kx in spots:
            fetch(b, k, kx).start()

    def take(sem, dst):
        remote(dst, dst, s1.at[0, 0, 0], sem, across).wait_recv()

    def added(b, k, kx):
        z, x = where(k, kx)
        fetch(b, k, kx).wait()
        here = land(a_core, b, z, x)
        take(r1.at[num[b], z, x], here)
        here[...] = here[...] + land(stage, b, z, x)[...]
        return here

    for b in blocks:
        if b == "o":
            for k, kx in spots:
                z, x = where(k, kx)
                go(remote(added(b, k, kx), a_pair.at[z, x], s2.at[k, kx], r2.at[z, x], pair))
            continue
        for k, kx in spots:
            z, x = where(k, kx)
            here = added(b, k, kx)
            if b == "m":
                take(r2.at[z, x], a_pair.at[z, x])
                here[...] = here[...] + a_pair[z, x]
            if kx == 1:
                go(remote(here, land(a_x, b, z), s3.at[num[b], k], r3.at[num[b], z], across))
        for k in order:
            z = at.z_at(k)
            here = land(a_core, b, z, at.x)
            take(r3.at[num[b], z], land(a_x, b, z))
            here[...] = here[...] + land(a_x, b, z)[...]
            if k:
                go(remote(here, land(a_z, b, at.z), s4.at[num[b], k], r4.at[num[b], at.z],
                          {"dp": at.dp_at(z, at.x, at.c)}))
    for b in ("m", "t", "q"):
        acc = land(a_core, b, at.z, at.x)[...].astype(jnp.float32)
        for k in near_first(lines):
            z = at.z_at(k)
            take(r4.at[num[b], z], land(a_z, b, z))
            acc = acc + land(a_z, b, z)[...].astype(jnp.float32)
        land(total, b)[...] = acc
        land(a_core, b, at.z, at.x)[...] = acc.astype(jnp.bfloat16)
        for k in range(1, ctx):
            go(remote(land(a_core, b, at.z, at.x), land(a_y, b, at.y), s5.at[num[b], k], r5.at[num[b], at.y],
                      {"ctx": at.y_at(k)}))
    outs = []
    for b in ("t", "q", "m", "o"):
        if b == "m":
            acc = land(total, b)[...]
        elif b == "o":
            acc = jnp.zeros((rows, third), jnp.float32)
        else:
            acc = land(total, b)[...]
        for k in range(1, ctx):
            y = at.y_at(k)
            if b in ("t", "q") or (b == "m" and k % 2 == 0):
                take(r5.at[num[b], y], land(a_y, b, y))
                acc = acc + land(a_y, b, y)[...].astype(jnp.float32)
            elif b == "o" and k % 2 == 1:
                here = a_y.at[1, y, :, pl.ds(0, third)]
                take(r5.at[1, y], here)
                acc = acc + here[...].astype(jnp.float32)
        land(total, b)[...] = acc
        copy = pltpu.make_async_copy(land(total, b), out.at[:, cols[b]], loc.at[num[b], 0, 0])
        copy.start()
        outs.append(copy)
    for copy in copies:
        copy.wait_send()
    for copy in outs:
        copy.wait()


def scatter(gq, gt, dp, ctx, head, third):
    lines = dp // 4
    _, rows, width = gq.shape[0], gq.shape[1], gq.shape[2] + gt.shape[2]
    bf, f32 = jnp.bfloat16, jnp.float32
    return pl.pallas_call(
        functools.partial(scatter_kernel, dp, ctx, head, third),
        out_shape=jax.ShapeDtypeStruct((rows, width), f32),
        in_specs=[ANY, ANY], out_specs=ANY,
        scratch_shapes=[pltpu.VMEM((4, lines, 2, rows, head), bf), pltpu.VMEM((lines, 2, rows, third), bf),
                        pltpu.VMEM((3, lines, rows, head), bf), pltpu.VMEM((3, lines, rows, head), bf),
                        pltpu.VMEM((3, ctx, rows, head), bf), pltpu.VMEM((4, lines, 2, rows, head), bf),
                        pltpu.VMEM((4, rows, head), f32),
                        DMA((4, lines, 2)), DMA((4, lines, 2)), DMA((4, lines, 2)),
                        DMA((lines, 2)), DMA((lines, 2)),
                        DMA((3, lines)), DMA((3, lines)), DMA((3, lines)), DMA((3, lines)),
                        DMA((3, ctx)), DMA((3, ctx))],
        compiler_params=pltpu.CompilerParams(collective_id=1, has_side_effects=True, vmem_limit_bytes=60 * 2**20),
    )(gq, gt)


F32, BF = jnp.float32, jnp.bfloat16
HEADS, HD, BLK = 12, 64, 256
PAIRS, LANES = HEADS // 2, 2 * HD


def dot(a, b):
    return jnp.dot(a, b, preferred_element_type=F32)


def dot_t(a, b):
    return lax.dot_general(a, b, (((1,), (1,)), ((), ())), preferred_element_type=F32)


def dot_l(a, b):
    return lax.dot_general(a, b, (((0,), (0,)), ((), ())), preferred_element_type=F32)


def normed(x):
    centred = x - jnp.mean(x, axis=-1, keepdims=True)
    inv = lax.rsqrt(jnp.mean(centred * centred, axis=-1, keepdims=True) + 1e-05)
    return centred * inv, inv


def norm_back(dy, unit, inv, gain):
    dn = dy * gain
    return inv * (dn - jnp.mean(dn, axis=-1, keepdims=True) - unit * jnp.mean(dn * unit, axis=-1, keepdims=True))


class Table:
    def __init__(self, tbl, nb, y, ordered=False):
        self.nb, self.half = nb, nb // 2
        self.own = [tbl[2 * y], tbl[2 * y + 1]]
        self.turned = self.own[0] >= self.half
        first_high = self.turned.astype(jnp.int32)
        self.place = [first_high, 1 - first_high]
        self.row_of = [first_high, 1 - first_high]
        self.slot_of = [first_high, 1 - first_high]
        self.block = [jnp.minimum(self.own[0], self.own[1]), jnp.maximum(self.own[0], self.own[1])]
        self.tbl = tbl
        if ordered:
            self.row_of, self.slot_of, self.pos = [0, 1], [0, 1], list(range(nb))
            return
        self.pos = []
        for j in range(nb):
            at = jnp.int32(0)
            for p in range(nb):
                at = at + jnp.where(tbl[p] == j, p, 0)
            self.pos.append(at)

    def keys(self, slot):
        return self.half if slot == 0 else self.nb

    def masked(self, slot, j):
        return j >= 1 if slot == 0 else j > self.half


def rows_of(ref, *idx):
    value = ref[idx]
    return value.reshape(value.shape[0] * value.shape[1], value.shape[2])


def block_rows(i):
    return pl.ds(i * BLK if isinstance(i, int) else pl.multiple_of(i * BLK, BLK), BLK)


def lane_masks(rows):
    lane = lax.broadcasted_iota(jnp.int32, (rows, LANES), 1)
    return [lane < HD, lane >= HD]


def project(ctx, tok, wall, h1, q, kv, vec, y):
    gain, shift = vec[0:1], vec[1:2]
    width = tok.shape[2]
    zero = jnp.zeros((1, width), F32)
    kv_bias = jnp.concatenate([zero, vec[3:4]], axis=1)
    w_kv = rows_of(wall, slice(None), slice(None), slice(128 + width, 128 + 3 * width))

    def rows(r, carry):
        x = tok[r // 2, pl.ds(pl.multiple_of((r % 2) * BLK, BLK), BLK)].astype(F32)
        low = (normed(x)[0] * gain + shift).astype(BF)
        kv[pl.ds(pl.multiple_of(r * BLK, BLK), BLK)] = (dot(low, w_kv) + kv_bias).astype(BF)
        return carry

    lax.fori_loop(0, 2 * ctx, rows, 0)
    w_q = rows_of(wall, slice(None), slice(None), slice(128, 128 + width))

    def own(i, carry):
        at = pl.ds(pl.multiple_of(i * BLK, BLK), BLK)
        low = (normed(tok[y, at].astype(F32))[0] * gain + shift).astype(BF)
        h1[at] = low
        q[at] = ((dot(low, w_q) + vec[2:3]).astype(BF).astype(F32) * HD ** (-0.5)).astype(BF)
        return carry

    lax.fori_loop(0, 2, own, 0)


def attend_pair(hp, table, q, kv, att, lse_acc, width):
    lanes = pl.ds(pl.multiple_of(hp * LANES, LANES), LANES)
    v_lanes = pl.ds(pl.multiple_of(width + hp * LANES, LANES), LANES)
    masks = lane_masks(BLK)
    lane = lax.broadcasted_iota(jnp.int32, (BLK, LANES), 1)
    for slot in range(2):
        q2 = q[block_rows(table.row_of[slot]), lanes]
        spots = [block_rows(table.pos[j]) for j in range(table.keys(slot))]
        mixed = []
        for h in range(2):
            qm = jnp.where(masks[h], q2, jnp.zeros_like(q2))
            scores = []
            for j, at in enumerate(spots):
                s = dot_t(qm, kv[at, lanes])
                if table.masked(slot, j):
                    s = jnp.where(j <= table.block[slot], s, -1e30)
                scores.append(s)
            largest = functools.reduce(jnp.maximum, scores)
            largest = jnp.max(largest, axis=-1, keepdims=True)
            exps = [jnp.exp(s - largest) for s in scores]
            total = jnp.sum(functools.reduce(jnp.add, exps), axis=-1, keepdims=True)
            out = functools.reduce(jnp.add, [dot(e.astype(BF), kv[at, v_lanes]) for e, at in zip(exps, spots)])
            mixed.append(out / total)
            lse_acc[slot] = jnp.where(lane == 2 * hp + h, largest + jnp.log(total), lse_acc[slot])
        att[slot, :, lanes] = jnp.where(masks[0], mixed[0], mixed[1]).astype(BF)


def attend_back_pair(hp, table, q, kv, da, lse, delta, put_dq, dk_acc, dv_acc, width):
    lanes = pl.ds(pl.multiple_of(hp * LANES, LANES), LANES)
    v_lanes = pl.ds(pl.multiple_of(width + hp * LANES, LANES), LANES)
    masks = lane_masks(BLK)
    for slot in (1, 0):
        row = block_rows(table.row_of[slot])
        q2, da2 = q[row, lanes], da[row, lanes]
        dq_acc = None
        for h in range(2):
            qm = jnp.where(masks[h], q2, jnp.zeros_like(q2))
            dam = jnp.where(masks[h], da2, jnp.zeros_like(da2))
            lse_row = lse[slot, pl.ds(2 * hp + h, 1), :]
            delta_row = delta[table.row_of[slot], pl.ds(2 * hp + h, 1), :]
            for j in range(table.keys(slot)):
                at = block_rows(table.pos[j])
                k2, v2 = kv[at, lanes], kv[at, v_lanes]
                st = dot_t(k2, qm)
                if table.masked(slot, j):
                    st = jnp.where(j <= table.block[slot], st, -1e30)
                pt = jnp.exp(st - lse_row)
                dst = (pt * (dot_t(v2, dam) - delta_row)).astype(BF)
                dv, dk = dot(pt.astype(BF), dam), dot(dst, qm)
                if slot == 1 and h == 0:
                    dv_acc[j], dk_acc[j] = dv, dk
                else:
                    dv_acc[j] += dv
                    dk_acc[j] += dk
                part = dot_l(dst, jnp.where(masks[h], k2, jnp.zeros_like(k2)))
                dq_acc = part if dq_acc is None else dq_acc + part
        put_dq(slot, (dq_acc * HD ** (-0.5)).astype(BF))


def feed(nd, off_up, off_down, table, tok, att, wall, cot, vec, bup, out, gt, da, dx1, delta, gvec, gup,
         x1, h2, acc, dh2):
    rows, width = cot.shape
    dp, r = wall.shape[0], wall.shape[1]
    chunk = 4 * nd * r
    w_out = rows_of(wall, slice(None), slice(None), slice(off_up - width, off_up))
    for i in range(2):
        at = pl.ds(i * BLK, BLK)
        mid = tok[at].astype(F32) + (dot(att[table.slot_of[i]], w_out) + vec[4:5])
        x1[at] = mid
        h2[at] = (normed(mid)[0] * vec[5:6] + vec[6:7]).astype(BF)
        acc[at] = mid + vec[7:8]
    dh2[...] = jnp.zeros_like(dh2)
    g = cot[...]

    def part(f, carry):
        cols = pl.ds(pl.multiple_of(off_up + f * chunk, 128), chunk)
        w_up = rows_of(wall, slice(None), slice(None), cols)
        w_down = jnp.concatenate(
            [wall[f * nd + d, :, pl.ds(off_down + j * width, width)] for d in range(nd) for j in range(4)], axis=0)
        low = h2[...]
        u = dot(low, w_up) + bup[:, pl.ds(pl.multiple_of(f * chunk, 128), chunk)]
        sq = u * u
        t = jnp.tanh(u * (0.7978845608028654 + 0.03567740813636141 * sq))
        act = (0.5 * u * (1.0 + t)).astype(BF)
        slope = 0.5 * (1.0 + t) + 0.5 * u * (1.0 - t * t) * (0.7978845608028654 + 0.10703222440908423 * sq)
        acc[...] += dot(act, w_down)
        du = slope * dot_t(g, w_down)
        dul = du.astype(BF)
        gup[:, pl.ds(pl.multiple_of(f * chunk, 128), chunk)] = jnp.sum(dul.astype(F32), axis=0, keepdims=True)
        dh2[...] += dot_t(dul, w_up)
        g_up = dot_l(low, dul).astype(BF)
        gt[:, :, pl.ds(pl.multiple_of(width + f * chunk, 128), chunk)] = g_up.reshape(dp, r, chunk)
        g_down = dot_l(act, g).astype(BF)
        for d in range(nd):
            for j in range(4):
                piece = g_down[(4 * d + j) * r:(4 * d + j + 1) * r]
                gt[f * nd + d, :, pl.ds(width + off_down - off_up + j * width, width)] = piece
        return carry

    lax.fori_loop(0, dp // nd, part, 0)
    out[...] = acc[...].astype(BF)
    gf = g.astype(F32)
    unit, inv = normed(x1[...])
    dy = dh2[...]
    mid_grad = gf + norm_back(dy, unit, inv, vec[5:6])
    dx1[...] = mid_grad
    branch = mid_grad.astype(BF)
    gvec[...] = jnp.zeros_like(gvec)
    gvec[4:5] = jnp.sum(branch.astype(F32), axis=0, keepdims=True)
    gvec[5:6] = jnp.sum(dy * unit, axis=0, keepdims=True)
    gvec[6:7] = jnp.sum(dy, axis=0, keepdims=True)
    gvec[7:8] = jnp.sum(gf, axis=0, keepdims=True)
    head = lax.broadcasted_iota(jnp.int32, (16, width), 0)
    pick = (lax.broadcasted_iota(jnp.int32, (16, width), 1) // HD == head).astype(F32)
    grad = None
    for i in range(2):
        own = att[table.slot_of[i]]
        low = branch[i * BLK:(i + 1) * BLK]
        piece = dot_l(own, low)
        grad = piece if grad is None else grad + piece
        back = dot_t(low, w_out).astype(BF)
        da[pl.ds(i * BLK, BLK)] = back
        prod = back.astype(F32) * own.astype(F32)
        delta[i] = lax.dot_general(pick, prod, (((1,), (1,)), ((), ())), precision=lax.Precision.HIGHEST,
                                   preferred_element_type=F32)
    gt[:, :, 0:width] = grad.astype(BF).reshape(dp, r, width)


def last(ctx, table, y, dq, own_kv, h1, tok, wall, dx1, vec, gvec, gq, gtok):
    width = h1.shape[1]
    dp, r = wall.shape[0], wall.shape[1]
    w_q = rows_of(wall, slice(None), slice(None), slice(128, 128 + width))
    low = h1[...]
    dq_all = jnp.concatenate([dq[table.slot_of[0]], dq[table.slot_of[1]]], axis=0)
    gq[:, :, 128:128 + width] = dot_l(low, dq_all).astype(BF).reshape(dp, r, width)
    dh1 = dot_t(dq_all, w_q)
    dkv = own_kv()
    w_kv = rows_of(wall, slice(None), slice(None), slice(128 + width, 128 + 3 * width))
    gq[:, :, 128 + width:128 + 3 * width] = dot_l(low, dkv).astype(BF).reshape(dp, r, 2 * width)
    dh1 = dh1 + dot_t(dkv, w_kv)
    unit, inv = normed(tok[...].astype(F32))
    gtok[...] = (dx1[...] + norm_back(dh1, unit, inv, vec[0:1])).astype(BF)
    sums = [jnp.sum(dh1 * unit, axis=0, keepdims=True), jnp.sum(dh1, axis=0, keepdims=True),
            jnp.sum(dq_all.astype(F32), axis=0, keepdims=True),
            jnp.sum(dkv[:, width:].astype(F32), axis=0, keepdims=True)]
    table_rows = jnp.concatenate(sums + [gvec[4:16], jnp.zeros((112, width), F32)], axis=0)
    gq[:, :, 0:128] = jnp.transpose(table_rows).astype(BF).reshape(dp, r, 128)


SM = pl.BlockSpec(memory_space=pltpu.SMEM)


def params(limit, **more):
    return pltpu.CompilerParams(vmem_limit_bytes=limit * 2**20, **more)


def shape(*dims, dtype=BF):
    return jax.ShapeDtypeStruct(dims, dtype)


def attend_kernel(ctx, tbl, tok, wall, h1, q, kv, att, lse, vec, lse_acc):
    width = tok.shape[2]
    y = lax.axis_index("ctx")
    table = Table(tbl, 2 * ctx, y)
    small = rows_of(wall, slice(None), slice(None), slice(0, 128)).astype(F32)
    vec[...] = jnp.transpose(small)[0:16]
    project(ctx, tok, wall, h1, q, kv, vec, y)
    lse_acc[...] = jnp.zeros_like(lse_acc)

    def pair(hp, carry):
        attend_pair(hp, table, q, kv, att, lse_acc, width)
        return carry

    lax.fori_loop(0, PAIRS, pair, 0)
    for slot in range(2):
        lse[slot] = jnp.transpose(lse_acc[slot])[0:16]


def attend(tbl, tok_all, wall, ctx):
    rows, width = tok_all.shape[1:]
    return pl.pallas_call(
        functools.partial(attend_kernel, ctx),
        out_shape=(shape(rows, width), shape(rows, width), shape(ctx * rows, 2 * width), shape(2, BLK, width),
                   shape(2, 16, BLK, dtype=F32), shape(16, width, dtype=F32)),
        in_specs=[SM, VM, VM], out_specs=(VM,) * 6,
        scratch_shapes=[pltpu.VMEM((2, BLK, LANES), F32)],
        compiler_params=params(62), name="attend",
    )(tbl, tok_all, wall)


def front_kernel(dp, ctx, tbl, tok, cot, *rest):
    vectors, rest = rest[:8], rest[8:]
    (b_up, w_qkv, w_out, w_up, w_down,
     wall, tok_slots, cot_slots, h1, q, kv, att, lse, vec,
     cat, small, toks, wq, lse_acc, loc, st, rt, sz, rz, sx, rx, sy, ry, sc, rc) = rest
    at = Spot(dp, ctx)
    lines = at.lines
    r, full = cat.shape
    width = tok.shape[1]
    head = 128 + 3 * width
    size = (full - head) // 6
    ky = at.y
    mate = {"dp": at.dp_at(at.z, at.x, 1 - at.c)}
    across = {"dp": at.dp_at(at.z, 1 - at.x, at.c)}
    pair_y = {"ctx": 1 - ky}
    table = Table(tbl, 2 * ctx, at.y, True)
    order = [0] + near_first(lines)

    small[...] = jnp.zeros_like(small)
    for i, ref in enumerate(vectors):
        small[i:i + 1, 0:r] = ref[...].astype(F32).reshape(1, r)
    small[8:12, 0:r] = b_up[...].astype(F32)
    cat[:, 0:128] = jnp.transpose(small[...])[0:r].astype(BF)
    cat[:, 128:head] = w_qkv[...]
    cat[:, head:head + width] = w_out[...]
    cat[:, head + width:head + 5 * width] = w_up[...]
    for j in range(4):
        cat[:, head + (5 + j) * width:head + (6 + j) * width] = w_down[j * r:(j + 1) * r]
    at.barrier()

    def cols(p):
        if isinstance(p, int) and p >= 5:
            place = 2 * (p - 4) + 1 - ky
        else:
            n = p - 1
            place = (1 - n % 2) * (2 + 2 * (n // 2) + ky) + (n % 2) * (n // 2)
        return pl.ds(pl.multiple_of(head + place * size, 128), size)

    def is_head(p):
        return isinstance(p, int) and p == 0

    def own_block(p):
        return cat.at[:, pl.ds(0, head)] if is_head(p) else cat.at[:, cols(p)]

    def block(p, z, x, c):
        return wq.at[at.dp_at(z, x, c)] if is_head(p) else wall.at[at.dp_at(z, x, c), :, cols(p)]

    def to_z(p, k):
        return remote(own_block(p), block(p, at.z, at.x, at.c), sz.at[p, k], rz.at[p, at.z],
                      {"dp": at.dp_at(at.z_at(k), at.x, at.c)})

    def to_x(p, k):
        z = at.z_at(k)
        src = own_block(p) if k == 0 else block(p, z, at.x, at.c)
        return remote(src, block(p, z, at.x, at.c), sx.at[p, k], rx.at[p, z], across)

    def to_c(p, k, kx):
        z, x = at.z_at(k), (at.x + kx) % 2
        src = own_block(p) if k == 0 and kx == 0 else block(p, z, x, at.c)
        return remote(src, block(p, z, x, at.c), sc.at[p, k, kx], rc.at[p, z, x], mate)

    def to_y(p, k, kx):
        z, x = at.z_at(k), (at.x + kx) % 2
        n = (p - 1) // 2
        here = block(p, z, x, at.c)
        return remote(here, here, sy.at[n, k, kx], ry.at[n, z, x], pair_y)

    def got(p, z, x, c, sem):
        here = block(p, z, x, c)
        remote(here, here, st, sem, across).wait_recv()

    def stage_z(p, shared):
        for k in order:
            if k:
                got(p, at.z_at(k), at.x, at.c, rz.at[p, at.z_at(k)])
                to_x(p, k).start()
                if shared is not None:
                    pl.when(shared)(lambda: to_y(p, k, 0).start())
                to_c(p, k, 0).start()

    def stage_x(p, shared):
        for k in order:
            got(p, at.z_at(k), 1 - at.x, at.c, rx.at[p, at.z_at(k)])
            if shared is not None:
                pl.when(shared)(lambda: to_y(p, k, 1).start())
            to_c(p, k, 1).start()

    def stage_y(n):
        p = 5 + n
        for kx in range(2):
            for k in order:
                if k or kx:
                    z, x = at.z_at(k), (at.x + kx) % 2
                    got(p, z, x, at.c, ry.at[n, z, x])
                    to_c(p, k, kx).start()

    def stage_c(p):
        for kx in range(2):
            for k in order:
                z, x = at.z_at(k), (at.x + kx) % 2
                got(p, z, x, 1 - at.c, rc.at[p, z, x])

    tok_mate = remote(tok, toks.at[at.y], st, rt, pair_y)
    tok_own = pltpu.make_async_copy(tok, toks.at[at.y], loc.at[0])
    wall_own = pltpu.make_async_copy(cat.at[:, pl.ds(head, full - head)],
                                     wall.at[at.me, :, pl.ds(head, full - head)], loc.at[1])
    head_own = pltpu.make_async_copy(cat.at[:, pl.ds(0, head)], wq.at[at.me], loc.at[2])
    to_x(0, 0).start()
    for k in near_first(lines):
        to_z(0, k).start()
    to_c(0, 0, 0).start()
    tok_mate.start()
    for copy in (tok_own, head_own, wall_own):
        copy.start()
    for p in range(1, 5):
        for k in near_first(lines):
            to_z(p, k).start()
        to_x(p, 0).start()
    for p in range(1, 7):
        to_c(p, 0, 0).start()
    stage_z(0, None)
    stage_x(0, None)
    stage_c(0)
    head_own.wait()
    head_all = pltpu.make_async_copy(wq, wall.at[:, :, pl.ds(0, head)], loc.at[2])
    head_all.start()
    tok_own.wait()
    tok_mate.wait_recv()

    columns = jnp.transpose(rows_of(wq, slice(None), slice(None), slice(0, 128)).astype(F32))
    vec[...] = columns[0:16]
    gain, shift = vec[0:1], vec[1:2]
    kv_bias = jnp.concatenate([jnp.zeros((1, width), F32), vec[3:4]], axis=1)

    def stored(i):
        return toks[i // 2, block_rows(i % 2)].astype(F32)

    for j in range(2 * ctx):
        here = stored(0)
        for i in range(1, 2 * ctx):
            here = jnp.where(tbl[i] == j, stored(i), here)
        low = (normed(here)[0] * gain + shift).astype(BF)
        kv[block_rows(j)] = (dot(low, rows_of(wq, slice(None), slice(None), slice(128 + width, head)))
                             + kv_bias).astype(BF)
    for i in range(2):
        def chosen(ref):
            a, b = ref[block_rows(i)].astype(F32), ref[block_rows(1 - i)].astype(F32)
            return jnp.where(table.turned, b, a)

        here = chosen(tok)
        low = (normed(here)[0] * gain + shift).astype(BF)
        h1[:, block_rows(i)] = jnp.transpose(low)
        w_q = rows_of(wq, slice(None), slice(None), slice(128, 128 + width))
        q[block_rows(i)] = ((dot(low, w_q) + vec[2:3]).astype(BF).astype(F32) * HD ** (-0.5)).astype(BF)
        tok_slots[block_rows(i)] = here.astype(BF)
        cot_slots[block_rows(i)] = chosen(cot).astype(BF)
    lse_acc[...] = jnp.zeros_like(lse_acc)

    def heads(hp, carry):
        attend_pair(hp, table, q, kv, att, lse_acc, width)
        return carry

    def stages(t, carry):
        @pl.when(t < 4)
        def _():
            stage_z(t + 1, t % 2 == 0)

        @pl.when(t >= 1)
        def _():
            stage_x(t, t % 2 == 1)

        lax.fori_loop(jnp.minimum(2 * t, PAIRS), jnp.minimum(2 * t + 2, PAIRS), heads, 0)
        return carry

    lax.fori_loop(0, 5, stages, 0)
    for slot in range(2):
        lse[slot] = jnp.transpose(lse_acc[slot])[0:16]
    stage_y(0)
    stage_y(1)
    for p in range(1, 7):
        stage_c(p)
    for p in range(5):
        for k in order:
            to_x(p, k).wait_send()
            if k:
                to_z(p, k).wait_send()
    for p in range(7):
        for kx in range(2):
            for k in order:
                to_c(p, k, kx).wait_send()
                if p in (1, 3) and (k or kx):
                    to_y(p, k, kx).wait_send()
    tok_mate.wait_send()
    wall_own.wait()
    head_all.wait()


def front(tbl, tok, cot, vectors, b_up, weights, dp, ctx):
    rows, width = tok.shape
    r = weights[0].shape[0]
    head = 128 + 3 * width
    full = head + 9 * width
    lines = dp // 4
    V = pltpu.VMEM
    return pl.pallas_call(
        functools.partial(front_kernel, dp, ctx),
        out_shape=(shape(dp, r, full), shape(rows, width), shape(rows, width), shape(width, rows), shape(rows, width),
                   shape(ctx * rows, 2 * width), shape(2, BLK, width), shape(2, 16, BLK, dtype=F32),
                   shape(16, width, dtype=F32)),
        in_specs=[SM] + [VM] * (2 + len(vectors) + 1 + len(weights)), out_specs=(ANY,) + (VM,) * 8,
        scratch_shapes=[V((r, full), BF), V((128, 128), F32), V((ctx, rows, width), BF), V((dp, r, head), BF),
                        V((2, BLK, LANES), F32), DMA((3,)), DMA, DMA,
                        DMA((5, lines)), DMA((5, lines)), DMA((5, lines)), DMA((5, lines)),
                        DMA((2, lines, 2)), DMA((2, lines, 2)), DMA((7, lines, 2)), DMA((7, lines, 2))],
        compiler_params=params(62, collective_id=0, has_side_effects=True), name="front",
    )(tbl, tok, cot, *vectors, b_up, *weights)


def feed_kernel(ctx, nd, off_up, off_down, tbl, tok, att, wall, cot, vec, bup, *rest):
    table = Table(tbl, 2 * ctx, lax.axis_index("ctx"))
    feed(nd, off_up, off_down, table, tok, att, wall, cot, vec, bup, *rest)


def feed_call(tbl, tok, att, wall, cot, vec, bup, ctx, off_up, off_down, gt_cols):
    rows, width = cot.shape
    dp, r = wall.shape[:2]
    return pl.pallas_call(
        functools.partial(feed_kernel, ctx, dp // 4, off_up, off_down),
        out_shape=(shape(rows, width), shape(dp, r, gt_cols), shape(rows, width), shape(rows, width, dtype=F32),
                   shape(2, 16, BLK, dtype=F32), shape(16, width, dtype=F32), shape(1, bup.shape[1], dtype=F32)),
        in_specs=[SM] + [VM] * 6, out_specs=(VM,) * 7,
        scratch_shapes=[pltpu.VMEM((rows, width), F32), pltpu.VMEM((rows, width), BF),
                        pltpu.VMEM((rows, width), F32), pltpu.VMEM((rows, width), F32)],
        compiler_params=params(62), name="feed",
    )(tbl, tok, att, wall, cot, vec, bup)


def attend_back_kernel(ctx, tbl, q, kv, da, lse, delta, dq, dkv, dk_acc, dv_acc):
    width = q.shape[1]
    table = Table(tbl, 2 * ctx, lax.axis_index("ctx"))

    def pair(hp, carry):
        def put_dq(slot, value):
            dq[slot, :, pl.ds(pl.multiple_of(hp * LANES, LANES), LANES)] = value

        attend_back_pair(hp, table, q, kv, da, lse, delta, put_dq, dk_acc, dv_acc, width)
        for j in range(2 * ctx):
            at = pl.ds(pl.multiple_of(table.pos[j] * BLK, BLK), BLK)
            dkv[at, pl.ds(pl.multiple_of(hp * LANES, LANES), LANES)] = dk_acc[j].astype(BF)
            dkv[at, pl.ds(pl.multiple_of(width + hp * LANES, LANES), LANES)] = dv_acc[j].astype(BF)
        return carry

    lax.fori_loop(0, PAIRS, pair, 0)


def attend_back(tbl, q, kv, da, lse, delta, ctx):
    rows, width = q.shape
    return pl.pallas_call(
        functools.partial(attend_back_kernel, ctx),
        out_shape=(shape(2, BLK, width), shape(*kv.shape)),
        in_specs=[SM] + [VM] * 5, out_specs=(VM,) * 2,
        scratch_shapes=[pltpu.VMEM((2 * ctx, BLK, LANES), F32), pltpu.VMEM((2 * ctx, BLK, LANES), F32)],
        compiler_params=params(62), name="attend_back",
    )(tbl, q, kv, da, lse, delta)


def last_kernel(ctx, tbl, dq, dkv, h1, tok, wall, dx1, vec, gvec, gq, gtok, land, ssem, rsem):
    rows = h1.shape[0]
    y = lax.axis_index("ctx")
    table = Table(tbl, 2 * ctx, y)
    sem = pltpu.get_barrier_semaphore()
    peers = [lax.rem(y + k, ctx) for k in range(1, ctx)]
    for peer in peers:
        pl.semaphore_signal(sem, inc=1, device_id={"ctx": peer}, device_id_type=pl.DeviceIdType.MESH)
    pl.semaphore_wait(sem, ctx - 1)
    copies = []
    for k, peer in enumerate(peers):
        copy = remote(dkv.at[pl.ds(pl.multiple_of(peer * rows, BLK), rows)], land.at[y], ssem.at[k], rsem.at[y], {"ctx": peer})
        copy.start()
        copies.append(copy)

    def own_kv():
        total = dkv[pl.ds(pl.multiple_of(y * rows, BLK), rows)].astype(F32)
        for peer in peers:
            remote(land.at[peer], land.at[peer], ssem.at[0], rsem.at[peer], {"ctx": peer}).wait_recv()
            total = total + land[peer].astype(F32)
        return total.astype(BF)

    last(ctx, table, y, dq, own_kv, h1, tok, wall, dx1, vec, gvec, gq, gtok)
    for copy in copies:
        copy.wait_send()


def last_call(tbl, dq, dkv, h1, tok, wall, dx1, vec, gvec, ctx, head):
    rows, width = h1.shape
    dp, r = wall.shape[:2]
    return pl.pallas_call(
        functools.partial(last_kernel, ctx),
        out_shape=(shape(dp, r, head), shape(rows, width)),
        in_specs=[SM] + [VM] * 8, out_specs=(VM,) * 2,
        scratch_shapes=[pltpu.VMEM((ctx, rows, 2 * width), BF), DMA((ctx,)), DMA((ctx,))],
        compiler_params=params(62, collective_id=2, has_side_effects=True), name="last",
    )(tbl, dq, dkv, h1, tok, wall, dx1, vec, gvec)


class Reduce:
    def __init__(self, at, g, a_core, a_x, a_z, a_y, sems):
        self.at, self.g = at, g
        self.a_core, self.a_x, self.a_z, self.a_y = a_core, a_x, a_z, a_y
        self.s1, self.r1, self.s2, self.r2, self.s3, self.r3, self.s4, self.r4 = sems
        self.mate = {"dp": at.dp_at(at.z, at.x, 1 - at.c)}
        self.across = {"dp": at.dp_at(at.z, 1 - at.x, at.c)}

    def to_core(self, p, cols, held=None):
        return remote(self.g.at[:, :, 1 - self.at.c, :, cols if held is None else held], self.a_core.at[:, :, :, cols],
                      self.s1.at[p], self.r1.at[p], self.mate)

    def to_x(self, p, cols):
        return remote(self.a_core.at[:, 1 - self.at.x, :, cols], self.a_x.at[:, :, cols],
                      self.s2.at[p], self.r2.at[p], self.across)

    def to_z(self, p, cols, k):
        at = self.at
        return remote(self.a_core.at[at.z_at(k), at.x, :, cols], self.a_z.at[k - 1, :, cols],
                      self.s3.at[p, k - 1], self.r3.at[p, k - 1], {"dp": at.dp_at(at.z_at(k), at.x, at.c)})

    def to_y(self, p, cols, k):
        at = self.at
        return remote(self.a_core.at[at.z, at.x, :, cols], self.a_y.at[k - 1, :, cols],
                      self.s4.at[p, k - 1], self.r4.at[p, k - 1], {"ctx": at.y_at(k)})

    def level1(self, p, cols, held=None):
        self.to_core(p, cols, held).start()

    def level2(self, p, cols, held=None):
        self.to_core(p, cols, held).wait_recv()
        own = self.g[:, :, self.at.c, :, cols if held is None else held]
        self.a_core[:, :, :, cols] = self.a_core[:, :, :, cols] + own
        self.to_x(p, cols).start()

    def level3(self, p, cols):
        at = self.at
        self.to_x(p, cols).wait_recv()
        self.a_core[:, at.x, :, cols] = self.a_core[:, at.x, :, cols] + self.a_x[:, :, cols]
        for k in near_first(at.lines):
            self.to_z(p, cols, k).start()

    def level4(self, p, cols):
        at = self.at
        total = self.a_core[at.z, at.x, :, cols].astype(F32)
        for k in near_first(at.lines):
            self.to_z(p, cols, k).wait_recv()
            total = total + self.a_z[k - 1, :, cols].astype(F32)
        self.a_core[at.z, at.x, :, cols] = total.astype(BF)
        for k in range(1, at.ctx):
            self.to_y(p, cols, k).start()

    def level5(self, p, cols):
        at = self.at
        total = self.a_core[at.z, at.x, :, cols].astype(F32)
        for k in range(1, at.ctx):
            self.to_y(p, cols, k).wait_recv()
            total = total + self.a_y[k - 1, :, cols].astype(F32)
        return total

    def finish(self, p, cols, core=True, held=None):
        at = self.at
        if core:
            self.to_core(p, cols, held).wait_send()
        self.to_x(p, cols).wait_send()
        for k in range(1, at.lines):
            self.to_z(p, cols, k).wait_send()
        for k in range(1, at.ctx):
            self.to_y(p, cols, k).wait_send()


def backward_kernel(dp, ctx, tbl, tok, att, cot, q, kv, h1t, lse, vec, bup, wall,
                    out, gtok, o_small, o_qkv, o_out, o_up, o_down,
                    x1, acc, dh2, da, delta, dq, dk_acc, dv_acc, send, recv, dqkv, gup, rows,
                    wub, wdb, g, a_core, a_x, a_z, a_y, wsem, ys, yr, *sems):
    at = Spot(dp, ctx)
    width = tok.shape[1]
    r = wall.shape[1]
    nd = dp // 4
    chunk = 4 * nd * r
    off_out = 128 + 3 * width
    off_up = off_out + width
    off_down = off_up + 4 * chunk
    table = Table(tbl, 2 * ctx, at.y, True)
    red = Reduce(at, g, a_core, a_x, a_z, a_y, sems)
    lines = at.lines
    last_t = 9
    actb, dub, h2 = dqkv.at[0], dqkv.at[1], dqkv.at[2]

    def cols_of(p):
        return pl.ds(pl.multiple_of(p * width, 128), width)

    def cols_q(hp):
        return pl.ds(pl.multiple_of(last_t * width + hp * 3 * LANES, 128), 3 * LANES)

    def held_q(hp):
        return pl.ds(pl.multiple_of(last_t * width + 128 + lax.rem(hp, 3) * 3 * LANES, 128), 3 * LANES)

    cols_small = pl.ds(last_t * width + 3 * width, 128)
    held_small = pl.ds(last_t * width, 128)

    def up_copy(f, slot):
        return pltpu.make_async_copy(wall.at[:, :, pl.ds(pl.multiple_of(off_up + f * chunk, 128), chunk)],
                                     wub.at[slot], wsem.at[0, slot])

    def down_copy(f, slot, j):
        return pltpu.make_async_copy(wall.at[pl.ds(f * nd, nd), :, pl.ds(off_down + j * width, width)],
                                     wdb.at[slot, :, j], wsem.at[1 + j, slot])

    def plain_copy(i, slot):
        return pltpu.make_async_copy(wall.at[:, :, pl.ds(128 + i * width, width)], wub.at[slot], wsem.at[5, slot])

    def fetch(f, slot):
        up_copy(f, slot).start()
        for j in range(4):
            down_copy(f, slot, j).start()

    plain_copy(3, 2).start()
    fetch(0, 0)
    at.barrier()
    plain_copy(3, 2).wait()
    w_out = wub[2].reshape(width, width)
    halves = [pl.ds(i * BLK, BLK) for i in range(2)]
    for i, half in enumerate(halves):
        mid = tok[half].astype(F32) + (dot(att[table.slot_of[i]], w_out) + vec[4:5])
        x1[half] = mid
        low = (normed(mid)[0] * vec[5:6] + vec[6:7]).astype(BF)
        h2[half] = low
        acc[half] = mid + vec[7:8]
        dh2[half] = jnp.zeros((BLK, width), F32)

    def part(f, carry):
        slot = lax.rem(f, 2)

        @pl.when(f < 3)
        def _():
            fetch(f + 1, 1 - slot)

        up_copy(f, slot).wait()
        for j in range(4):
            down_copy(f, slot, j).wait()
        w_up = wub[slot].reshape(width, chunk)
        w_down = wdb[slot].reshape(chunk, width)
        hid = pl.ds(pl.multiple_of(f * chunk, 128), chunk)
        bias = bup[:, hid]
        sums = jnp.zeros((1, chunk), F32)
        for half in halves:
            u = dot(h2[half], w_up) + bias
            sq = u * u
            t = jnp.tanh(u * (0.7978845608028654 + 0.03567740813636141 * sq))
            act = (0.5 * u * (1.0 + t)).astype(BF)
            actb[half] = act
            slope = 0.5 * (1.0 + t) + 0.5 * u * (1.0 - t * t) * (0.7978845608028654 + 0.10703222440908423 * sq)
            acc[half] += dot(act, w_down)
            dul = (slope * dot_t(cot[half], w_down)).astype(BF)
            dub[half] = dul
            sums = sums + jnp.sum(dul.astype(F32), axis=0, keepdims=True)
            dh2[half] += dot_t(dul, w_up)
        gup[:, hid] = sums
        g[:, :, :, :, cols_of(f)] = dot_l(h2[...], dub[...]).astype(BF).reshape(lines, 2, 2, r, chunk)
        red.level1(f, cols_of(f))
        g_down = dot_l(actb[...], cot[...]).astype(BF).reshape(nd // 4, 2, 2, 4, r, width)
        for j in range(4):
            g[pl.ds(f * (nd // 4), nd // 4), :, :, :, pl.ds((4 + j) * width, width)] = g_down[:, :, :, j]
        for lag, level in ((1, red.level2), (2, red.level3), (3, red.level4)):
            @pl.when(f >= lag)
            def _():
                level(f - lag, cols_of(f - lag))
        return carry

    lax.fori_loop(0, 4, part, 0)
    for p in range(4, 8):
        red.level1(p, cols_of(p))
    for i, half in enumerate(halves):
        out[half] = jnp.where(table.turned, acc[halves[1 - i]], acc[half]).astype(BF)
    rows[...] = jnp.zeros_like(rows)
    lane_head = lax.broadcasted_iota(jnp.int32, (16, width), 0)
    pick = (lax.broadcasted_iota(jnp.int32, (16, width), 1) // HD == lane_head).astype(F32)
    grad = None
    w_out = wub[2].reshape(width, width)
    for i, half in enumerate(halves):
        gf = cot[half].astype(F32)
        unit, inv = normed(x1[half])
        dy = dh2[half]
        mid_grad = gf + norm_back(dy, unit, inv, vec[5:6])
        acc[half] = mid_grad
        branch = mid_grad.astype(BF)
        rows[4:5] += jnp.sum(branch.astype(F32), axis=0, keepdims=True)
        rows[5:6] += jnp.sum(dy * unit, axis=0, keepdims=True)
        rows[6:7] += jnp.sum(dy, axis=0, keepdims=True)
        rows[7:8] += jnp.sum(gf, axis=0, keepdims=True)
        own = att[table.slot_of[i]]
        piece = dot_l(own, branch)
        grad = piece if grad is None else grad + piece
        back = dot_t(branch, w_out).astype(BF)
        da[half] = back
        delta[i] = lax.dot_general(pick, back.astype(F32) * own.astype(F32), (((1,), (1,)), ((), ())),
                                   precision=lax.Precision.HIGHEST, preferred_element_type=F32)
    g[:, :, :, :, cols_of(8)] = grad.astype(BF).reshape(lines, 2, 2, r, width)
    red.level1(8, cols_of(8))
    for i in range(3):
        plain_copy(i, i).start()
    red.level2(3, cols_of(3))
    red.level3(2, cols_of(2))
    red.level4(1, cols_of(1))

    def done_t(p):
        total = red.level5(p, cols_of(p))

        @pl.when(p < 4)
        def _():
            o_up[:, pl.ds(pl.multiple_of(jnp.minimum(p, 3) * width, 128), width)] = total

        @pl.when(p >= 4)
        def _():
            o_down[pl.ds(pl.multiple_of(jnp.clip(p - 4, 0, 3) * r, 8), r), :] = total

    done_t(jnp.int32(0))
    other = lax.rem(at.y + 1, 2)
    mate_y = {"ctx": other}

    def kv_copy(hp):
        return remote(send.at[hp], recv.at[hp], ys.at[hp], yr.at[hp], mate_y)

    def q_grad(hp):
        lanes = pl.ds(pl.multiple_of(hp * LANES, LANES), LANES)
        kv_copy(hp).wait_recv()
        for i in range(2):
            dqkv[1 + i, :, lanes] = (dqkv[1 + i, :, lanes].astype(F32)
                                     + recv[hp, :, i * LANES:(i + 1) * LANES].astype(F32)).astype(BF)
        low = jnp.concatenate([dqkv[i, :, lanes] for i in range(3)], axis=1)

        @pl.when(hp >= 3)
        def _():
            red.to_core(last_t + jnp.maximum(hp - 3, 0), cols_q(0), held_q(0)).wait_send()

        g[:, :, :, :, held_q(hp)] = dot(h1t[...], low).astype(BF).reshape(lines, 2, 2, r, 3 * LANES)
        red.level1(last_t + hp, cols_q(hp), held_q(hp))

    def done_q(hp):
        total = red.level5(last_t + hp, cols_q(hp))
        for i in range(3):
            o_qkv[:, pl.ds(pl.multiple_of(i * width + hp * LANES, LANES), LANES)] = total[:, i * LANES:(i + 1) * LANES]

    def level_q(level, hp):
        if level == red.level2:
            level(last_t + hp, cols_q(hp), held_q(hp))
        else:
            level(last_t + hp, cols_q(hp))

    outermost = table.block[0] == 0

    def pair(hp, carry):
        def put_dq(slot, value):
            dq[slot] = value

        attend_back_pair(hp, table, q, kv, da, lse, delta, put_dq, dk_acc, dv_acc, width)
        lanes = pl.ds(pl.multiple_of(hp * LANES, LANES), LANES)
        for i, half in enumerate(halves):
            dqkv[0, half, lanes] = dq[i]
            outer, inner = (0, 1) if i == 0 else (3, 2)
            for n, sums in enumerate((dk_acc, dv_acc)):
                dqkv[1 + n, half, lanes] = jnp.where(outermost, sums[outer], sums[inner]).astype(BF)
                send[hp, half, n * LANES:(n + 1) * LANES] = jnp.where(outermost, sums[inner], sums[outer]).astype(BF)
        kv_copy(hp).start()

        @pl.when(hp < 5)
        def _():
            red.level2(4 + hp, cols_of(4 + hp))

        red.level3(3 + hp, cols_of(3 + hp))
        red.level4(2 + hp, cols_of(2 + hp))
        done_t(1 + hp)

        @pl.when(hp >= 2)
        def _():
            q_grad(hp - 2)

        for lag, level in ((3, red.level2), (4, red.level3), (5, red.level4)):
            @pl.when(hp >= lag)
            def _():
                level_q(level, hp - lag)
        return carry

    lax.fori_loop(0, PAIRS, pair, 0)
    for i in range(3):
        plain_copy(i, i).wait()
    red.level4(8, cols_of(8))
    done_t(jnp.int32(7))
    q_grad(jnp.int32(4))
    level_q(red.level2, 3)
    level_q(red.level3, 2)
    level_q(red.level4, 1)
    o_out[...] = red.level5(8, cols_of(8))
    done_q(0)
    q_grad(jnp.int32(5))
    level_q(red.level2, 4)
    level_q(red.level3, 3)
    level_q(red.level4, 2)
    done_q(1)
    for i in range(3):
        piece = dot_t(dqkv[i], wub[i].reshape(width, width))
        if i == 0:
            dh2[...] = piece
        else:
            dh2[...] += piece
    level_q(red.level2, 5)
    level_q(red.level3, 4)
    level_q(red.level4, 3)
    for half in halves:
        dy = dh2[half]
        unit, inv = normed(tok[half].astype(F32))
        acc[half] += norm_back(dy, unit, inv, vec[0:1])
        rows[0:1] += jnp.sum(dy * unit, axis=0, keepdims=True)
        rows[1:2] += jnp.sum(dy, axis=0, keepdims=True)
        rows[2:3] += jnp.sum(dqkv[0, half].astype(F32), axis=0, keepdims=True)
        rows[3:4] += jnp.sum(dqkv[2, half].astype(F32), axis=0, keepdims=True)
    for i, half in enumerate(halves):
        gtok[half] = jnp.where(table.turned, acc[halves[1 - i]], acc[half]).astype(BF)
    small = jnp.transpose(rows[...])
    lane = lax.broadcasted_iota(jnp.int32, small.shape, 1)
    tall = jnp.transpose(jnp.broadcast_to(gup[...], (8, 4 * chunk))).reshape(dp, 4, r, 8)
    for j in range(4):
        small = jnp.where(lane == 8 + j, tall[:, j].reshape(width, 8)[:, 0:1], small)
    g[:, :, :, :, held_small] = small.astype(BF).reshape(lines, 2, 2, r, 128)
    red.level1(last_t + 6, cols_small, held_small)
    level_q(red.level3, 5)
    red.level2(last_t + 6, cols_small, held_small)
    level_q(red.level4, 4)
    done_q(2)
    done_q(3)
    red.level3(last_t + 6, cols_small)
    level_q(red.level4, 5)
    red.level4(last_t + 6, cols_small)
    done_q(4)
    done_q(5)
    o_small[...] = red.level5(last_t + 6, cols_small)
    for p in range(last_t):
        red.finish(p, cols_of(p))
    for hp in range(PAIRS):
        red.finish(last_t + hp, cols_q(hp), hp >= 3, held_q(hp))
        kv_copy(hp).wait_send()
    red.finish(last_t + 6, cols_small, True, held_small)


def backward(tbl, tok, att, cot, q, kv, h1t, lse, vec, bup, wall, ctx):
    rows, width = tok.shape
    dp, r, full = wall.shape
    lines, nd = dp // 4, dp // 4
    chunk = 4 * nd * r
    V = pltpu.VMEM
    return pl.pallas_call(
        functools.partial(backward_kernel, dp, ctx),
        out_shape=(shape(rows, width), shape(rows, width), shape(r, 128, dtype=F32), shape(r, 3 * width, dtype=F32),
                   shape(r, width, dtype=F32), shape(r, 4 * chunk, dtype=F32), shape(4 * r, width, dtype=F32)),
        in_specs=[SM] + [VM] * 9 + [ANY], out_specs=(VM,) * 7,
        scratch_shapes=[V((rows, width), F32), V((rows, width), F32), V((rows, width), F32), V((rows, width), BF),
                        V((2, 16, BLK), F32),
                        V((2, BLK, LANES), BF), V((2 * ctx, BLK, LANES), F32), V((2 * ctx, BLK, LANES), F32),
                        V((PAIRS, rows, 2 * LANES), BF), V((PAIRS, rows, 2 * LANES), BF), V((3, rows, width), BF),
                        V((1, 4 * chunk), F32), V((128, width), F32),
                        V((3, dp, r, chunk), BF), V((2, nd, 4, r, width), BF),
                        V((lines, 2, 2, r, 9 * width + 128 + 9 * LANES), BF), V((lines, 2, r, full), BF), V((lines, r, full), BF),
                        V((lines - 1, r, full), BF), V((ctx - 1, r, full), BF),
                        DMA((6, 3)), DMA((PAIRS,)), DMA((PAIRS,)),
                        DMA((16,)), DMA((16,)), DMA((16,)), DMA((16,)), DMA((16, lines - 1)), DMA((16, lines - 1)),
                        DMA((16, ctx - 1)), DMA((16, ctx - 1))],
        compiler_params=pltpu.CompilerParams(vmem_limit_bytes=67043328, collective_id=3, has_side_effects=True),
        name="backward",
    )(tbl, tok, att, cot, q, kv, h1t, lse, vec, bup, wall)


def finish_kernel(count, *refs):
    ins, small, outs = refs[:count], refs[count], refs[count + 1:2 * count + 1]
    vectors, rest = refs[2 * count + 1:2 * count + 10], refs[2 * count + 10:]
    held, fetched, given = rest[:count], rest[count], rest[count + 1]

    def fetch(i):
        return pltpu.make_async_copy(ins[i], held[i], fetched.at[i])

    def give(i):
        return pltpu.make_async_copy(held[i], outs[i], given.at[i])

    for i in range(count):
        fetch(i).start()
    r = small.shape[0]
    total = jnp.transpose(jnp.concatenate([small[...], jnp.zeros((128 - r, 128), F32)], axis=0))
    for i in range(8):
        vectors[i][...] = total[i:i + 1, 0:r].reshape(r)
    vectors[8][...] = total[8:12, 0:r]
    for i in range(count):
        fetch(i).wait()
        give(i).start()
    for i in range(count):
        give(i).wait()


def finish(results, small):
    count, r = len(results), small.shape[0]
    outs = tuple(jax.ShapeDtypeStruct(a.shape, a.dtype) for a in results)
    return pl.pallas_call(
        functools.partial(finish_kernel, count),
        out_shape=outs + (shape(r, dtype=F32),) * 8 + (shape(4, r, dtype=F32),),
        in_specs=[HBM] * count + [VM], out_specs=(HBM,) * count + (VM,) * 9,
        scratch_shapes=[pltpu.VMEM(a.shape, a.dtype) for a in results] + [DMA((count,)), DMA((count,))],
        compiler_params=pltpu.CompilerParams(vmem_limit_bytes=67043328), name="finish",
    )(*results, small)


def shards(tokens, block_table, ln1_gain, ln1_bias, w_qkv, bias_query, bias_value, w_out, bias_out,
           ln2_gain, ln2_bias, w_up, bias_up, w_down, bias_down, cotangent):
    dp, ctx = lax.axis_size("dp"), lax.axis_size("ctx")
    width, hidden = tokens.shape[2], w_up.shape[1]
    r = w_qkv.shape[0]
    head = 128 + 3 * width
    third = (width + 2 * hidden) // 3
    off_up = head + width
    off_down = off_up + hidden
    vectors = [ln1_gain, ln1_bias, bias_query, bias_value, bias_out, ln2_gain, ln2_bias, bias_down]
    if ctx == 2 and dp == 16:
        wall, tok, cot, h1, q, kv, att, lse, vec = front(
            block_table, tokens[0], cotangent[0], vectors, bias_up.reshape(4, r), (w_qkv, w_out, w_up, w_down), dp, ctx)
        bup = vec[8:12].reshape(4, dp, r).transpose(1, 0, 2).reshape(1, hidden)
        out, gtok, g_small, g_qkv, g_out, g_up, g_down = backward(
            block_table, tok, att, cot, q, kv, h1, lse, vec, bup, wall, ctx)
        out, gtok, g_qkv, g_out, g_up, g_down, *rows = finish((out, gtok, g_qkv, g_out, g_up, g_down), g_small)
        return (out[None], gtok[None], rows[0], rows[1], g_qkv, rows[2], rows[3], g_out, rows[4], rows[5], rows[6],
                g_up, rows[8].reshape(4 * r), g_down, rows[7])
    small = jnp.concatenate([jnp.stack(vectors), bias_up.reshape(4, r), jnp.zeros((116, r), BF)]).T
    cat = jnp.concatenate([small, w_qkv, w_out, w_up] + [w_down[j * r:(j + 1) * r] for j in range(4)], axis=1)
    tok_all, wall = gather(tokens[0], cat, dp, ctx, head, third)
    h1, q, kv, att, lse, vec = attend(block_table, tok_all, wall, ctx)
    bup = vec[8:12].reshape(4, dp, r).transpose(1, 0, 2).reshape(1, hidden)
    out, gt, da, dx1, delta, gvec, gup = feed_call(block_table, tokens[0], att, wall, cotangent[0], vec, bup,
                                                   ctx, off_up, off_down, 3 * third)
    dq, dkv = attend_back(block_table, q, kv, da, lse, delta, ctx)
    gvec = gvec.at[8:12].set(gup.reshape(dp, 4, r).transpose(1, 0, 2).reshape(4, width))
    gq, gtok = last_call(block_table, dq, dkv, h1, tokens[0], wall, dx1, vec, gvec, ctx, head)
    total = scatter(gq, gt, dp, ctx, head, third)
    rows = total[:, 0:128].T
    g_down = jnp.concatenate([total[:, off_down + j * width:off_down + (j + 1) * width] for j in range(4)], axis=0)
    return (out[None], gtok[None], rows[0], rows[1], total[:, 128:head], rows[2], rows[3],
            total[:, head:off_up], rows[4], rows[5], rows[6], total[:, off_up:off_down],
            rows[8:12].reshape(4 * r), g_down, rows[7])


def solution(mesh):
    row, mat = P("dp"), P("dp", None)
    act = P("dp", "ctx", None)
    in_specs = (act, P(), row, row, mat, row, row, mat, row, row, row, mat, row, mat, row, act)
    out_specs = (act, act, row, row, mat, row, row, mat, row, row, row, mat, row, mat, row)
    return jax.shard_map(shards, mesh=mesh, in_specs=in_specs, out_specs=out_specs, check_vma=False)
```

```python
import functools
import jax
import jax.numpy as jnp
from jax import lax
from jax.experimental import pallas as pl
from jax.experimental.pallas import tpu as pltpu
from jax.sharding import PartitionSpec as P

ANY = pl.BlockSpec(memory_space=pl.ANY)
VM = pl.BlockSpec(memory_space=pltpu.VMEM)
HBM = pl.BlockSpec(memory_space=pltpu.HBM)
DMA = pltpu.SemaphoreType.DMA


def near_first(count):
    order = []
    for step in range(1, count):
        order.append((step + 1) // 2 if step % 2 else count - step // 2)
    return order


class Spot:
    def __init__(self, dp, ctx):
        self.dp, self.ctx = dp, ctx
        self.lines = dp // 4
        me = lax.axis_index("dp")
        self.y = lax.axis_index("ctx")
        self.z = me // 4
        self.x = (me // 2) % 2
        self.c = me % 2
        self.me = me

    def dp_at(self, z, x, c):
        return (z * 2 + x) * 2 + c

    def z_at(self, k):
        return lax.rem(self.z + k, self.lines)

    def y_at(self, k):
        return lax.rem(self.y + k, self.ctx)

    def barrier(self):
        sem = pltpu.get_barrier_semaphore()
        peers = [{"dp": self.dp_at(self.z_at(k), self.x, self.c)} for k in range(1, self.lines)]
        peers.append({"dp": self.dp_at(self.z, 1 - self.x, self.c)})
        peers.append({"dp": self.dp_at(self.z, self.x, 1 - self.c)})
        peers += [{"ctx": self.y_at(k)} for k in range(1, self.ctx)]
        for peer in peers:
            pl.semaphore_signal(sem, inc=1, device_id=peer, device_id_type=pl.DeviceIdType.MESH)
        pl.semaphore_wait(sem, len(peers))


def remote(src, dst, ssem, rsem, device):
    return pltpu.make_async_remote_copy(
        src_ref=src, dst_ref=dst, send_sem=ssem, recv_sem=rsem,
        device_id=device, device_id_type=pl.DeviceIdType.MESH,
    )


def gather_kernel(dp, ctx, head, third, tok_ref, cat_ref, tok_all, wall,
                  loc, st, rt, sz, rz, sx, rx, sy, ry, sc, rc):
    at = Spot(dp, ctx)
    lines = at.lines
    ky = at.y % 2
    mine = pl.multiple_of(head + third + ky * third, 128)
    other = pl.multiple_of(head + third + (1 - ky) * third, 128)
    cols = {"q": pl.ds(0, head), "m": pl.ds(mine, third), "t": pl.ds(head, third), "o": pl.ds(other, third)}
    num = {"q": 0, "m": 1, "t": 2, "o": 3}
    own = at.me
    mate = {"dp": at.dp_at(at.z, at.x, 1 - at.c)}
    across = {"dp": at.dp_at(at.z, 1 - at.x, at.c)}
    pair = {"ctx": at.y + 1 - 2 * ky}
    at.barrier()
    copies = []

    def go(copy):
        copy.start()
        copies.append(copy)

    local = [pltpu.make_async_copy(cat_ref, wall.at[own], loc.at[0]),
             pltpu.make_async_copy(tok_ref, tok_all.at[at.y], loc.at[1])]
    for copy in local:
        copy.start()

    def block(b, z, x, c):
        return wall.at[at.dp_at(z, x, c), :, cols[b]]

    def own_block(b):
        return cat_ref.at[:, cols[b]]

    def send_z(b):
        for k in near_first(lines):
            go(remote(own_block(b), block(b, at.z, at.x, at.c), sz.at[num[b], k], rz.at[num[b], at.z],
                      {"dp": at.dp_at(at.z_at(k), at.x, at.c)}))

    def send_x(b, z, k, src):
        go(remote(src, block(b, z, at.x, at.c), sx.at[num[b], k], rx.at[num[b], z], across))

    def send_c(b, z, x, k, kx, src):
        go(remote(src, block(b, z, x, at.c), sc.at[num[b], k, kx], rc.at[num[b], z, x], mate))

    def send_y(z, x, k, kx, src):
        go(remote(src, block("m", z, x, at.c), sy.at[k, kx], ry.at[z, x], pair))

    def got_z(b, k):
        z = at.z_at(k)
        remote(own_block(b), block(b, z, at.x, at.c), sz.at[num[b], 0], rz.at[num[b], z], across).wait_recv()

    def got_x(b, k):
        z = at.z_at(k)
        remote(own_block(b), block(b, z, 1 - at.x, at.c), sz.at[num[b], 0], rx.at[num[b], z], across).wait_recv()

    def got_y(k, kx):
        z, x = at.z_at(k), (at.x + kx) % 2
        remote(own_block("o"), block("o", z, x, at.c), sz.at[0, 0], ry.at[z, x], across).wait_recv()

    def got_c(b, k, kx):
        z, x = at.z_at(k), (at.x + kx) % 2
        remote(own_block(b), block(b, z, x, 1 - at.c), sz.at[0, 0], rc.at[num[b], z, x], across).wait_recv()

    order = [0] + near_first(lines)
    for k in range(1, ctx):
        go(remote(tok_ref, tok_all.at[at.y], st.at[k], rt.at[at.y], {"ctx": at.y_at(k)}))
    for b in ("q", "m", "t"):
        send_z(b)
    for b in ("q", "m", "t"):
        send_x(b, at.z, 0, own_block(b))
        send_c(b, at.z, at.x, 0, 0, own_block(b))
        for k in order[1:]:
            got_z(b, k)
            z = at.z_at(k)
            src = block(b, z, at.x, at.c)
            send_x(b, z, k, src)
            if b == "m":
                send_y(z, at.x, k, 0, src)
            send_c(b, z, at.x, k, 0, src)
        for k in order:
            got_x(b, k)
            z = at.z_at(k)
            src = block(b, z, 1 - at.x, at.c)
            if b == "m":
                send_y(z, 1 - at.x, k, 1, src)
            send_c(b, z, 1 - at.x, k, 1, src)
    send_c("o", at.z, at.x, 0, 0, own_block("o"))
    for kx in range(2):
        for k in order:
            if k == 0 and kx == 0:
                continue
            got_y(k, kx)
            z, x = at.z_at(k), (at.x + kx) % 2
            send_c("o", z, x, k, kx, block("o", z, x, at.c))
    for b in ("q", "m", "t", "o"):
        for kx in range(2):
            for k in order:
                got_c(b, k, kx)
    for k in range(1, ctx):
        y = at.y_at(k)
        remote(tok_ref, tok_all.at[y], st.at[0], rt.at[y], across).wait_recv()
    for copy in copies:
        copy.wait_send()
    for copy in local:
        copy.wait()


def gather(tok, cat, dp, ctx, head, third):
    lines = dp // 4
    rows, width = cat.shape
    return pl.pallas_call(
        functools.partial(gather_kernel, dp, ctx, head, third),
        out_shape=(jax.ShapeDtypeStruct((ctx, *tok.shape), tok.dtype),
                   jax.ShapeDtypeStruct((dp, rows, width), cat.dtype)),
        in_specs=[VM, VM], out_specs=(ANY, ANY),
        scratch_shapes=[DMA((2,)), DMA((ctx,)), DMA((ctx,)),
                        DMA((3, lines)), DMA((3, lines)), DMA((3, lines)), DMA((3, lines)),
                        DMA((lines, 2)), DMA((lines, 2)), DMA((4, lines, 2)), DMA((4, lines, 2))],
        compiler_params=pltpu.CompilerParams(collective_id=0, has_side_effects=True, vmem_limit_bytes=32 * 2**20),
    )(tok, cat)


def scatter_kernel(dp, ctx, head, third, gq, gt, out, a_core, a_pair, a_x, a_z, a_y, stage, total,
                   loc, s1, r1, s2, r2, s3, r3, s4, r4, s5, r5):
    at = Spot(dp, ctx)
    lines = at.lines
    rows = gq.shape[1]
    ky = at.y % 2
    mine = pl.multiple_of(head + third + ky * third, 128)
    other = pl.multiple_of(head + third + (1 - ky) * third, 128)
    cols = {"q": pl.ds(0, head), "m": pl.ds(mine, third), "t": pl.ds(head, third), "o": pl.ds(other, third)}
    size = {"q": head, "m": third, "t": third, "o": third}
    num = {"q": 0, "m": 1, "t": 2, "o": 3}
    mate = {"dp": at.dp_at(at.z, at.x, 1 - at.c)}
    across = {"dp": at.dp_at(at.z, 1 - at.x, at.c)}
    pair = {"ctx": at.y + 1 - 2 * ky}
    at.barrier()
    copies = []

    def go(copy):
        copy.start()
        copies.append(copy)

    first = {"m": pl.multiple_of(third + ky * third, 128), "o": pl.multiple_of(third + (1 - ky) * third, 128), "t": 0}

    def full(b, at_dp):
        if b == "q":
            return gq.at[at_dp]
        return gt.at[at_dp, :, pl.ds(first[b], third)]

    order = [0] + near_first(lines)
    order = order[::-1]
    spots = [(k, kx) for kx in (1, 0) for k in order]

    def where(k, kx):
        return at.z_at(k), (at.x + kx) % 2

    def land(ref, b, *idx):
        return ref.at[(num[b], *idx, slice(None), pl.ds(0, size[b]))]

    blocks = ("o", "m", "t", "q")
    for b in blocks:
        for k, kx in spots:
            z, x = where(k, kx)
            go(remote(full(b, at.dp_at(z, x, 1 - at.c)), land(a_core, b, z, x),
                      s1.at[num[b], k, kx], r1.at[num[b], z, x], mate))
    def fetch(b, k, kx):
        z, x = where(k, kx)
        return pltpu.make_async_copy(full(b, at.dp_at(z, x, at.c)), land(stage, b, z, x),
                                     loc.at[num[b], k, kx])
    for b in blocks:
        for k, kx in spots:
            fetch(b, k, kx).start()

    def take(sem, dst):
        remote(dst, dst, s1.at[0, 0, 0], sem, across).wait_recv()

    def added(b, k, kx):
        z, x = where(k, kx)
        fetch(b, k, kx).wait()
        here = land(a_core, b, z, x)
        take(r1.at[num[b], z, x], here)
        here[...] = here[...] + land(stage, b, z, x)[...]
        return here

    for b in blocks:
        if b == "o":
            for k, kx in spots:
                z, x = where(k, kx)
                go(remote(added(b, k, kx), a_pair.at[z, x], s2.at[k, kx], r2.at[z, x], pair))
            continue
        for k, kx in spots:
            z, x = where(k, kx)
            here = added(b, k, kx)
            if b == "m":
                take(r2.at[z, x], a_pair.at[z, x])
                here[...] = here[...] + a_pair[z, x]
            if kx == 1:
                go(remote(here, land(a_x, b, z), s3.at[num[b], k], r3.at[num[b], z], across))
        for k in order:
            z = at.z_at(k)
            here = land(a_core, b, z, at.x)
            take(r3.at[num[b], z], land(a_x, b, z))
            here[...] = here[...] + land(a_x, b, z)[...]
            if k:
                go(remote(here, land(a_z, b, at.z), s4.at[num[b], k], r4.at[num[b], at.z],
                          {"dp": at.dp_at(z, at.x, at.c)}))
    for b in ("m", "t", "q"):
        acc = land(a_core, b, at.z, at.x)[...].astype(jnp.float32)
        for k in near_first(lines):
            z = at.z_at(k)
            take(r4.at[num[b], z], land(a_z, b, z))
            acc = acc + land(a_z, b, z)[...].astype(jnp.float32)
        land(total, b)[...] = acc
        land(a_core, b, at.z, at.x)[...] = acc.astype(jnp.bfloat16)
        for k in range(1, ctx):
            go(remote(land(a_core, b, at.z, at.x), land(a_y, b, at.y), s5.at[num[b], k], r5.at[num[b], at.y],
                      {"ctx": at.y_at(k)}))
    outs = []
    for b in ("t", "q", "m", "o"):
        if b == "m":
            acc = land(total, b)[...]
        elif b == "o":
            acc = jnp.zeros((rows, third), jnp.float32)
        else:
            acc = land(total, b)[...]
        for k in range(1, ctx):
            y = at.y_at(k)
            if b in ("t", "q") or (b == "m" and k % 2 == 0):
                take(r5.at[num[b], y], land(a_y, b, y))
                acc = acc + land(a_y, b, y)[...].astype(jnp.float32)
            elif b == "o" and k % 2 == 1:
                here = a_y.at[1, y, :, pl.ds(0, third)]
                take(r5.at[1, y], here)
                acc = acc + here[...].astype(jnp.float32)
        land(total, b)[...] = acc
        copy = pltpu.make_async_copy(land(total, b), out.at[:, cols[b]], loc.at[num[b], 0, 0])
        copy.start()
        outs.append(copy)
    for copy in copies:
        copy.wait_send()
    for copy in outs:
        copy.wait()


def scatter(gq, gt, dp, ctx, head, third):
    lines = dp // 4
    _, rows, width = gq.shape[0], gq.shape[1], gq.shape[2] + gt.shape[2]
    bf, f32 = jnp.bfloat16, jnp.float32
    return pl.pallas_call(
        functools.partial(scatter_kernel, dp, ctx, head, third),
        out_shape=jax.ShapeDtypeStruct((rows, width), f32),
        in_specs=[ANY, ANY], out_specs=ANY,
        scratch_shapes=[pltpu.VMEM((4, lines, 2, rows, head), bf), pltpu.VMEM((lines, 2, rows, third), bf),
                        pltpu.VMEM((3, lines, rows, head), bf), pltpu.VMEM((3, lines, rows, head), bf),
                        pltpu.VMEM((3, ctx, rows, head), bf), pltpu.VMEM((4, lines, 2, rows, head), bf),
                        pltpu.VMEM((4, rows, head), f32),
                        DMA((4, lines, 2)), DMA((4, lines, 2)), DMA((4, lines, 2)),
                        DMA((lines, 2)), DMA((lines, 2)),
                        DMA((3, lines)), DMA((3, lines)), DMA((3, lines)), DMA((3, lines)),
                        DMA((3, ctx)), DMA((3, ctx))],
        compiler_params=pltpu.CompilerParams(collective_id=1, has_side_effects=True, vmem_limit_bytes=60 * 2**20),
    )(gq, gt)


F32, BF = jnp.float32, jnp.bfloat16
HEADS, HD, BLK = 12, 64, 256
PAIRS, LANES = HEADS // 2, 2 * HD


def dot(a, b):
    return jnp.dot(a, b, preferred_element_type=F32)


def dot_t(a, b):
    return lax.dot_general(a, b, (((1,), (1,)), ((), ())), preferred_element_type=F32)


def dot_l(a, b):
    return lax.dot_general(a, b, (((0,), (0,)), ((), ())), preferred_element_type=F32)


def normed(x):
    centred = x - jnp.mean(x, axis=-1, keepdims=True)
    inv = lax.rsqrt(jnp.mean(centred * centred, axis=-1, keepdims=True) + 1e-05)
    return centred * inv, inv


def norm_back(dy, unit, inv, gain):
    dn = dy * gain
    return inv * (dn - jnp.mean(dn, axis=-1, keepdims=True) - unit * jnp.mean(dn * unit, axis=-1, keepdims=True))


class Table:
    def __init__(self, tbl, nb, y, ordered=False):
        self.nb, self.half = nb, nb // 2
        self.own = [tbl[2 * y], tbl[2 * y + 1]]
        self.turned = self.own[0] >= self.half
        first_high = self.turned.astype(jnp.int32)
        self.place = [first_high, 1 - first_high]
        self.row_of = [first_high, 1 - first_high]
        self.slot_of = [first_high, 1 - first_high]
        self.block = [jnp.minimum(self.own[0], self.own[1]), jnp.maximum(self.own[0], self.own[1])]
        self.tbl = tbl
        if ordered:
            self.row_of, self.slot_of, self.pos = [0, 1], [0, 1], list(range(nb))
            return
        self.pos = []
        for j in range(nb):
            at = jnp.int32(0)
            for p in range(nb):
                at = at + jnp.where(tbl[p] == j, p, 0)
            self.pos.append(at)

    def keys(self, slot):
        return self.half if slot == 0 else self.nb

    def masked(self, slot, j):
        return j >= 1 if slot == 0 else j > self.half


def rows_of(ref, *idx):
    value = ref[idx]
    return value.reshape(value.shape[0] * value.shape[1], value.shape[2])


def block_rows(i):
    return pl.ds(i * BLK if isinstance(i, int) else pl.multiple_of(i * BLK, BLK), BLK)


def lane_masks(rows):
    lane = lax.broadcasted_iota(jnp.int32, (rows, LANES), 1)
    return [lane < HD, lane >= HD]


def project(ctx, tok, wall, h1, q, kv, vec, y):
    gain, shift = vec[0:1], vec[1:2]
    width = tok.shape[2]
    zero = jnp.zeros((1, width), F32)
    kv_bias = jnp.concatenate([zero, vec[3:4]], axis=1)
    w_kv = rows_of(wall, slice(None), slice(None), slice(128 + width, 128 + 3 * width))

    def rows(r, carry):
        x = tok[r // 2, pl.ds(pl.multiple_of((r % 2) * BLK, BLK), BLK)].astype(F32)
        low = (normed(x)[0] * gain + shift).astype(BF)
        kv[pl.ds(pl.multiple_of(r * BLK, BLK), BLK)] = (dot(low, w_kv) + kv_bias).astype(BF)
        return carry

    lax.fori_loop(0, 2 * ctx, rows, 0)
    w_q = rows_of(wall, slice(None), slice(None), slice(128, 128 + width))

    def own(i, carry):
        at = pl.ds(pl.multiple_of(i * BLK, BLK), BLK)
        low = (normed(tok[y, at].astype(F32))[0] * gain + shift).astype(BF)
        h1[at] = low
        q[at] = ((dot(low, w_q) + vec[2:3]).astype(BF).astype(F32) * HD ** (-0.5)).astype(BF)
        return carry

    lax.fori_loop(0, 2, own, 0)


def attend_pair(hp, table, q, kv, att, lse_acc, width):
    lanes = pl.ds(pl.multiple_of(hp * LANES, LANES), LANES)
    v_lanes = pl.ds(pl.multiple_of(width + hp * LANES, LANES), LANES)
    masks = lane_masks(BLK)
    lane = lax.broadcasted_iota(jnp.int32, (BLK, LANES), 1)
    for slot in range(2):
        q2 = q[block_rows(table.row_of[slot]), lanes]
        spots = [block_rows(table.pos[j]) for j in range(table.keys(slot))]
        mixed = []
        for h in range(2):
            qm = jnp.where(masks[h], q2, jnp.zeros_like(q2))
            scores = []
            for j, at in enumerate(spots):
                s = dot_t(qm, kv[at, lanes])
                if table.masked(slot, j):
                    s = jnp.where(j <= table.block[slot], s, -1e30)
                scores.append(s)
            largest = functools.reduce(jnp.maximum, scores)
            largest = jnp.max(largest, axis=-1, keepdims=True)
            exps = [jnp.exp(s - largest) for s in scores]
            total = jnp.sum(functools.reduce(jnp.add, exps), axis=-1, keepdims=True)
            out = functools.reduce(jnp.add, [dot(e.astype(BF), kv[at, v_lanes]) for e, at in zip(exps, spots)])
            mixed.append(out / total)
            lse_acc[slot] = jnp.where(lane == 2 * hp + h, largest + jnp.log(total), lse_acc[slot])
        att[slot, :, lanes] = jnp.where(masks[0], mixed[0], mixed[1]).astype(BF)


def attend_back_pair(hp, table, q, kv, da, lse, delta, put_dq, dk_acc, dv_acc, width):
    lanes = pl.ds(pl.multiple_of(hp * LANES, LANES), LANES)
    v_lanes = pl.ds(pl.multiple_of(width + hp * LANES, LANES), LANES)
    masks = lane_masks(BLK)
    for slot in (1, 0):
        row = block_rows(table.row_of[slot])
        q2, da2 = q[row, lanes], da[row, lanes]
        dq_acc = None
        for h in range(2):
            qm = jnp.where(masks[h], q2, jnp.zeros_like(q2))
            dam = jnp.where(masks[h], da2, jnp.zeros_like(da2))
            lse_row = lse[slot, pl.ds(2 * hp + h, 1), :]
            delta_row = delta[table.row_of[slot], pl.ds(2 * hp + h, 1), :]
            for j in range(table.keys(slot)):
                at = block_rows(table.pos[j])
                k2, v2 = kv[at, lanes], kv[at, v_lanes]
                st = dot_t(k2, qm)
                if table.masked(slot, j):
                    st = jnp.where(j <= table.block[slot], st, -1e30)
                pt = jnp.exp(st - lse_row)
                dst = (pt * (dot_t(v2, dam) - delta_row)).astype(BF)
                dv, dk = dot(pt.astype(BF), dam), dot(dst, qm)
                if slot == 1 and h == 0:
                    dv_acc[j], dk_acc[j] = dv, dk
                else:
                    dv_acc[j] += dv
                    dk_acc[j] += dk
                part = dot_l(dst, jnp.where(masks[h], k2, jnp.zeros_like(k2)))
                dq_acc = part if dq_acc is None else dq_acc + part
        put_dq(slot, (dq_acc * HD ** (-0.5)).astype(BF))


def feed(nd, off_up, off_down, table, tok, att, wall, cot, vec, bup, out, gt, da, dx1, delta, gvec, gup,
         x1, h2, acc, dh2):
    rows, width = cot.shape
    dp, r = wall.shape[0], wall.shape[1]
    chunk = 4 * nd * r
    w_out = rows_of(wall, slice(None), slice(None), slice(off_up - width, off_up))
    for i in range(2):
        at = pl.ds(i * BLK, BLK)
        mid = tok[at].astype(F32) + (dot(att[table.slot_of[i]], w_out) + vec[4:5])
        x1[at] = mid
        h2[at] = (normed(mid)[0] * vec[5:6] + vec[6:7]).astype(BF)
        acc[at] = mid + vec[7:8]
    dh2[...] = jnp.zeros_like(dh2)
    g = cot[...]

    def part(f, carry):
        cols = pl.ds(pl.multiple_of(off_up + f * chunk, 128), chunk)
        w_up = rows_of(wall, slice(None), slice(None), cols)
        w_down = jnp.concatenate(
            [wall[f * nd + d, :, pl.ds(off_down + j * width, width)] for d in range(nd) for j in range(4)], axis=0)
        low = h2[...]
        u = dot(low, w_up) + bup[:, pl.ds(pl.multiple_of(f * chunk, 128), chunk)]
        sq = u * u
        t = jnp.tanh(u * (0.7978845608028654 + 0.03567740813636141 * sq))
        act = (0.5 * u * (1.0 + t)).astype(BF)
        slope = 0.5 * (1.0 + t) + 0.5 * u * (1.0 - t * t) * (0.7978845608028654 + 0.10703222440908423 * sq)
        acc[...] += dot(act, w_down)
        du = slope * dot_t(g, w_down)
        dul = du.astype(BF)
        gup[:, pl.ds(pl.multiple_of(f * chunk, 128), chunk)] = jnp.sum(dul.astype(F32), axis=0, keepdims=True)
        dh2[...] += dot_t(dul, w_up)
        g_up = dot_l(low, dul).astype(BF)
        gt[:, :, pl.ds(pl.multiple_of(width + f * chunk, 128), chunk)] = g_up.reshape(dp, r, chunk)
        g_down = dot_l(act, g).astype(BF)
        for d in range(nd):
            for j in range(4):
                piece = g_down[(4 * d + j) * r:(4 * d + j + 1) * r]
                gt[f * nd + d, :, pl.ds(width + off_down - off_up + j * width, width)] = piece
        return carry

    lax.fori_loop(0, dp // nd, part, 0)
    out[...] = acc[...].astype(BF)
    gf = g.astype(F32)
    unit, inv = normed(x1[...])
    dy = dh2[...]
    mid_grad = gf + norm_back(dy, unit, inv, vec[5:6])
    dx1[...] = mid_grad
    branch = mid_grad.astype(BF)
    gvec[...] = jnp.zeros_like(gvec)
    gvec[4:5] = jnp.sum(branch.astype(F32), axis=0, keepdims=True)
    gvec[5:6] = jnp.sum(dy * unit, axis=0, keepdims=True)
    gvec[6:7] = jnp.sum(dy, axis=0, keepdims=True)
    gvec[7:8] = jnp.sum(gf, axis=0, keepdims=True)
    head = lax.broadcasted_iota(jnp.int32, (16, width), 0)
    pick = (lax.broadcasted_iota(jnp.int32, (16, width), 1) // HD == head).astype(F32)
    grad = None
    for i in range(2):
        own = att[table.slot_of[i]]
        low = branch[i * BLK:(i + 1) * BLK]
        piece = dot_l(own, low)
        grad = piece if grad is None else grad + piece
        back = dot_t(low, w_out).astype(BF)
        da[pl.ds(i * BLK, BLK)] = back
        prod = back.astype(F32) * own.astype(F32)
        delta[i] = lax.dot_general(pick, prod, (((1,), (1,)), ((), ())), precision=lax.Precision.HIGHEST,
                                   preferred_element_type=F32)
    gt[:, :, 0:width] = grad.astype(BF).reshape(dp, r, width)


def last(ctx, table, y, dq, own_kv, h1, tok, wall, dx1, vec, gvec, gq, gtok):
    width = h1.shape[1]
    dp, r = wall.shape[0], wall.shape[1]
    w_q = rows_of(wall, slice(None), slice(None), slice(128, 128 + width))
    low = h1[...]
    dq_all = jnp.concatenate([dq[table.slot_of[0]], dq[table.slot_of[1]]], axis=0)
    gq[:, :, 128:128 + width] = dot_l(low, dq_all).astype(BF).reshape(dp, r, width)
    dh1 = dot_t(dq_all, w_q)
    dkv = own_kv()
    w_kv = rows_of(wall, slice(None), slice(None), slice(128 + width, 128 + 3 * width))
    gq[:, :, 128 + width:128 + 3 * width] = dot_l(low, dkv).astype(BF).reshape(dp, r, 2 * width)
    dh1 = dh1 + dot_t(dkv, w_kv)
    unit, inv = normed(tok[...].astype(F32))
    gtok[...] = (dx1[...] + norm_back(dh1, unit, inv, vec[0:1])).astype(BF)
    sums = [jnp.sum(dh1 * unit, axis=0, keepdims=True), jnp.sum(dh1, axis=0, keepdims=True),
            jnp.sum(dq_all.astype(F32), axis=0, keepdims=True),
            jnp.sum(dkv[:, width:].astype(F32), axis=0, keepdims=True)]
    table_rows = jnp.concatenate(sums + [gvec[4:16], jnp.zeros((112, width), F32)], axis=0)
    gq[:, :, 0:128] = jnp.transpose(table_rows).astype(BF).reshape(dp, r, 128)


SM = pl.BlockSpec(memory_space=pltpu.SMEM)


def params(limit, **more):
    return pltpu.CompilerParams(vmem_limit_bytes=limit * 2**20, **more)


def shape(*dims, dtype=BF):
    return jax.ShapeDtypeStruct(dims, dtype)


def attend_kernel(ctx, tbl, tok, wall, h1, q, kv, att, lse, vec, lse_acc):
    width = tok.shape[2]
    y = lax.axis_index("ctx")
    table = Table(tbl, 2 * ctx, y)
    small = rows_of(wall, slice(None), slice(None), slice(0, 128)).astype(F32)
    vec[...] = jnp.transpose(small)[0:16]
    project(ctx, tok, wall, h1, q, kv, vec, y)
    lse_acc[...] = jnp.zeros_like(lse_acc)

    def pair(hp, carry):
        attend_pair(hp, table, q, kv, att, lse_acc, width)
        return carry

    lax.fori_loop(0, PAIRS, pair, 0)
    for slot in range(2):
        lse[slot] = jnp.transpose(lse_acc[slot])[0:16]


def attend(tbl, tok_all, wall, ctx):
    rows, width = tok_all.shape[1:]
    return pl.pallas_call(
        functools.partial(attend_kernel, ctx),
        out_shape=(shape(rows, width), shape(rows, width), shape(ctx * rows, 2 * width), shape(2, BLK, width),
                   shape(2, 16, BLK, dtype=F32), shape(16, width, dtype=F32)),
        in_specs=[SM, VM, VM], out_specs=(VM,) * 6,
        scratch_shapes=[pltpu.VMEM((2, BLK, LANES), F32)],
        compiler_params=params(62), name="attend",
    )(tbl, tok_all, wall)


def front_kernel(dp, ctx, tbl, tok, cot, *rest):
    vectors, rest = rest[:8], rest[8:]
    (b_up, w_qkv, w_out, w_up, w_down,
     wall, tok_slots, cot_slots, h1, q, kv, att, lse, vec, bup,
     cat, small, tall, toks, wq, lse_acc, loc, st, rt, sz, rz, sx, rx, sy, ry, sc, rc) = rest
    at = Spot(dp, ctx)
    lines = at.lines
    r, full = cat.shape
    width = tok.shape[1]
    head = 128 + 3 * width
    size = (full - head) // 6
    ky = at.y
    mate = {"dp": at.dp_at(at.z, at.x, 1 - at.c)}
    across = {"dp": at.dp_at(at.z, 1 - at.x, at.c)}
    pair_y = {"ctx": 1 - ky}
    table = Table(tbl, 2 * ctx, at.y, True)
    order = [0] + near_first(lines)

    small[...] = jnp.zeros_like(small)
    for i, ref in enumerate(vectors):
        small[i:i + 1, 0:r] = ref[...].astype(F32).reshape(1, r)
    ups = b_up[...].astype(F32).reshape(1, 4 * r)
    for j in range(4):
        small[8 + j:9 + j, 0:r] = ups[:, j * r:(j + 1) * r]
    cat[:, 0:128] = jnp.transpose(small[...])[0:r].astype(BF)
    cat[:, 128:head] = w_qkv[...]
    cat[:, head:head + width] = w_out[...]
    cat[:, head + width:head + 5 * width] = w_up[...]
    for j in range(4):
        cat[:, head + (5 + j) * width:head + (6 + j) * width] = w_down[j * r:(j + 1) * r]
    at.barrier()

    def cols(p):
        if isinstance(p, int) and p >= 5:
            place = 2 * (p - 4) + 1 - ky
        else:
            n = p - 1
            place = (1 - n % 2) * (2 + 2 * (n // 2) + ky) + (n % 2) * (n // 2)
        return pl.ds(pl.multiple_of(head + place * size, 128), size)

    def is_head(p):
        return isinstance(p, int) and p == 0

    def own_block(p):
        return cat.at[:, pl.ds(0, head)] if is_head(p) else cat.at[:, cols(p)]

    def block(p, z, x, c):
        return wq.at[at.dp_at(z, x, c)] if is_head(p) else wall.at[at.dp_at(z, x, c), :, cols(p)]

    def to_z(p, k):
        return remote(own_block(p), block(p, at.z, at.x, at.c), sz.at[p, k], rz.at[p, at.z],
                      {"dp": at.dp_at(at.z_at(k), at.x, at.c)})

    def to_x(p, k):
        z = at.z_at(k)
        src = own_block(p) if k == 0 else block(p, z, at.x, at.c)
        return remote(src, block(p, z, at.x, at.c), sx.at[p, k], rx.at[p, z], across)

    def to_c(p, k, kx):
        z, x = at.z_at(k), (at.x + kx) % 2
        src = own_block(p) if k == 0 and kx == 0 else block(p, z, x, at.c)
        return remote(src, block(p, z, x, at.c), sc.at[p, k, kx], rc.at[p, z, x], mate)

    def to_y(p, k, kx):
        z, x = at.z_at(k), (at.x + kx) % 2
        n = (p - 1) // 2
        here = block(p, z, x, at.c)
        return remote(here, here, sy.at[n, k, kx], ry.at[n, z, x], pair_y)

    def got(p, z, x, c, sem):
        here = block(p, z, x, c)
        remote(here, here, st, sem, across).wait_recv()

    def stage_z(p, shared):
        for k in order:
            if k:
                got(p, at.z_at(k), at.x, at.c, rz.at[p, at.z_at(k)])
                to_x(p, k).start()
                if shared is not None:
                    pl.when(shared)(lambda: to_y(p, k, 0).start())
                to_c(p, k, 0).start()

    def stage_x(p, shared):
        for k in order:
            got(p, at.z_at(k), 1 - at.x, at.c, rx.at[p, at.z_at(k)])
            if shared is not None:
                pl.when(shared)(lambda: to_y(p, k, 1).start())
            to_c(p, k, 1).start()

    def stage_y(n):
        p = 5 + n
        for kx in range(2):
            for k in order:
                if k or kx:
                    z, x = at.z_at(k), (at.x + kx) % 2
                    got(p, z, x, at.c, ry.at[n, z, x])
                    to_c(p, k, kx).start()

    def stage_c(p):
        for kx in range(2):
            for k in order:
                z, x = at.z_at(k), (at.x + kx) % 2
                got(p, z, x, 1 - at.c, rc.at[p, z, x])

    tok_mate = remote(tok, toks.at[at.y], st, rt, pair_y)
    tok_own = pltpu.make_async_copy(tok, toks.at[at.y], loc.at[0])
    wall_own = pltpu.make_async_copy(cat.at[:, pl.ds(head, full - head)],
                                     wall.at[at.me, :, pl.ds(head, full - head)], loc.at[1])
    head_own = pltpu.make_async_copy(cat.at[:, pl.ds(0, head)], wq.at[at.me], loc.at[2])
    to_x(0, 0).start()
    for k in near_first(lines):
        to_z(0, k).start()
    to_c(0, 0, 0).start()
    tok_mate.start()
    for copy in (tok_own, head_own, wall_own):
        copy.start()
    for p in range(1, 5):
        for k in near_first(lines):
            to_z(p, k).start()
        to_x(p, 0).start()
    for p in range(1, 7):
        to_c(p, 0, 0).start()
    stage_z(0, None)
    stage_x(0, None)
    stage_c(0)
    head_own.wait()
    head_all = pltpu.make_async_copy(wq, wall.at[:, :, pl.ds(0, head)], loc.at[2])
    head_all.start()
    tok_own.wait()
    tok_mate.wait_recv()

    columns = jnp.transpose(rows_of(wq, slice(None), slice(None), slice(0, 128)).astype(F32))
    vec[...] = columns[0:16]
    for d in range(dp):
        for j in range(4):
            tall[(4 * d + j) * r:(4 * d + j + 1) * r] = jnp.broadcast_to(
                wq[d, :, 0:128].astype(F32)[:, 8 + j:9 + j], (r, 128))
    bup[...] = jnp.transpose(tall[...])[0:1]
    gain, shift = vec[0:1], vec[1:2]
    kv_bias = jnp.concatenate([jnp.zeros((1, width), F32), vec[3:4]], axis=1)

    def stored(i):
        return toks[i // 2, block_rows(i % 2)].astype(F32)

    for j in range(2 * ctx):
        here = stored(0)
        for i in range(1, 2 * ctx):
            here = jnp.where(tbl[i] == j, stored(i), here)
        low = (normed(here)[0] * gain + shift).astype(BF)
        kv[block_rows(j)] = (dot(low, rows_of(wq, slice(None), slice(None), slice(128 + width, head)))
                             + kv_bias).astype(BF)
    for i in range(2):
        def chosen(ref):
            a, b = ref[block_rows(i)].astype(F32), ref[block_rows(1 - i)].astype(F32)
            return jnp.where(table.turned, b, a)

        here = chosen(tok)
        low = (normed(here)[0] * gain + shift).astype(BF)
        h1[:, block_rows(i)] = jnp.transpose(low)
        w_q = rows_of(wq, slice(None), slice(None), slice(128, 128 + width))
        q[block_rows(i)] = ((dot(low, w_q) + vec[2:3]).astype(BF).astype(F32) * HD ** (-0.5)).astype(BF)
        tok_slots[block_rows(i)] = here.astype(BF)
        cot_slots[block_rows(i)] = chosen(cot).astype(BF)
    lse_acc[...] = jnp.zeros_like(lse_acc)

    def heads(hp, carry):
        attend_pair(hp, table, q, kv, att, lse_acc, width)
        return carry

    def stages(t, carry):
        @pl.when(t < 4)
        def _():
            stage_z(t + 1, t % 2 == 0)

        @pl.when(t >= 1)
        def _():
            stage_x(t, t % 2 == 1)

        lax.fori_loop(jnp.minimum(2 * t, PAIRS), jnp.minimum(2 * t + 2, PAIRS), heads, 0)
        return carry

    lax.fori_loop(0, 5, stages, 0)
    for slot in range(2):
        lse[slot] = jnp.transpose(lse_acc[slot])[0:16]
    stage_y(0)
    stage_y(1)
    for p in range(1, 7):
        stage_c(p)
    for p in range(5):
        for k in order:
            to_x(p, k).wait_send()
            if k:
                to_z(p, k).wait_send()
    for p in range(7):
        for kx in range(2):
            for k in order:
                to_c(p, k, kx).wait_send()
                if p in (1, 3) and (k or kx):
                    to_y(p, k, kx).wait_send()
    tok_mate.wait_send()
    wall_own.wait()
    head_all.wait()


def front(tbl, tok, cot, vectors, b_up, weights, dp, ctx):
    rows, width = tok.shape
    r = weights[0].shape[0]
    head = 128 + 3 * width
    full = head + 9 * width
    lines = dp // 4
    V = pltpu.VMEM
    return pl.pallas_call(
        functools.partial(front_kernel, dp, ctx),
        out_shape=(shape(dp, r, full), shape(rows, width), shape(rows, width), shape(width, rows), shape(rows, width),
                   shape(ctx * rows, 2 * width), shape(2, BLK, width), shape(2, 16, BLK, dtype=F32),
                   shape(16, width, dtype=F32), shape(1, 4 * width, dtype=F32)),
        in_specs=[SM] + [VM] * (2 + len(vectors) + 1 + len(weights)), out_specs=(ANY,) + (VM,) * 9,
        scratch_shapes=[V((r, full), BF), V((128, 128), F32), V((4 * width, 128), F32), V((ctx, rows, width), BF), V((dp, r, head), BF),
                        V((2, BLK, LANES), F32), DMA((3,)), DMA, DMA,
                        DMA((5, lines)), DMA((5, lines)), DMA((5, lines)), DMA((5, lines)),
                        DMA((2, lines, 2)), DMA((2, lines, 2)), DMA((7, lines, 2)), DMA((7, lines, 2))],
        compiler_params=params(62, collective_id=0, has_side_effects=True), name="front",
    )(tbl, tok, cot, *vectors, b_up, *weights)


def feed_kernel(ctx, nd, off_up, off_down, tbl, tok, att, wall, cot, vec, bup, *rest):
    table = Table(tbl, 2 * ctx, lax.axis_index("ctx"))
    feed(nd, off_up, off_down, table, tok, att, wall, cot, vec, bup, *rest)


def feed_call(tbl, tok, att, wall, cot, vec, bup, ctx, off_up, off_down, gt_cols):
    rows, width = cot.shape
    dp, r = wall.shape[:2]
    return pl.pallas_call(
        functools.partial(feed_kernel, ctx, dp // 4, off_up, off_down),
        out_shape=(shape(rows, width), shape(dp, r, gt_cols), shape(rows, width), shape(rows, width, dtype=F32),
                   shape(2, 16, BLK, dtype=F32), shape(16, width, dtype=F32), shape(1, bup.shape[1], dtype=F32)),
        in_specs=[SM] + [VM] * 6, out_specs=(VM,) * 7,
        scratch_shapes=[pltpu.VMEM((rows, width), F32), pltpu.VMEM((rows, width), BF),
                        pltpu.VMEM((rows, width), F32), pltpu.VMEM((rows, width), F32)],
        compiler_params=params(62), name="feed",
    )(tbl, tok, att, wall, cot, vec, bup)


def attend_back_kernel(ctx, tbl, q, kv, da, lse, delta, dq, dkv, dk_acc, dv_acc):
    width = q.shape[1]
    table = Table(tbl, 2 * ctx, lax.axis_index("ctx"))

    def pair(hp, carry):
        def put_dq(slot, value):
            dq[slot, :, pl.ds(pl.multiple_of(hp * LANES, LANES), LANES)] = value

        attend_back_pair(hp, table, q, kv, da, lse, delta, put_dq, dk_acc, dv_acc, width)
        for j in range(2 * ctx):
            at = pl.ds(pl.multiple_of(table.pos[j] * BLK, BLK), BLK)
            dkv[at, pl.ds(pl.multiple_of(hp * LANES, LANES), LANES)] = dk_acc[j].astype(BF)
            dkv[at, pl.ds(pl.multiple_of(width + hp * LANES, LANES), LANES)] = dv_acc[j].astype(BF)
        return carry

    lax.fori_loop(0, PAIRS, pair, 0)


def attend_back(tbl, q, kv, da, lse, delta, ctx):
    rows, width = q.shape
    return pl.pallas_call(
        functools.partial(attend_back_kernel, ctx),
        out_shape=(shape(2, BLK, width), shape(*kv.shape)),
        in_specs=[SM] + [VM] * 5, out_specs=(VM,) * 2,
        scratch_shapes=[pltpu.VMEM((2 * ctx, BLK, LANES), F32), pltpu.VMEM((2 * ctx, BLK, LANES), F32)],
        compiler_params=params(62), name="attend_back",
    )(tbl, q, kv, da, lse, delta)


def last_kernel(ctx, tbl, dq, dkv, h1, tok, wall, dx1, vec, gvec, gq, gtok, land, ssem, rsem):
    rows = h1.shape[0]
    y = lax.axis_index("ctx")
    table = Table(tbl, 2 * ctx, y)
    sem = pltpu.get_barrier_semaphore()
    peers = [lax.rem(y + k, ctx) for k in range(1, ctx)]
    for peer in peers:
        pl.semaphore_signal(sem, inc=1, device_id={"ctx": peer}, device_id_type=pl.DeviceIdType.MESH)
    pl.semaphore_wait(sem, ctx - 1)
    copies = []
    for k, peer in enumerate(peers):
        copy = remote(dkv.at[pl.ds(pl.multiple_of(peer * rows, BLK), rows)], land.at[y], ssem.at[k], rsem.at[y], {"ctx": peer})
        copy.start()
        copies.append(copy)

    def own_kv():
        total = dkv[pl.ds(pl.multiple_of(y * rows, BLK), rows)].astype(F32)
        for peer in peers:
            remote(land.at[peer], land.at[peer], ssem.at[0], rsem.at[peer], {"ctx": peer}).wait_recv()
            total = total + land[peer].astype(F32)
        return total.astype(BF)

    last(ctx, table, y, dq, own_kv, h1, tok, wall, dx1, vec, gvec, gq, gtok)
    for copy in copies:
        copy.wait_send()


def last_call(tbl, dq, dkv, h1, tok, wall, dx1, vec, gvec, ctx, head):
    rows, width = h1.shape
    dp, r = wall.shape[:2]
    return pl.pallas_call(
        functools.partial(last_kernel, ctx),
        out_shape=(shape(dp, r, head), shape(rows, width)),
        in_specs=[SM] + [VM] * 8, out_specs=(VM,) * 2,
        scratch_shapes=[pltpu.VMEM((ctx, rows, 2 * width), BF), DMA((ctx,)), DMA((ctx,))],
        compiler_params=params(62, collective_id=2, has_side_effects=True), name="last",
    )(tbl, dq, dkv, h1, tok, wall, dx1, vec, gvec)


class Reduce:
    def __init__(self, at, g, a_core, a_x, a_z, a_y, sems):
        self.at, self.g = at, g
        self.a_core, self.a_x, self.a_z, self.a_y = a_core, a_x, a_z, a_y
        self.s1, self.r1, self.s2, self.r2, self.s3, self.r3, self.s4, self.r4 = sems
        self.mate = {"dp": at.dp_at(at.z, at.x, 1 - at.c)}
        self.across = {"dp": at.dp_at(at.z, 1 - at.x, at.c)}

    def to_core(self, p, cols, held=None):
        return remote(self.g.at[:, :, 1 - self.at.c, :, cols if held is None else held], self.a_core.at[:, :, :, cols],
                      self.s1.at[p], self.r1.at[p], self.mate)

    def to_x(self, p, cols):
        return remote(self.a_core.at[:, 1 - self.at.x, :, cols], self.a_x.at[:, :, cols],
                      self.s2.at[p], self.r2.at[p], self.across)

    def to_z(self, p, cols, k):
        at = self.at
        return remote(self.a_core.at[at.z_at(k), at.x, :, cols], self.a_z.at[k - 1, :, cols],
                      self.s3.at[p, k - 1], self.r3.at[p, k - 1], {"dp": at.dp_at(at.z_at(k), at.x, at.c)})

    def to_y(self, p, cols, k):
        at = self.at
        return remote(self.a_core.at[at.z, at.x, :, cols], self.a_y.at[k - 1, :, cols],
                      self.s4.at[p, k - 1], self.r4.at[p, k - 1], {"ctx": at.y_at(k)})

    def level1(self, p, cols, held=None):
        self.to_core(p, cols, held).start()

    def level2(self, p, cols, held=None):
        self.to_core(p, cols, held).wait_recv()
        own = self.g[:, :, self.at.c, :, cols if held is None else held]
        self.a_core[:, :, :, cols] = self.a_core[:, :, :, cols] + own
        self.to_x(p, cols).start()

    def level3(self, p, cols):
        at = self.at
        self.to_x(p, cols).wait_recv()
        self.a_core[:, at.x, :, cols] = self.a_core[:, at.x, :, cols] + self.a_x[:, :, cols]
        for k in near_first(at.lines):
            self.to_z(p, cols, k).start()

    def level4(self, p, cols):
        at = self.at
        total = self.a_core[at.z, at.x, :, cols].astype(F32)
        for k in near_first(at.lines):
            self.to_z(p, cols, k).wait_recv()
            total = total + self.a_z[k - 1, :, cols].astype(F32)
        self.a_core[at.z, at.x, :, cols] = total.astype(BF)
        for k in range(1, at.ctx):
            self.to_y(p, cols, k).start()

    def level5(self, p, cols):
        at = self.at
        total = self.a_core[at.z, at.x, :, cols].astype(F32)
        for k in range(1, at.ctx):
            self.to_y(p, cols, k).wait_recv()
            total = total + self.a_y[k - 1, :, cols].astype(F32)
        return total

    def finish(self, p, cols, core=True, held=None):
        at = self.at
        if core:
            self.to_core(p, cols, held).wait_send()
        self.to_x(p, cols).wait_send()
        for k in range(1, at.lines):
            self.to_z(p, cols, k).wait_send()
        for k in range(1, at.ctx):
            self.to_y(p, cols, k).wait_send()


def backward_kernel(dp, ctx, tbl, tok, att, cot, q, kv, h1t, lse, vec, bup, wall,
                    out, gtok, o_small, o_qkv, o_out, o_up, o_down,
                    x1, acc, dh2, da, delta, dq, dk_acc, dv_acc, send, recv, dqkv, gup, rows,
                    wub, wdb, g, a_core, a_x, a_z, a_y, wsem, ys, yr, *sems):
    at = Spot(dp, ctx)
    width = tok.shape[1]
    r = wall.shape[1]
    nd = dp // 4
    chunk = 4 * nd * r
    off_out = 128 + 3 * width
    off_up = off_out + width
    off_down = off_up + 4 * chunk
    table = Table(tbl, 2 * ctx, at.y, True)
    red = Reduce(at, g, a_core, a_x, a_z, a_y, sems)
    lines = at.lines
    last_t = 9
    actb, dub, h2 = dqkv.at[0], dqkv.at[1], dqkv.at[2]

    def cols_of(p):
        return pl.ds(pl.multiple_of(p * width, 128), width)

    def cols_q(hp):
        return pl.ds(pl.multiple_of(last_t * width + hp * 3 * LANES, 128), 3 * LANES)

    def held_q(hp):
        return pl.ds(pl.multiple_of(last_t * width + 128 + lax.rem(hp, 3) * 3 * LANES, 128), 3 * LANES)

    cols_small = pl.ds(last_t * width + 3 * width, 128)
    held_small = pl.ds(last_t * width, 128)

    def up_copy(f, slot):
        return pltpu.make_async_copy(wall.at[:, :, pl.ds(pl.multiple_of(off_up + f * chunk, 128), chunk)],
                                     wub.at[slot], wsem.at[0, slot])

    def down_copy(f, slot, j):
        return pltpu.make_async_copy(wall.at[pl.ds(f * nd, nd), :, pl.ds(off_down + j * width, width)],
                                     wdb.at[slot, :, j], wsem.at[1 + j, slot])

    def plain_copy(i, slot):
        return pltpu.make_async_copy(wall.at[:, :, pl.ds(128 + i * width, width)], wub.at[slot], wsem.at[5, slot])

    def fetch(f, slot):
        up_copy(f, slot).start()
        for j in range(4):
            down_copy(f, slot, j).start()

    plain_copy(3, 2).start()
    fetch(0, 0)
    at.barrier()
    plain_copy(3, 2).wait()
    w_out = wub[2].reshape(width, width)
    halves = [pl.ds(i * BLK, BLK) for i in range(2)]
    for i, half in enumerate(halves):
        mid = tok[half].astype(F32) + (dot(att[table.slot_of[i]], w_out) + vec[4:5])
        x1[half] = mid
        low = (normed(mid)[0] * vec[5:6] + vec[6:7]).astype(BF)
        h2[half] = low
        acc[half] = mid + vec[7:8]
        dh2[half] = jnp.zeros((BLK, width), F32)

    def part(f, carry):
        slot = lax.rem(f, 2)

        @pl.when(f < 3)
        def _():
            fetch(f + 1, 1 - slot)

        up_copy(f, slot).wait()
        for j in range(4):
            down_copy(f, slot, j).wait()
        w_up = wub[slot].reshape(width, chunk)
        w_down = wdb[slot].reshape(chunk, width)
        hid = pl.ds(pl.multiple_of(f * chunk, 128), chunk)
        bias = bup[:, hid]
        sums = jnp.zeros((1, chunk), F32)
        for half in halves:
            u = dot(h2[half], w_up) + bias
            sq = u * u
            t = jnp.tanh(u * (0.7978845608028654 + 0.03567740813636141 * sq))
            act = (0.5 * u * (1.0 + t)).astype(BF)
            actb[half] = act
            slope = 0.5 * (1.0 + t) + 0.5 * u * (1.0 - t * t) * (0.7978845608028654 + 0.10703222440908423 * sq)
            acc[half] += dot(act, w_down)
            dul = (slope * dot_t(cot[half], w_down)).astype(BF)
            dub[half] = dul
            sums = sums + jnp.sum(dul.astype(F32), axis=0, keepdims=True)
            dh2[half] += dot_t(dul, w_up)
        gup[:, hid] = sums
        g[:, :, :, :, cols_of(f)] = dot_l(h2[...], dub[...]).astype(BF).reshape(lines, 2, 2, r, chunk)
        red.level1(f, cols_of(f))
        g_down = dot_l(actb[...], cot[...]).astype(BF).reshape(nd // 4, 2, 2, 4, r, width)
        for j in range(4):
            g[pl.ds(f * (nd // 4), nd // 4), :, :, :, pl.ds((4 + j) * width, width)] = g_down[:, :, :, j]
        for lag, level in ((1, red.level2), (2, red.level3), (3, red.level4)):
            @pl.when(f >= lag)
            def _():
                level(f - lag, cols_of(f - lag))
        return carry

    lax.fori_loop(0, 4, part, 0)
    for p in range(4, 8):
        red.level1(p, cols_of(p))
    for i, half in enumerate(halves):
        out[half] = jnp.where(table.turned, acc[halves[1 - i]], acc[half]).astype(BF)
    rows[...] = jnp.zeros_like(rows)
    lane_head = lax.broadcasted_iota(jnp.int32, (16, width), 0)
    pick = (lax.broadcasted_iota(jnp.int32, (16, width), 1) // HD == lane_head).astype(F32)
    grad = None
    w_out = wub[2].reshape(width, width)
    for i, half in enumerate(halves):
        gf = cot[half].astype(F32)
        unit, inv = normed(x1[half])
        dy = dh2[half]
        mid_grad = gf + norm_back(dy, unit, inv, vec[5:6])
        acc[half] = mid_grad
        branch = mid_grad.astype(BF)
        rows[4:5] += jnp.sum(branch.astype(F32), axis=0, keepdims=True)
        rows[5:6] += jnp.sum(dy * unit, axis=0, keepdims=True)
        rows[6:7] += jnp.sum(dy, axis=0, keepdims=True)
        rows[7:8] += jnp.sum(gf, axis=0, keepdims=True)
        own = att[table.slot_of[i]]
        piece = dot_l(own, branch)
        grad = piece if grad is None else grad + piece
        back = dot_t(branch, w_out).astype(BF)
        da[half] = back
        delta[i] = lax.dot_general(pick, back.astype(F32) * own.astype(F32), (((1,), (1,)), ((), ())),
                                   precision=lax.Precision.HIGHEST, preferred_element_type=F32)
    g[:, :, :, :, cols_of(8)] = grad.astype(BF).reshape(lines, 2, 2, r, width)
    red.level1(8, cols_of(8))
    for i in range(3):
        plain_copy(i, i).start()
    red.level2(3, cols_of(3))
    red.level3(2, cols_of(2))
    red.level4(1, cols_of(1))

    def done_t(p):
        total = red.level5(p, cols_of(p))

        @pl.when(p < 4)
        def _():
            o_up[:, pl.ds(pl.multiple_of(jnp.minimum(p, 3) * width, 128), width)] = total

        @pl.when(p >= 4)
        def _():
            o_down[pl.ds(pl.multiple_of(jnp.clip(p - 4, 0, 3) * r, 8), r), :] = total

    done_t(jnp.int32(0))
    other = lax.rem(at.y + 1, 2)
    mate_y = {"ctx": other}

    def kv_copy(hp):
        return remote(send.at[hp], recv.at[hp], ys.at[hp], yr.at[hp], mate_y)

    def q_grad(hp):
        lanes = pl.ds(pl.multiple_of(hp * LANES, LANES), LANES)
        kv_copy(hp).wait_recv()
        for i in range(2):
            dqkv[1 + i, :, lanes] = (dqkv[1 + i, :, lanes].astype(F32)
                                     + recv[hp, :, i * LANES:(i + 1) * LANES].astype(F32)).astype(BF)
        low = jnp.concatenate([dqkv[i, :, lanes] for i in range(3)], axis=1)

        @pl.when(hp >= 3)
        def _():
            red.to_core(last_t + jnp.maximum(hp - 3, 0), cols_q(0), held_q(0)).wait_send()

        g[:, :, :, :, held_q(hp)] = dot(h1t[...], low).astype(BF).reshape(lines, 2, 2, r, 3 * LANES)
        red.level1(last_t + hp, cols_q(hp), held_q(hp))

    def done_q(hp):
        total = red.level5(last_t + hp, cols_q(hp))
        for i in range(3):
            o_qkv[:, pl.ds(pl.multiple_of(i * width + hp * LANES, LANES), LANES)] = total[:, i * LANES:(i + 1) * LANES]

    def level_q(level, hp):
        if level == red.level2:
            level(last_t + hp, cols_q(hp), held_q(hp))
        else:
            level(last_t + hp, cols_q(hp))

    outermost = table.block[0] == 0

    def pair(hp, carry):
        def put_dq(slot, value):
            dq[slot] = value

        attend_back_pair(hp, table, q, kv, da, lse, delta, put_dq, dk_acc, dv_acc, width)
        lanes = pl.ds(pl.multiple_of(hp * LANES, LANES), LANES)
        for i, half in enumerate(halves):
            dqkv[0, half, lanes] = dq[i]
            outer, inner = (0, 1) if i == 0 else (3, 2)
            for n, sums in enumerate((dk_acc, dv_acc)):
                dqkv[1 + n, half, lanes] = jnp.where(outermost, sums[outer], sums[inner]).astype(BF)
                send[hp, half, n * LANES:(n + 1) * LANES] = jnp.where(outermost, sums[inner], sums[outer]).astype(BF)
        kv_copy(hp).start()

        @pl.when(hp < 5)
        def _():
            red.level2(4 + hp, cols_of(4 + hp))

        red.level3(3 + hp, cols_of(3 + hp))
        red.level4(2 + hp, cols_of(2 + hp))
        done_t(1 + hp)

        @pl.when(hp >= 2)
        def _():
            q_grad(hp - 2)

        for lag, level in ((3, red.level2), (4, red.level3), (5, red.level4)):
            @pl.when(hp >= lag)
            def _():
                level_q(level, hp - lag)
        return carry

    lax.fori_loop(0, PAIRS, pair, 0)
    for i in range(3):
        plain_copy(i, i).wait()
    red.level4(8, cols_of(8))
    done_t(jnp.int32(7))
    q_grad(jnp.int32(4))
    level_q(red.level2, 3)
    level_q(red.level3, 2)
    level_q(red.level4, 1)
    o_out[...] = red.level5(8, cols_of(8))
    done_q(0)
    q_grad(jnp.int32(5))
    level_q(red.level2, 4)
    level_q(red.level3, 3)
    level_q(red.level4, 2)
    done_q(1)
    for i in range(3):
        piece = dot_t(dqkv[i], wub[i].reshape(width, width))
        if i == 0:
            dh2[...] = piece
        else:
            dh2[...] += piece
    level_q(red.level2, 5)
    level_q(red.level3, 4)
    level_q(red.level4, 3)
    for half in halves:
        dy = dh2[half]
        unit, inv = normed(tok[half].astype(F32))
        acc[half] += norm_back(dy, unit, inv, vec[0:1])
        rows[0:1] += jnp.sum(dy * unit, axis=0, keepdims=True)
        rows[1:2] += jnp.sum(dy, axis=0, keepdims=True)
        rows[2:3] += jnp.sum(dqkv[0, half].astype(F32), axis=0, keepdims=True)
        rows[3:4] += jnp.sum(dqkv[2, half].astype(F32), axis=0, keepdims=True)
    for i, half in enumerate(halves):
        gtok[half] = jnp.where(table.turned, acc[halves[1 - i]], acc[half]).astype(BF)
    small = jnp.transpose(rows[...])
    lane = lax.broadcasted_iota(jnp.int32, small.shape, 1)
    tall = jnp.transpose(jnp.broadcast_to(gup[...], (8, 4 * chunk))).reshape(dp, 4, r, 8)
    for j in range(4):
        small = jnp.where(lane == 8 + j, tall[:, j].reshape(width, 8)[:, 0:1], small)
    g[:, :, :, :, held_small] = small.astype(BF).reshape(lines, 2, 2, r, 128)
    red.level1(last_t + 6, cols_small, held_small)
    level_q(red.level3, 5)
    red.level2(last_t + 6, cols_small, held_small)
    level_q(red.level4, 4)
    done_q(2)
    done_q(3)
    red.level3(last_t + 6, cols_small)
    level_q(red.level4, 5)
    red.level4(last_t + 6, cols_small)
    done_q(4)
    done_q(5)
    o_small[...] = red.level5(last_t + 6, cols_small)
    for p in range(last_t):
        red.finish(p, cols_of(p))
    for hp in range(PAIRS):
        red.finish(last_t + hp, cols_q(hp), hp >= 3, held_q(hp))
        kv_copy(hp).wait_send()
    red.finish(last_t + 6, cols_small, True, held_small)


def backward(tbl, tok, att, cot, q, kv, h1t, lse, vec, bup, wall, ctx):
    rows, width = tok.shape
    dp, r, full = wall.shape
    lines, nd = dp // 4, dp // 4
    chunk = 4 * nd * r
    V = pltpu.VMEM
    return pl.pallas_call(
        functools.partial(backward_kernel, dp, ctx),
        out_shape=(shape(rows, width), shape(rows, width), shape(r, 128, dtype=F32), shape(r, 3 * width, dtype=F32),
                   shape(r, width, dtype=F32), shape(r, 4 * chunk, dtype=F32), shape(4 * r, width, dtype=F32)),
        in_specs=[SM] + [VM] * 9 + [ANY], out_specs=(VM,) * 7,
        scratch_shapes=[V((rows, width), F32), V((rows, width), F32), V((rows, width), F32), V((rows, width), BF),
                        V((2, 16, BLK), F32),
                        V((2, BLK, LANES), BF), V((2 * ctx, BLK, LANES), F32), V((2 * ctx, BLK, LANES), F32),
                        V((PAIRS, rows, 2 * LANES), BF), V((PAIRS, rows, 2 * LANES), BF), V((3, rows, width), BF),
                        V((1, 4 * chunk), F32), V((128, width), F32),
                        V((3, dp, r, chunk), BF), V((2, nd, 4, r, width), BF),
                        V((lines, 2, 2, r, 9 * width + 128 + 9 * LANES), BF), V((lines, 2, r, full), BF), V((lines, r, full), BF),
                        V((lines - 1, r, full), BF), V((ctx - 1, r, full), BF),
                        DMA((6, 3)), DMA((PAIRS,)), DMA((PAIRS,)),
                        DMA((16,)), DMA((16,)), DMA((16,)), DMA((16,)), DMA((16, lines - 1)), DMA((16, lines - 1)),
                        DMA((16, ctx - 1)), DMA((16, ctx - 1))],
        compiler_params=pltpu.CompilerParams(vmem_limit_bytes=67043328, collective_id=3, has_side_effects=True),
        name="backward",
    )(tbl, tok, att, cot, q, kv, h1t, lse, vec, bup, wall)


def finish_kernel(count, *refs):
    ins, small, outs = refs[:count], refs[count], refs[count + 1:2 * count + 1]
    vectors, rest = refs[2 * count + 1:2 * count + 10], refs[2 * count + 10:]
    held, fetched, given = rest[:count], rest[count], rest[count + 1]

    def fetch(i):
        return pltpu.make_async_copy(ins[i], held[i], fetched.at[i])

    def give(i):
        return pltpu.make_async_copy(held[i], outs[i], given.at[i])

    for i in range(count):
        fetch(i).start()
    r = small.shape[0]
    total = jnp.transpose(jnp.concatenate([small[...], jnp.zeros((128 - r, 128), F32)], axis=0))
    for i in range(8):
        vectors[i][...] = total[i:i + 1, 0:r].reshape(r)
    vectors[8][...] = jnp.concatenate([total[8 + j:9 + j, 0:r] for j in range(4)], axis=1).reshape(4 * r)
    for i in range(count):
        fetch(i).wait()
        give(i).start()
    for i in range(count):
        give(i).wait()


def finish(results, small):
    count, r = len(results), small.shape[0]
    outs = tuple(jax.ShapeDtypeStruct(a.shape, a.dtype) for a in results)
    return pl.pallas_call(
        functools.partial(finish_kernel, count),
        out_shape=outs + (shape(r, dtype=F32),) * 8 + (shape(4 * r, dtype=F32),),
        in_specs=[HBM] * count + [VM], out_specs=(HBM,) * count + (VM,) * 9,
        scratch_shapes=[pltpu.VMEM(a.shape, a.dtype) for a in results] + [DMA((count,)), DMA((count,))],
        compiler_params=pltpu.CompilerParams(vmem_limit_bytes=67043328), name="finish",
    )(*results, small)


def shards(tokens, block_table, ln1_gain, ln1_bias, w_qkv, bias_query, bias_value, w_out, bias_out,
           ln2_gain, ln2_bias, w_up, bias_up, w_down, bias_down, cotangent):
    dp, ctx = lax.axis_size("dp"), lax.axis_size("ctx")
    width, hidden = tokens.shape[2], w_up.shape[1]
    r = w_qkv.shape[0]
    head = 128 + 3 * width
    third = (width + 2 * hidden) // 3
    off_up = head + width
    off_down = off_up + hidden
    vectors = [ln1_gain, ln1_bias, bias_query, bias_value, bias_out, ln2_gain, ln2_bias, bias_down]
    if ctx == 2 and dp == 16:
        wall, tok, cot, h1, q, kv, att, lse, vec, bup = front(
            block_table, tokens[0], cotangent[0], vectors, bias_up, (w_qkv, w_out, w_up, w_down), dp, ctx)
        out, gtok, g_small, g_qkv, g_out, g_up, g_down = backward(
            block_table, tok, att, cot, q, kv, h1, lse, vec, bup, wall, ctx)
        out, gtok, g_qkv, g_out, g_up, g_down, *rows = finish((out, gtok, g_qkv, g_out, g_up, g_down), g_small)
        return (out[None], gtok[None], rows[0], rows[1], g_qkv, rows[2], rows[3], g_out, rows[4], rows[5], rows[6],
                g_up, rows[8], g_down, rows[7])
    small = jnp.concatenate([jnp.stack(vectors), bias_up.reshape(4, r), jnp.zeros((116, r), BF)]).T
    cat = jnp.concatenate([small, w_qkv, w_out, w_up] + [w_down[j * r:(j + 1) * r] for j in range(4)], axis=1)
    tok_all, wall = gather(tokens[0], cat, dp, ctx, head, third)
    h1, q, kv, att, lse, vec = attend(block_table, tok_all, wall, ctx)
    bup = vec[8:12].reshape(4, dp, r).transpose(1, 0, 2).reshape(1, hidden)
    out, gt, da, dx1, delta, gvec, gup = feed_call(block_table, tokens[0], att, wall, cotangent[0], vec, bup,
                                                   ctx, off_up, off_down, 3 * third)
    dq, dkv = attend_back(block_table, q, kv, da, lse, delta, ctx)
    gvec = gvec.at[8:12].set(gup.reshape(dp, 4, r).transpose(1, 0, 2).reshape(4, width))
    gq, gtok = last_call(block_table, dq, dkv, h1, tokens[0], wall, dx1, vec, gvec, ctx, head)
    total = scatter(gq, gt, dp, ctx, head, third)
    rows = total[:, 0:128].T
    g_down = jnp.concatenate([total[:, off_down + j * width:off_down + (j + 1) * width] for j in range(4)], axis=0)
    return (out[None], gtok[None], rows[0], rows[1], total[:, 128:head], rows[2], rows[3],
            total[:, head:off_up], rows[4], rows[5], rows[6], total[:, off_up:off_down],
            rows[8:12].reshape(4 * r), g_down, rows[7])


def solution(mesh):
    row, mat = P("dp"), P("dp", None)
    act = P("dp", "ctx", None)
    in_specs = (act, P(), row, row, mat, row, row, mat, row, row, row, mat, row, mat, row, act)
    out_specs = (act, act, row, row, mat, row, row, mat, row, row, row, mat, row, mat, row)
    return jax.shard_map(shards, mesh=mesh, in_specs=in_specs, out_specs=out_specs, check_vma=False)
```

```python
import functools
import jax
import jax.numpy as jnp
from jax import lax
from jax.experimental import pallas as pl
from jax.experimental.pallas import tpu as pltpu
from jax.sharding import PartitionSpec as P

ANY = pl.BlockSpec(memory_space=pl.ANY)
VM = pl.BlockSpec(memory_space=pltpu.VMEM)
HBM = pl.BlockSpec(memory_space=pltpu.HBM)
DMA = pltpu.SemaphoreType.DMA


def near_first(count):
    order = []
    for step in range(1, count):
        order.append((step + 1) // 2 if step % 2 else count - step // 2)
    return order


class Spot:
    def __init__(self, dp, ctx):
        self.dp, self.ctx = dp, ctx
        self.lines = dp // 4
        me = lax.axis_index("dp")
        self.y = lax.axis_index("ctx")
        self.z = me // 4
        self.x = (me // 2) % 2
        self.c = me % 2
        self.me = me

    def dp_at(self, z, x, c):
        return (z * 2 + x) * 2 + c

    def z_at(self, k):
        return lax.rem(self.z + k, self.lines)

    def y_at(self, k):
        return lax.rem(self.y + k, self.ctx)

    def barrier(self):
        sem = pltpu.get_barrier_semaphore()
        peers = [{"dp": self.dp_at(self.z_at(k), self.x, self.c)} for k in range(1, self.lines)]
        peers.append({"dp": self.dp_at(self.z, 1 - self.x, self.c)})
        peers.append({"dp": self.dp_at(self.z, self.x, 1 - self.c)})
        peers += [{"ctx": self.y_at(k)} for k in range(1, self.ctx)]
        for peer in peers:
            pl.semaphore_signal(sem, inc=1, device_id=peer, device_id_type=pl.DeviceIdType.MESH)
        pl.semaphore_wait(sem, len(peers))


def remote(src, dst, ssem, rsem, device):
    return pltpu.make_async_remote_copy(
        src_ref=src, dst_ref=dst, send_sem=ssem, recv_sem=rsem,
        device_id=device, device_id_type=pl.DeviceIdType.MESH,
    )


def gather_kernel(dp, ctx, head, third, tok_ref, cat_ref, tok_all, wall,
                  loc, st, rt, sz, rz, sx, rx, sy, ry, sc, rc):
    at = Spot(dp, ctx)
    lines = at.lines
    ky = at.y % 2
    mine = pl.multiple_of(head + third + ky * third, 128)
    other = pl.multiple_of(head + third + (1 - ky) * third, 128)
    cols = {"q": pl.ds(0, head), "m": pl.ds(mine, third), "t": pl.ds(head, third), "o": pl.ds(other, third)}
    num = {"q": 0, "m": 1, "t": 2, "o": 3}
    own = at.me
    mate = {"dp": at.dp_at(at.z, at.x, 1 - at.c)}
    across = {"dp": at.dp_at(at.z, 1 - at.x, at.c)}
    pair = {"ctx": at.y + 1 - 2 * ky}
    at.barrier()
    copies = []

    def go(copy):
        copy.start()
        copies.append(copy)

    local = [pltpu.make_async_copy(cat_ref, wall.at[own], loc.at[0]),
             pltpu.make_async_copy(tok_ref, tok_all.at[at.y], loc.at[1])]
    for copy in local:
        copy.start()

    def block(b, z, x, c):
        return wall.at[at.dp_at(z, x, c), :, cols[b]]

    def own_block(b):
        return cat_ref.at[:, cols[b]]

    def send_z(b):
        for k in near_first(lines):
            go(remote(own_block(b), block(b, at.z, at.x, at.c), sz.at[num[b], k], rz.at[num[b], at.z],
                      {"dp": at.dp_at(at.z_at(k), at.x, at.c)}))

    def send_x(b, z, k, src):
        go(remote(src, block(b, z, at.x, at.c), sx.at[num[b], k], rx.at[num[b], z], across))

    def send_c(b, z, x, k, kx, src):
        go(remote(src, block(b, z, x, at.c), sc.at[num[b], k, kx], rc.at[num[b], z, x], mate))

    def send_y(z, x, k, kx, src):
        go(remote(src, block("m", z, x, at.c), sy.at[k, kx], ry.at[z, x], pair))

    def got_z(b, k):
        z = at.z_at(k)
        remote(own_block(b), block(b, z, at.x, at.c), sz.at[num[b], 0], rz.at[num[b], z], across).wait_recv()

    def got_x(b, k):
        z = at.z_at(k)
        remote(own_block(b), block(b, z, 1 - at.x, at.c), sz.at[num[b], 0], rx.at[num[b], z], across).wait_recv()

    def got_y(k, kx):
        z, x = at.z_at(k), (at.x + kx) % 2
        remote(own_block("o"), block("o", z, x, at.c), sz.at[0, 0], ry.at[z, x], across).wait_recv()

    def got_c(b, k, kx):
        z, x = at.z_at(k), (at.x + kx) % 2
        remote(own_block(b), block(b, z, x, 1 - at.c), sz.at[0, 0], rc.at[num[b], z, x], across).wait_recv()

    order = [0] + near_first(lines)
    for k in range(1, ctx):
        go(remote(tok_ref, tok_all.at[at.y], st.at[k], rt.at[at.y], {"ctx": at.y_at(k)}))
    for b in ("q", "m", "t"):
        send_z(b)
    for b in ("q", "m", "t"):
        send_x(b, at.z, 0, own_block(b))
        send_c(b, at.z, at.x, 0, 0, own_block(b))
        for k in order[1:]:
            got_z(b, k)
            z = at.z_at(k)
            src = block(b, z, at.x, at.c)
            send_x(b, z, k, src)
            if b == "m":
                send_y(z, at.x, k, 0, src)
            send_c(b, z, at.x, k, 0, src)
        for k in order:
            got_x(b, k)
            z = at.z_at(k)
            src = block(b, z, 1 - at.x, at.c)
            if b == "m":
                send_y(z, 1 - at.x, k, 1, src)
            send_c(b, z, 1 - at.x, k, 1, src)
    send_c("o", at.z, at.x, 0, 0, own_block("o"))
    for kx in range(2):
        for k in order:
            if k == 0 and kx == 0:
                continue
            got_y(k, kx)
            z, x = at.z_at(k), (at.x + kx) % 2
            send_c("o", z, x, k, kx, block("o", z, x, at.c))
    for b in ("q", "m", "t", "o"):
        for kx in range(2):
            for k in order:
                got_c(b, k, kx)
    for k in range(1, ctx):
        y = at.y_at(k)
        remote(tok_ref, tok_all.at[y], st.at[0], rt.at[y], across).wait_recv()
    for copy in copies:
        copy.wait_send()
    for copy in local:
        copy.wait()


def gather(tok, cat, dp, ctx, head, third):
    lines = dp // 4
    rows, width = cat.shape
    return pl.pallas_call(
        functools.partial(gather_kernel, dp, ctx, head, third),
        out_shape=(jax.ShapeDtypeStruct((ctx, *tok.shape), tok.dtype),
                   jax.ShapeDtypeStruct((dp, rows, width), cat.dtype)),
        in_specs=[VM, VM], out_specs=(ANY, ANY),
        scratch_shapes=[DMA((2,)), DMA((ctx,)), DMA((ctx,)),
                        DMA((3, lines)), DMA((3, lines)), DMA((3, lines)), DMA((3, lines)),
                        DMA((lines, 2)), DMA((lines, 2)), DMA((4, lines, 2)), DMA((4, lines, 2))],
        compiler_params=pltpu.CompilerParams(collective_id=0, has_side_effects=True, vmem_limit_bytes=32 * 2**20),
    )(tok, cat)


def scatter_kernel(dp, ctx, head, third, gq, gt, out, a_core, a_pair, a_x, a_z, a_y, stage, total,
                   loc, s1, r1, s2, r2, s3, r3, s4, r4, s5, r5):
    at = Spot(dp, ctx)
    lines = at.lines
    rows = gq.shape[1]
    ky = at.y % 2
    mine = pl.multiple_of(head + third + ky * third, 128)
    other = pl.multiple_of(head + third + (1 - ky) * third, 128)
    cols = {"q": pl.ds(0, head), "m": pl.ds(mine, third), "t": pl.ds(head, third), "o": pl.ds(other, third)}
    size = {"q": head, "m": third, "t": third, "o": third}
    num = {"q": 0, "m": 1, "t": 2, "o": 3}
    mate = {"dp": at.dp_at(at.z, at.x, 1 - at.c)}
    across = {"dp": at.dp_at(at.z, 1 - at.x, at.c)}
    pair = {"ctx": at.y + 1 - 2 * ky}
    at.barrier()
    copies = []

    def go(copy):
        copy.start()
        copies.append(copy)

    first = {"m": pl.multiple_of(third + ky * third, 128), "o": pl.multiple_of(third + (1 - ky) * third, 128), "t": 0}

    def full(b, at_dp):
        if b == "q":
            return gq.at[at_dp]
        return gt.at[at_dp, :, pl.ds(first[b], third)]

    order = [0] + near_first(lines)
    order = order[::-1]
    spots = [(k, kx) for kx in (1, 0) for k in order]

    def where(k, kx):
        return at.z_at(k), (at.x + kx) % 2

    def land(ref, b, *idx):
        return ref.at[(num[b], *idx, slice(None), pl.ds(0, size[b]))]

    blocks = ("o", "m", "t", "q")
    for b in blocks:
        for k, kx in spots:
            z, x = where(k, kx)
            go(remote(full(b, at.dp_at(z, x, 1 - at.c)), land(a_core, b, z, x),
                      s1.at[num[b], k, kx], r1.at[num[b], z, x], mate))
    def fetch(b, k, kx):
        z, x = where(k, kx)
        return pltpu.make_async_copy(full(b, at.dp_at(z, x, at.c)), land(stage, b, z, x),
                                     loc.at[num[b], k, kx])
    for b in blocks:
        for k, kx in spots:
            fetch(b, k, kx).start()

    def take(sem, dst):
        remote(dst, dst, s1.at[0, 0, 0], sem, across).wait_recv()

    def added(b, k, kx):
        z, x = where(k, kx)
        fetch(b, k, kx).wait()
        here = land(a_core, b, z, x)
        take(r1.at[num[b], z, x], here)
        here[...] = here[...] + land(stage, b, z, x)[...]
        return here

    for b in blocks:
        if b == "o":
            for k, kx in spots:
                z, x = where(k, kx)
                go(remote(added(b, k, kx), a_pair.at[z, x], s2.at[k, kx], r2.at[z, x], pair))
            continue
        for k, kx in spots:
            z, x = where(k, kx)
            here = added(b, k, kx)
            if b == "m":
                take(r2.at[z, x], a_pair.at[z, x])
                here[...] = here[...] + a_pair[z, x]
            if kx == 1:
                go(remote(here, land(a_x, b, z), s3.at[num[b], k], r3.at[num[b], z], across))
        for k in order:
            z = at.z_at(k)
            here = land(a_core, b, z, at.x)
            take(r3.at[num[b], z], land(a_x, b, z))
            here[...] = here[...] + land(a_x, b, z)[...]
            if k:
                go(remote(here, land(a_z, b, at.z), s4.at[num[b], k], r4.at[num[b], at.z],
                          {"dp": at.dp_at(z, at.x, at.c)}))
    for b in ("m", "t", "q"):
        acc = land(a_core, b, at.z, at.x)[...].astype(jnp.float32)
        for k in near_first(lines):
            z = at.z_at(k)
            take(r4.at[num[b], z], land(a_z, b, z))
            acc = acc + land(a_z, b, z)[...].astype(jnp.float32)
        land(total, b)[...] = acc
        land(a_core, b, at.z, at.x)[...] = acc.astype(jnp.bfloat16)
        for k in range(1, ctx):
            go(remote(land(a_core, b, at.z, at.x), land(a_y, b, at.y), s5.at[num[b], k], r5.at[num[b], at.y],
                      {"ctx": at.y_at(k)}))
    outs = []
    for b in ("t", "q", "m", "o"):
        if b == "m":
            acc = land(total, b)[...]
        elif b == "o":
            acc = jnp.zeros((rows, third), jnp.float32)
        else:
            acc = land(total, b)[...]
        for k in range(1, ctx):
            y = at.y_at(k)
            if b in ("t", "q") or (b == "m" and k % 2 == 0):
                take(r5.at[num[b], y], land(a_y, b, y))
                acc = acc + land(a_y, b, y)[...].astype(jnp.float32)
            elif b == "o" and k % 2 == 1:
                here = a_y.at[1, y, :, pl.ds(0, third)]
                take(r5.at[1, y], here)
                acc = acc + here[...].astype(jnp.float32)
        land(total, b)[...] = acc
        copy = pltpu.make_async_copy(land(total, b), out.at[:, cols[b]], loc.at[num[b], 0, 0])
        copy.start()
        outs.append(copy)
    for copy in copies:
        copy.wait_send()
    for copy in outs:
        copy.wait()


def scatter(gq, gt, dp, ctx, head, third):
    lines = dp // 4
    _, rows, width = gq.shape[0], gq.shape[1], gq.shape[2] + gt.shape[2]
    bf, f32 = jnp.bfloat16, jnp.float32
    return pl.pallas_call(
        functools.partial(scatter_kernel, dp, ctx, head, third),
        out_shape=jax.ShapeDtypeStruct((rows, width), f32),
        in_specs=[ANY, ANY], out_specs=ANY,
        scratch_shapes=[pltpu.VMEM((4, lines, 2, rows, head), bf), pltpu.VMEM((lines, 2, rows, third), bf),
                        pltpu.VMEM((3, lines, rows, head), bf), pltpu.VMEM((3, lines, rows, head), bf),
                        pltpu.VMEM((3, ctx, rows, head), bf), pltpu.VMEM((4, lines, 2, rows, head), bf),
                        pltpu.VMEM((4, rows, head), f32),
                        DMA((4, lines, 2)), DMA((4, lines, 2)), DMA((4, lines, 2)),
                        DMA((lines, 2)), DMA((lines, 2)),
                        DMA((3, lines)), DMA((3, lines)), DMA((3, lines)), DMA((3, lines)),
                        DMA((3, ctx)), DMA((3, ctx))],
        compiler_params=pltpu.CompilerParams(collective_id=1, has_side_effects=True, vmem_limit_bytes=60 * 2**20),
    )(gq, gt)


F32, BF = jnp.float32, jnp.bfloat16
HEADS, HD, BLK = 12, 64, 256
PAIRS, LANES = HEADS // 2, 2 * HD


def dot(a, b):
    return jnp.dot(a, b, preferred_element_type=F32)


def dot_t(a, b):
    return lax.dot_general(a, b, (((1,), (1,)), ((), ())), preferred_element_type=F32)


def dot_l(a, b):
    return lax.dot_general(a, b, (((0,), (0,)), ((), ())), preferred_element_type=F32)


def normed(x):
    centred = x - jnp.mean(x, axis=-1, keepdims=True)
    inv = lax.rsqrt(jnp.mean(centred * centred, axis=-1, keepdims=True) + 1e-05)
    return centred * inv, inv


def norm_back(dy, unit, inv, gain):
    dn = dy * gain
    return inv * (dn - jnp.mean(dn, axis=-1, keepdims=True) - unit * jnp.mean(dn * unit, axis=-1, keepdims=True))


class Table:
    def __init__(self, tbl, nb, y, ordered=False):
        self.nb, self.half = nb, nb // 2
        self.own = [tbl[2 * y], tbl[2 * y + 1]]
        self.turned = self.own[0] >= self.half
        first_high = self.turned.astype(jnp.int32)
        self.place = [first_high, 1 - first_high]
        self.row_of = [first_high, 1 - first_high]
        self.slot_of = [first_high, 1 - first_high]
        self.block = [jnp.minimum(self.own[0], self.own[1]), jnp.maximum(self.own[0], self.own[1])]
        self.tbl = tbl
        if ordered:
            self.row_of, self.slot_of, self.pos = [0, 1], [0, 1], list(range(nb))
            return
        self.pos = []
        for j in range(nb):
            at = jnp.int32(0)
            for p in range(nb):
                at = at + jnp.where(tbl[p] == j, p, 0)
            self.pos.append(at)

    def keys(self, slot):
        return self.half if slot == 0 else self.nb

    def masked(self, slot, j):
        return j >= 1 if slot == 0 else j > self.half


def rows_of(ref, *idx):
    value = ref[idx]
    return value.reshape(value.shape[0] * value.shape[1], value.shape[2])


def block_rows(i):
    return pl.ds(i * BLK if isinstance(i, int) else pl.multiple_of(i * BLK, BLK), BLK)


def lane_masks(rows):
    lane = lax.broadcasted_iota(jnp.int32, (rows, LANES), 1)
    return [lane < HD, lane >= HD]


def project(ctx, tok, wall, h1, q, kv, vec, y):
    gain, shift = vec[0:1], vec[1:2]
    width = tok.shape[2]
    zero = jnp.zeros((1, width), F32)
    kv_bias = jnp.concatenate([zero, vec[3:4]], axis=1)
    w_kv = rows_of(wall, slice(None), slice(None), slice(128 + width, 128 + 3 * width))

    def rows(r, carry):
        x = tok[r // 2, pl.ds(pl.multiple_of((r % 2) * BLK, BLK), BLK)].astype(F32)
        low = (normed(x)[0] * gain + shift).astype(BF)
        kv[pl.ds(pl.multiple_of(r * BLK, BLK), BLK)] = (dot(low, w_kv) + kv_bias).astype(BF)
        return carry

    lax.fori_loop(0, 2 * ctx, rows, 0)
    w_q = rows_of(wall, slice(None), slice(None), slice(128, 128 + width))

    def own(i, carry):
        at = pl.ds(pl.multiple_of(i * BLK, BLK), BLK)
        low = (normed(tok[y, at].astype(F32))[0] * gain + shift).astype(BF)
        h1[at] = low
        q[at] = ((dot(low, w_q) + vec[2:3]).astype(BF).astype(F32) * HD ** (-0.5)).astype(BF)
        return carry

    lax.fori_loop(0, 2, own, 0)


def attend_pair(hp, table, q, kv, att, lse_acc, width):
    lanes = pl.ds(pl.multiple_of(hp * LANES, LANES), LANES)
    v_lanes = pl.ds(pl.multiple_of(width + hp * LANES, LANES), LANES)
    masks = lane_masks(BLK)
    lane = lax.broadcasted_iota(jnp.int32, (BLK, LANES), 1)
    for slot in range(2):
        q2 = q[block_rows(table.row_of[slot]), lanes]
        spots = [block_rows(table.pos[j]) for j in range(table.keys(slot))]
        mixed = []
        for h in range(2):
            qm = jnp.where(masks[h], q2, jnp.zeros_like(q2))
            scores = []
            for j, at in enumerate(spots):
                s = dot_t(qm, kv[at, lanes])
                if table.masked(slot, j):
                    s = jnp.where(j <= table.block[slot], s, -1e30)
                scores.append(s)
            largest = functools.reduce(jnp.maximum, scores)
            largest = jnp.max(largest, axis=-1, keepdims=True)
            exps = [jnp.exp(s - largest) for s in scores]
            total = jnp.sum(functools.reduce(jnp.add, exps), axis=-1, keepdims=True)
            out = functools.reduce(jnp.add, [dot(e.astype(BF), kv[at, v_lanes]) for e, at in zip(exps, spots)])
            mixed.append(out / total)
            lse_acc[slot] = jnp.where(lane == 2 * hp + h, largest + jnp.log(total), lse_acc[slot])
        att[slot, :, lanes] = jnp.where(masks[0], mixed[0], mixed[1]).astype(BF)


def attend_back_pair(hp, table, q, kv, da, lse, delta, put_dq, dk_acc, dv_acc, width):
    lanes = pl.ds(pl.multiple_of(hp * LANES, LANES), LANES)
    v_lanes = pl.ds(pl.multiple_of(width + hp * LANES, LANES), LANES)
    masks = lane_masks(BLK)
    for slot in (1, 0):
        row = block_rows(table.row_of[slot])
        q2, da2 = q[row, lanes], da[row, lanes]
        dq_acc = None
        for h in range(2):
            qm = jnp.where(masks[h], q2, jnp.zeros_like(q2))
            dam = jnp.where(masks[h], da2, jnp.zeros_like(da2))
            lse_row = lse[slot, pl.ds(2 * hp + h, 1), :]
            delta_row = delta[table.row_of[slot], pl.ds(2 * hp + h, 1), :]
            for j in range(table.keys(slot)):
                at = block_rows(table.pos[j])
                k2, v2 = kv[at, lanes], kv[at, v_lanes]
                st = dot_t(k2, qm)
                if table.masked(slot, j):
                    st = jnp.where(j <= table.block[slot], st, -1e30)
                pt = jnp.exp(st - lse_row)
                dst = (pt * (dot_t(v2, dam) - delta_row)).astype(BF)
                dv, dk = dot(pt.astype(BF), dam), dot(dst, qm)
                if slot == 1 and h == 0:
                    dv_acc[j], dk_acc[j] = dv, dk
                else:
                    dv_acc[j] += dv
                    dk_acc[j] += dk
                part = dot_l(dst, jnp.where(masks[h], k2, jnp.zeros_like(k2)))
                dq_acc = part if dq_acc is None else dq_acc + part
        put_dq(slot, (dq_acc * HD ** (-0.5)).astype(BF))


def feed(nd, off_up, off_down, table, tok, att, wall, cot, vec, bup, out, gt, da, dx1, delta, gvec, gup,
         x1, h2, acc, dh2):
    rows, width = cot.shape
    dp, r = wall.shape[0], wall.shape[1]
    chunk = 4 * nd * r
    w_out = rows_of(wall, slice(None), slice(None), slice(off_up - width, off_up))
    for i in range(2):
        at = pl.ds(i * BLK, BLK)
        mid = tok[at].astype(F32) + (dot(att[table.slot_of[i]], w_out) + vec[4:5])
        x1[at] = mid
        h2[at] = (normed(mid)[0] * vec[5:6] + vec[6:7]).astype(BF)
        acc[at] = mid + vec[7:8]
    dh2[...] = jnp.zeros_like(dh2)
    g = cot[...]

    def part(f, carry):
        cols = pl.ds(pl.multiple_of(off_up + f * chunk, 128), chunk)
        w_up = rows_of(wall, slice(None), slice(None), cols)
        w_down = jnp.concatenate(
            [wall[f * nd + d, :, pl.ds(off_down + j * width, width)] for d in range(nd) for j in range(4)], axis=0)
        low = h2[...]
        u = dot(low, w_up) + bup[:, pl.ds(pl.multiple_of(f * chunk, 128), chunk)]
        sq = u * u
        t = jnp.tanh(u * (0.7978845608028654 + 0.03567740813636141 * sq))
        act = (0.5 * u * (1.0 + t)).astype(BF)
        slope = 0.5 * (1.0 + t) + 0.5 * u * (1.0 - t * t) * (0.7978845608028654 + 0.10703222440908423 * sq)
        acc[...] += dot(act, w_down)
        du = slope * dot_t(g, w_down)
        dul = du.astype(BF)
        gup[:, pl.ds(pl.multiple_of(f * chunk, 128), chunk)] = jnp.sum(dul.astype(F32), axis=0, keepdims=True)
        dh2[...] += dot_t(dul, w_up)
        g_up = dot_l(low, dul).astype(BF)
        gt[:, :, pl.ds(pl.multiple_of(width + f * chunk, 128), chunk)] = g_up.reshape(dp, r, chunk)
        g_down = dot_l(act, g).astype(BF)
        for d in range(nd):
            for j in range(4):
                piece = g_down[(4 * d + j) * r:(4 * d + j + 1) * r]
                gt[f * nd + d, :, pl.ds(width + off_down - off_up + j * width, width)] = piece
        return carry

    lax.fori_loop(0, dp // nd, part, 0)
    out[...] = acc[...].astype(BF)
    gf = g.astype(F32)
    unit, inv = normed(x1[...])
    dy = dh2[...]
    mid_grad = gf + norm_back(dy, unit, inv, vec[5:6])
    dx1[...] = mid_grad
    branch = mid_grad.astype(BF)
    gvec[...] = jnp.zeros_like(gvec)
    gvec[4:5] = jnp.sum(branch.astype(F32), axis=0, keepdims=True)
    gvec[5:6] = jnp.sum(dy * unit, axis=0, keepdims=True)
    gvec[6:7] = jnp.sum(dy, axis=0, keepdims=True)
    gvec[7:8] = jnp.sum(gf, axis=0, keepdims=True)
    head = lax.broadcasted_iota(jnp.int32, (16, width), 0)
    pick = (lax.broadcasted_iota(jnp.int32, (16, width), 1) // HD == head).astype(F32)
    grad = None
    for i in range(2):
        own = att[table.slot_of[i]]
        low = branch[i * BLK:(i + 1) * BLK]
        piece = dot_l(own, low)
        grad = piece if grad is None else grad + piece
        back = dot_t(low, w_out).astype(BF)
        da[pl.ds(i * BLK, BLK)] = back
        prod = back.astype(F32) * own.astype(F32)
        delta[i] = lax.dot_general(pick, prod, (((1,), (1,)), ((), ())), precision=lax.Precision.HIGHEST,
                                   preferred_element_type=F32)
    gt[:, :, 0:width] = grad.astype(BF).reshape(dp, r, width)


def last(ctx, table, y, dq, own_kv, h1, tok, wall, dx1, vec, gvec, gq, gtok):
    width = h1.shape[1]
    dp, r = wall.shape[0], wall.shape[1]
    w_q = rows_of(wall, slice(None), slice(None), slice(128, 128 + width))
    low = h1[...]
    dq_all = jnp.concatenate([dq[table.slot_of[0]], dq[table.slot_of[1]]], axis=0)
    gq[:, :, 128:128 + width] = dot_l(low, dq_all).astype(BF).reshape(dp, r, width)
    dh1 = dot_t(dq_all, w_q)
    dkv = own_kv()
    w_kv = rows_of(wall, slice(None), slice(None), slice(128 + width, 128 + 3 * width))
    gq[:, :, 128 + width:128 + 3 * width] = dot_l(low, dkv).astype(BF).reshape(dp, r, 2 * width)
    dh1 = dh1 + dot_t(dkv, w_kv)
    unit, inv = normed(tok[...].astype(F32))
    gtok[...] = (dx1[...] + norm_back(dh1, unit, inv, vec[0:1])).astype(BF)
    sums = [jnp.sum(dh1 * unit, axis=0, keepdims=True), jnp.sum(dh1, axis=0, keepdims=True),
            jnp.sum(dq_all.astype(F32), axis=0, keepdims=True),
            jnp.sum(dkv[:, width:].astype(F32), axis=0, keepdims=True)]
    table_rows = jnp.concatenate(sums + [gvec[4:16], jnp.zeros((112, width), F32)], axis=0)
    gq[:, :, 0:128] = jnp.transpose(table_rows).astype(BF).reshape(dp, r, 128)


SM = pl.BlockSpec(memory_space=pltpu.SMEM)


def params(limit, **more):
    return pltpu.CompilerParams(vmem_limit_bytes=limit * 2**20, **more)


def shape(*dims, dtype=BF):
    return jax.ShapeDtypeStruct(dims, dtype)


def attend_kernel(ctx, tbl, tok, wall, h1, q, kv, att, lse, vec, lse_acc):
    width = tok.shape[2]
    y = lax.axis_index("ctx")
    table = Table(tbl, 2 * ctx, y)
    small = rows_of(wall, slice(None), slice(None), slice(0, 128)).astype(F32)
    vec[...] = jnp.transpose(small)[0:16]
    project(ctx, tok, wall, h1, q, kv, vec, y)
    lse_acc[...] = jnp.zeros_like(lse_acc)

    def pair(hp, carry):
        attend_pair(hp, table, q, kv, att, lse_acc, width)
        return carry

    lax.fori_loop(0, PAIRS, pair, 0)
    for slot in range(2):
        lse[slot] = jnp.transpose(lse_acc[slot])[0:16]


def attend(tbl, tok_all, wall, ctx):
    rows, width = tok_all.shape[1:]
    return pl.pallas_call(
        functools.partial(attend_kernel, ctx),
        out_shape=(shape(rows, width), shape(rows, width), shape(ctx * rows, 2 * width), shape(2, BLK, width),
                   shape(2, 16, BLK, dtype=F32), shape(16, width, dtype=F32)),
        in_specs=[SM, VM, VM], out_specs=(VM,) * 6,
        scratch_shapes=[pltpu.VMEM((2, BLK, LANES), F32)],
        compiler_params=params(62), name="attend",
    )(tbl, tok_all, wall)


def front_kernel(dp, ctx, tbl, tok, cot, *rest):
    vectors, rest = rest[:8], rest[8:]
    (b_up, w_qkv, w_out, w_up, w_down,
     wall, tok_slots, cot_slots, h1, q, kv, att, lse, vec, bup,
     cat, small, tall, toks, wq, lse_acc, loc, st, rt, sz, rz, sx, rx, sy, ry, sc, rc) = rest
    at = Spot(dp, ctx)
    lines = at.lines
    r, full = cat.shape
    width = tok.shape[1]
    head = 128 + 3 * width
    size = (full - head) // 6
    ky = at.y
    mate = {"dp": at.dp_at(at.z, at.x, 1 - at.c)}
    across = {"dp": at.dp_at(at.z, 1 - at.x, at.c)}
    pair_y = {"ctx": 1 - ky}
    table = Table(tbl, 2 * ctx, at.y, True)
    order = [0] + near_first(lines)

    small[...] = jnp.zeros_like(small)
    for i, ref in enumerate(vectors):
        small[i:i + 1, 0:r] = ref[...].astype(F32).reshape(1, r)
    ups = b_up[...].astype(F32).reshape(1, 4 * r)
    for j in range(4):
        small[8 + j:9 + j, 0:r] = ups[:, j * r:(j + 1) * r]
    cat[:, 0:128] = jnp.transpose(small[...])[0:r].astype(BF)
    cat[:, 128:head] = w_qkv[...]
    cat[:, head:head + width] = w_out[...]
    cat[:, head + width:head + 5 * width] = w_up[...]
    for j in range(4):
        cat[:, head + (5 + j) * width:head + (6 + j) * width] = w_down[j * r:(j + 1) * r]
    at.barrier()

    def cols(p):
        if isinstance(p, int) and p >= 5:
            place = 2 * (p - 4) + 1 - ky
        else:
            n = p - 1
            place = (1 - n // 2) * (2 + 2 * n + ky) + (n // 2) * (n - 2)
        return pl.ds(pl.multiple_of(head + place * size, 128), size)

    def is_head(p):
        return isinstance(p, int) and p == 0

    def own_block(p):
        return cat.at[:, pl.ds(0, head)] if is_head(p) else cat.at[:, cols(p)]

    def block(p, z, x, c):
        return wq.at[at.dp_at(z, x, c)] if is_head(p) else wall.at[at.dp_at(z, x, c), :, cols(p)]

    def to_z(p, k):
        return remote(own_block(p), block(p, at.z, at.x, at.c), sz.at[p, k], rz.at[p, at.z],
                      {"dp": at.dp_at(at.z_at(k), at.x, at.c)})

    def to_x(p, k):
        z = at.z_at(k)
        src = own_block(p) if k == 0 else block(p, z, at.x, at.c)
        return remote(src, block(p, z, at.x, at.c), sx.at[p, k], rx.at[p, z], across)

    def to_c(p, k, kx):
        z, x = at.z_at(k), (at.x + kx) % 2
        src = own_block(p) if k == 0 and kx == 0 else block(p, z, x, at.c)
        return remote(src, block(p, z, x, at.c), sc.at[p, k, kx], rc.at[p, z, x], mate)

    def to_y(p, k, kx):
        z, x = at.z_at(k), (at.x + kx) % 2
        n = p - 1
        here = block(p, z, x, at.c)
        return remote(here, here, sy.at[n, k, kx], ry.at[n, z, x], pair_y)

    def got(p, z, x, c, sem):
        here = block(p, z, x, c)
        remote(here, here, st, sem, across).wait_recv()

    def stage_z(p, shared):
        for k in order:
            if k:
                got(p, at.z_at(k), at.x, at.c, rz.at[p, at.z_at(k)])
                to_x(p, k).start()
                if shared is not None:
                    pl.when(shared)(lambda: to_y(p, k, 0).start())
                to_c(p, k, 0).start()

    def stage_x(p, shared):
        for k in order:
            got(p, at.z_at(k), 1 - at.x, at.c, rx.at[p, at.z_at(k)])
            if shared is not None:
                pl.when(shared)(lambda: to_y(p, k, 1).start())
            to_c(p, k, 1).start()

    def stage_y(n):
        p = 5 + n
        for kx in range(2):
            for k in order:
                if k or kx:
                    z, x = at.z_at(k), (at.x + kx) % 2
                    got(p, z, x, at.c, ry.at[n, z, x])
                    to_c(p, k, kx).start()

    def stage_c(p):
        for kx in range(2):
            for k in order:
                z, x = at.z_at(k), (at.x + kx) % 2
                got(p, z, x, 1 - at.c, rc.at[p, z, x])

    low_end, high_end = (at.z == 0).astype(jnp.int32), (at.z == 3).astype(jnp.int32)
    nearest = [1 + 2 * high_end, 3 - low_end - high_end, 2 + low_end - high_end]
    tok_mate = remote(tok, toks.at[at.y], st, rt, pair_y)
    tok_own = pltpu.make_async_copy(tok, toks.at[at.y], loc.at[0])
    wall_own = pltpu.make_async_copy(cat.at[:, pl.ds(head, full - head)],
                                     wall.at[at.me, :, pl.ds(head, full - head)], loc.at[1])
    head_own = pltpu.make_async_copy(cat.at[:, pl.ds(0, head)], wq.at[at.me], loc.at[2])
    to_x(0, 0).start()
    for k in nearest:
        to_z(0, k).start()
    to_c(0, 0, 0).start()
    tok_mate.start()
    for copy in (tok_own, head_own, wall_own):
        copy.start()
    for p in range(1, 5):
        for k in nearest:
            to_z(p, k).start()
        to_x(p, 0).start()
    for p in range(1, 7):
        to_c(p, 0, 0).start()
    stage_z(0, None)
    stage_x(0, None)
    stage_c(0)
    head_own.wait()
    head_all = pltpu.make_async_copy(wq, wall.at[:, :, pl.ds(0, head)], loc.at[2])
    head_all.start()
    tok_own.wait()
    tok_mate.wait_recv()

    columns = jnp.transpose(rows_of(wq, slice(None), slice(None), slice(0, 128)).astype(F32))
    vec[...] = columns[0:16]
    for d in range(dp):
        for j in range(4):
            tall[(4 * d + j) * r:(4 * d + j + 1) * r] = jnp.broadcast_to(
                wq[d, :, 0:128].astype(F32)[:, 8 + j:9 + j], (r, 128))
    bup[...] = jnp.transpose(tall[...])[0:1]
    gain, shift = vec[0:1], vec[1:2]
    kv_bias = jnp.concatenate([jnp.zeros((1, width), F32), vec[3:4]], axis=1)

    def stored(i):
        return toks[i // 2, block_rows(i % 2)].astype(F32)

    for j in range(2 * ctx):
        here = stored(0)
        for i in range(1, 2 * ctx):
            here = jnp.where(tbl[i] == j, stored(i), here)
        low = (normed(here)[0] * gain + shift).astype(BF)
        kv[block_rows(j)] = (dot(low, rows_of(wq, slice(None), slice(None), slice(128 + width, head)))
                             + kv_bias).astype(BF)
    for i in range(2):
        def chosen(ref):
            a, b = ref[block_rows(i)].astype(F32), ref[block_rows(1 - i)].astype(F32)
            return jnp.where(table.turned, b, a)

        here = chosen(tok)
        low = (normed(here)[0] * gain + shift).astype(BF)
        h1[:, block_rows(i)] = jnp.transpose(low)
        w_q = rows_of(wq, slice(None), slice(None), slice(128, 128 + width))
        q[block_rows(i)] = ((dot(low, w_q) + vec[2:3]).astype(BF).astype(F32) * HD ** (-0.5)).astype(BF)
        tok_slots[block_rows(i)] = here.astype(BF)
        cot_slots[block_rows(i)] = chosen(cot).astype(BF)
    lse_acc[...] = jnp.zeros_like(lse_acc)

    def heads(hp, carry):
        attend_pair(hp, table, q, kv, att, lse_acc, width)
        return carry

    def stages(t, carry):
        @pl.when(t < 4)
        def _():
            stage_z(t + 1, t < 2)

        @pl.when(t >= 1)
        def _():
            stage_x(t, t < 3)

        lax.fori_loop(jnp.minimum(2 * t, PAIRS), jnp.minimum(2 * t + 2, PAIRS), heads, 0)
        return carry

    lax.fori_loop(0, 5, stages, 0)
    for slot in range(2):
        lse[slot] = jnp.transpose(lse_acc[slot])[0:16]
    stage_y(0)
    stage_y(1)
    for p in range(1, 7):
        stage_c(p)
    for p in range(5):
        for k in order:
            to_x(p, k).wait_send()
            if k:
                to_z(p, k).wait_send()
    for p in range(7):
        for kx in range(2):
            for k in order:
                to_c(p, k, kx).wait_send()
                if p in (1, 2) and (k or kx):
                    to_y(p, k, kx).wait_send()
    tok_mate.wait_send()
    wall_own.wait()
    head_all.wait()


def front(tbl, tok, cot, vectors, b_up, weights, dp, ctx):
    rows, width = tok.shape
    r = weights[0].shape[0]
    head = 128 + 3 * width
    full = head + 9 * width
    lines = dp // 4
    V = pltpu.VMEM
    return pl.pallas_call(
        functools.partial(front_kernel, dp, ctx),
        out_shape=(shape(dp, r, full), shape(rows, width), shape(rows, width), shape(width, rows), shape(rows, width),
                   shape(ctx * rows, 2 * width), shape(2, BLK, width), shape(2, 16, BLK, dtype=F32),
                   shape(16, width, dtype=F32), shape(1, 4 * width, dtype=F32)),
        in_specs=[SM] + [VM] * (2 + len(vectors) + 1 + len(weights)), out_specs=(ANY,) + (VM,) * 9,
        scratch_shapes=[V((r, full), BF), V((128, 128), F32), V((4 * width, 128), F32), V((ctx, rows, width), BF), V((dp, r, head), BF),
                        V((2, BLK, LANES), F32), DMA((3,)), DMA, DMA,
                        DMA((5, lines)), DMA((5, lines)), DMA((5, lines)), DMA((5, lines)),
                        DMA((2, lines, 2)), DMA((2, lines, 2)), DMA((7, lines, 2)), DMA((7, lines, 2))],
        compiler_params=params(62, collective_id=0, has_side_effects=True), name="front",
    )(tbl, tok, cot, *vectors, b_up, *weights)


def feed_kernel(ctx, nd, off_up, off_down, tbl, tok, att, wall, cot, vec, bup, *rest):
    table = Table(tbl, 2 * ctx, lax.axis_index("ctx"))
    feed(nd, off_up, off_down, table, tok, att, wall, cot, vec, bup, *rest)


def feed_call(tbl, tok, att, wall, cot, vec, bup, ctx, off_up, off_down, gt_cols):
    rows, width = cot.shape
    dp, r = wall.shape[:2]
    return pl.pallas_call(
        functools.partial(feed_kernel, ctx, dp // 4, off_up, off_down),
        out_shape=(shape(rows, width), shape(dp, r, gt_cols), shape(rows, width), shape(rows, width, dtype=F32),
                   shape(2, 16, BLK, dtype=F32), shape(16, width, dtype=F32), shape(1, bup.shape[1], dtype=F32)),
        in_specs=[SM] + [VM] * 6, out_specs=(VM,) * 7,
        scratch_shapes=[pltpu.VMEM((rows, width), F32), pltpu.VMEM((rows, width), BF),
                        pltpu.VMEM((rows, width), F32), pltpu.VMEM((rows, width), F32)],
        compiler_params=params(62), name="feed",
    )(tbl, tok, att, wall, cot, vec, bup)


def attend_back_kernel(ctx, tbl, q, kv, da, lse, delta, dq, dkv, dk_acc, dv_acc):
    width = q.shape[1]
    table = Table(tbl, 2 * ctx, lax.axis_index("ctx"))

    def pair(hp, carry):
        def put_dq(slot, value):
            dq[slot, :, pl.ds(pl.multiple_of(hp * LANES, LANES), LANES)] = value

        attend_back_pair(hp, table, q, kv, da, lse, delta, put_dq, dk_acc, dv_acc, width)
        for j in range(2 * ctx):
            at = pl.ds(pl.multiple_of(table.pos[j] * BLK, BLK), BLK)
            dkv[at, pl.ds(pl.multiple_of(hp * LANES, LANES), LANES)] = dk_acc[j].astype(BF)
            dkv[at, pl.ds(pl.multiple_of(width + hp * LANES, LANES), LANES)] = dv_acc[j].astype(BF)
        return carry

    lax.fori_loop(0, PAIRS, pair, 0)


def attend_back(tbl, q, kv, da, lse, delta, ctx):
    rows, width = q.shape
    return pl.pallas_call(
        functools.partial(attend_back_kernel, ctx),
        out_shape=(shape(2, BLK, width), shape(*kv.shape)),
        in_specs=[SM] + [VM] * 5, out_specs=(VM,) * 2,
        scratch_shapes=[pltpu.VMEM((2 * ctx, BLK, LANES), F32), pltpu.VMEM((2 * ctx, BLK, LANES), F32)],
        compiler_params=params(62), name="attend_back",
    )(tbl, q, kv, da, lse, delta)


def last_kernel(ctx, tbl, dq, dkv, h1, tok, wall, dx1, vec, gvec, gq, gtok, land, ssem, rsem):
    rows = h1.shape[0]
    y = lax.axis_index("ctx")
    table = Table(tbl, 2 * ctx, y)
    sem = pltpu.get_barrier_semaphore()
    peers = [lax.rem(y + k, ctx) for k in range(1, ctx)]
    for peer in peers:
        pl.semaphore_signal(sem, inc=1, device_id={"ctx": peer}, device_id_type=pl.DeviceIdType.MESH)
    pl.semaphore_wait(sem, ctx - 1)
    copies = []
    for k, peer in enumerate(peers):
        copy = remote(dkv.at[pl.ds(pl.multiple_of(peer * rows, BLK), rows)], land.at[y], ssem.at[k], rsem.at[y], {"ctx": peer})
        copy.start()
        copies.append(copy)

    def own_kv():
        total = dkv[pl.ds(pl.multiple_of(y * rows, BLK), rows)].astype(F32)
        for peer in peers:
            remote(land.at[peer], land.at[peer], ssem.at[0], rsem.at[peer], {"ctx": peer}).wait_recv()
            total = total + land[peer].astype(F32)
        return total.astype(BF)

    last(ctx, table, y, dq, own_kv, h1, tok, wall, dx1, vec, gvec, gq, gtok)
    for copy in copies:
        copy.wait_send()


def last_call(tbl, dq, dkv, h1, tok, wall, dx1, vec, gvec, ctx, head):
    rows, width = h1.shape
    dp, r = wall.shape[:2]
    return pl.pallas_call(
        functools.partial(last_kernel, ctx),
        out_shape=(shape(dp, r, head), shape(rows, width)),
        in_specs=[SM] + [VM] * 8, out_specs=(VM,) * 2,
        scratch_shapes=[pltpu.VMEM((ctx, rows, 2 * width), BF), DMA((ctx,)), DMA((ctx,))],
        compiler_params=params(62, collective_id=2, has_side_effects=True), name="last",
    )(tbl, dq, dkv, h1, tok, wall, dx1, vec, gvec)


class Reduce:
    def __init__(self, at, g, a_core, a_x, a_z, a_y, sems):
        self.at, self.g = at, g
        self.a_core, self.a_x, self.a_z, self.a_y = a_core, a_x, a_z, a_y
        self.s1, self.r1, self.s2, self.r2, self.s3, self.r3, self.s4, self.r4 = sems
        self.mate = {"dp": at.dp_at(at.z, at.x, 1 - at.c)}
        self.across = {"dp": at.dp_at(at.z, 1 - at.x, at.c)}

    def to_core(self, p, cols, held=None):
        return remote(self.g.at[:, :, 1 - self.at.c, :, cols if held is None else held], self.a_core.at[:, :, :, cols],
                      self.s1.at[p], self.r1.at[p], self.mate)

    def to_x(self, p, cols):
        return remote(self.a_core.at[:, 1 - self.at.x, :, cols], self.a_x.at[:, :, cols],
                      self.s2.at[p], self.r2.at[p], self.across)

    def to_z(self, p, cols, k):
        at = self.at
        return remote(self.a_core.at[at.z_at(k), at.x, :, cols], self.a_z.at[k - 1, :, cols],
                      self.s3.at[p, k - 1], self.r3.at[p, k - 1], {"dp": at.dp_at(at.z_at(k), at.x, at.c)})

    def to_y(self, p, cols, k):
        at = self.at
        return remote(self.a_core.at[at.z, at.x, :, cols], self.a_y.at[k - 1, :, cols],
                      self.s4.at[p, k - 1], self.r4.at[p, k - 1], {"ctx": at.y_at(k)})

    def level1(self, p, cols, held=None):
        self.to_core(p, cols, held).start()

    def level2(self, p, cols, held=None):
        self.to_core(p, cols, held).wait_recv()
        own = self.g[:, :, self.at.c, :, cols if held is None else held]
        self.a_core[:, :, :, cols] = self.a_core[:, :, :, cols] + own
        self.to_x(p, cols).start()

    def level3(self, p, cols):
        at = self.at
        self.to_x(p, cols).wait_recv()
        self.a_core[:, at.x, :, cols] = self.a_core[:, at.x, :, cols] + self.a_x[:, :, cols]
        for k in near_first(at.lines):
            self.to_z(p, cols, k).start()

    def level4(self, p, cols):
        at = self.at
        total = self.a_core[at.z, at.x, :, cols].astype(F32)
        for k in near_first(at.lines):
            self.to_z(p, cols, k).wait_recv()
            total = total + self.a_z[k - 1, :, cols].astype(F32)
        self.a_core[at.z, at.x, :, cols] = total.astype(BF)
        for k in range(1, at.ctx):
            self.to_y(p, cols, k).start()

    def level5(self, p, cols):
        at = self.at
        total = self.a_core[at.z, at.x, :, cols].astype(F32)
        for k in range(1, at.ctx):
            self.to_y(p, cols, k).wait_recv()
            total = total + self.a_y[k - 1, :, cols].astype(F32)
        return total

    def finish(self, p, cols, core=True, held=None):
        at = self.at
        if core:
            self.to_core(p, cols, held).wait_send()
        self.to_x(p, cols).wait_send()
        for k in range(1, at.lines):
            self.to_z(p, cols, k).wait_send()
        for k in range(1, at.ctx):
            self.to_y(p, cols, k).wait_send()


def backward_kernel(dp, ctx, tbl, tok, att, cot, q, kv, h1t, lse, vec, bup, wall,
                    out, gtok, o_small, o_qkv, o_out, o_up, o_down,
                    x1, acc, dh2, da, delta, dq, dk_acc, dv_acc, send, recv, dqkv, gup, rows,
                    wub, wdb, g, a_core, a_x, a_z, a_y, wsem, ys, yr, *sems):
    at = Spot(dp, ctx)
    width = tok.shape[1]
    r = wall.shape[1]
    nd = dp // 4
    chunk = 4 * nd * r
    off_out = 128 + 3 * width
    off_up = off_out + width
    off_down = off_up + 4 * chunk
    table = Table(tbl, 2 * ctx, at.y, True)
    red = Reduce(at, g, a_core, a_x, a_z, a_y, sems)
    lines = at.lines
    last_t = 9
    actb, dub, h2 = dqkv.at[0], dqkv.at[1], dqkv.at[2]

    def cols_of(p):
        return pl.ds(pl.multiple_of(p * width, 128), width)

    def cols_q(hp):
        return pl.ds(pl.multiple_of(last_t * width + hp * 3 * LANES, 128), 3 * LANES)

    def held_q(hp):
        return pl.ds(pl.multiple_of(last_t * width + 128 + lax.rem(hp, 3) * 3 * LANES, 128), 3 * LANES)

    cols_small = pl.ds(last_t * width + 3 * width, 128)
    held_small = pl.ds(last_t * width, 128)

    def up_copy(f, slot):
        return pltpu.make_async_copy(wall.at[:, :, pl.ds(pl.multiple_of(off_up + f * chunk, 128), chunk)],
                                     wub.at[slot], wsem.at[0, slot])

    def down_copy(f, slot, j):
        return pltpu.make_async_copy(wall.at[pl.ds(f * nd, nd), :, pl.ds(off_down + j * width, width)],
                                     wdb.at[slot, :, j], wsem.at[1 + j, slot])

    def plain_copy(i, slot):
        return pltpu.make_async_copy(wall.at[:, :, pl.ds(128 + i * width, width)], wub.at[slot], wsem.at[5, slot])

    def fetch(f, slot):
        up_copy(f, slot).start()
        for j in range(4):
            down_copy(f, slot, j).start()

    plain_copy(3, 2).start()
    fetch(0, 0)
    at.barrier()
    plain_copy(3, 2).wait()
    w_out = wub[2].reshape(width, width)
    halves = [pl.ds(i * BLK, BLK) for i in range(2)]
    for i, half in enumerate(halves):
        mid = tok[half].astype(F32) + (dot(att[table.slot_of[i]], w_out) + vec[4:5])
        x1[half] = mid
        low = (normed(mid)[0] * vec[5:6] + vec[6:7]).astype(BF)
        h2[half] = low
        acc[half] = mid + vec[7:8]
        dh2[half] = jnp.zeros((BLK, width), F32)

    def part(f, carry):
        slot = lax.rem(f, 2)

        @pl.when(f < 3)
        def _():
            fetch(f + 1, 1 - slot)

        up_copy(f, slot).wait()
        for j in range(4):
            down_copy(f, slot, j).wait()
        w_up = wub[slot].reshape(width, chunk)
        w_down = wdb[slot].reshape(chunk, width)
        hid = pl.ds(pl.multiple_of(f * chunk, 128), chunk)
        bias = bup[:, hid]
        sums = jnp.zeros((1, chunk), F32)
        for half in halves:
            u = dot(h2[half], w_up) + bias
            sq = u * u
            t = jnp.tanh(u * (0.7978845608028654 + 0.03567740813636141 * sq))
            act = (0.5 * u * (1.0 + t)).astype(BF)
            actb[half] = act
            slope = 0.5 * (1.0 + t) + 0.5 * u * (1.0 - t * t) * (0.7978845608028654 + 0.10703222440908423 * sq)
            acc[half] += dot(act, w_down)
            dul = (slope * dot_t(cot[half], w_down)).astype(BF)
            dub[half] = dul
            sums = sums + jnp.sum(dul.astype(F32), axis=0, keepdims=True)
            dh2[half] += dot_t(dul, w_up)
        gup[:, hid] = sums
        g[:, :, :, :, cols_of(f)] = dot_l(h2[...], dub[...]).astype(BF).reshape(lines, 2, 2, r, chunk)
        red.level1(f, cols_of(f))
        g_down = dot_l(actb[...], cot[...]).astype(BF).reshape(nd // 4, 2, 2, 4, r, width)
        for j in range(4):
            g[pl.ds(f * (nd // 4), nd // 4), :, :, :, pl.ds((4 + j) * width, width)] = g_down[:, :, :, j]
        for lag, level in ((1, red.level2), (2, red.level3), (3, red.level4)):
            @pl.when(f >= lag)
            def _():
                level(f - lag, cols_of(f - lag))
        return carry

    lax.fori_loop(0, 4, part, 0)
    for p in range(4, 8):
        red.level1(p, cols_of(p))
    for i, half in enumerate(halves):
        out[half] = jnp.where(table.turned, acc[halves[1 - i]], acc[half]).astype(BF)
    rows[...] = jnp.zeros_like(rows)
    lane_head = lax.broadcasted_iota(jnp.int32, (16, width), 0)
    pick = (lax.broadcasted_iota(jnp.int32, (16, width), 1) // HD == lane_head).astype(F32)
    grad = None
    w_out = wub[2].reshape(width, width)
    for i, half in enumerate(halves):
        gf = cot[half].astype(F32)
        unit, inv = normed(x1[half])
        dy = dh2[half]
        mid_grad = gf + norm_back(dy, unit, inv, vec[5:6])
        acc[half] = mid_grad
        branch = mid_grad.astype(BF)
        rows[4:5] += jnp.sum(branch.astype(F32), axis=0, keepdims=True)
        rows[5:6] += jnp.sum(dy * unit, axis=0, keepdims=True)
        rows[6:7] += jnp.sum(dy, axis=0, keepdims=True)
        rows[7:8] += jnp.sum(gf, axis=0, keepdims=True)
        own = att[table.slot_of[i]]
        piece = dot_l(own, branch)
        grad = piece if grad is None else grad + piece
        back = dot_t(branch, w_out).astype(BF)
        da[half] = back
        delta[i] = lax.dot_general(pick, back.astype(F32) * own.astype(F32), (((1,), (1,)), ((), ())),
                                   precision=lax.Precision.HIGHEST, preferred_element_type=F32)
    g[:, :, :, :, cols_of(8)] = grad.astype(BF).reshape(lines, 2, 2, r, width)
    red.level1(8, cols_of(8))
    for i in range(3):
        plain_copy(i, i).start()
    red.level2(3, cols_of(3))
    red.level3(2, cols_of(2))
    red.level4(1, cols_of(1))

    def done_t(p):
        total = red.level5(p, cols_of(p))

        @pl.when(p < 4)
        def _():
            o_up[:, pl.ds(pl.multiple_of(jnp.minimum(p, 3) * width, 128), width)] = total

        @pl.when(p >= 4)
        def _():
            o_down[pl.ds(pl.multiple_of(jnp.clip(p - 4, 0, 3) * r, 8), r), :] = total

    done_t(jnp.int32(0))
    other = lax.rem(at.y + 1, 2)
    mate_y = {"ctx": other}

    def kv_copy(hp):
        return remote(send.at[hp], recv.at[hp], ys.at[hp], yr.at[hp], mate_y)

    def q_grad(hp):
        lanes = pl.ds(pl.multiple_of(hp * LANES, LANES), LANES)
        kv_copy(hp).wait_recv()
        for i in range(2):
            dqkv[1 + i, :, lanes] = (dqkv[1 + i, :, lanes].astype(F32)
                                     + recv[hp, :, i * LANES:(i + 1) * LANES].astype(F32)).astype(BF)
        low = jnp.concatenate([dqkv[i, :, lanes] for i in range(3)], axis=1)

        @pl.when(hp >= 3)
        def _():
            red.to_core(last_t + jnp.maximum(hp - 3, 0), cols_q(0), held_q(0)).wait_send()

        g[:, :, :, :, held_q(hp)] = dot(h1t[...], low).astype(BF).reshape(lines, 2, 2, r, 3 * LANES)
        red.level1(last_t + hp, cols_q(hp), held_q(hp))

    def done_q(hp):
        total = red.level5(last_t + hp, cols_q(hp))
        for i in range(3):
            o_qkv[:, pl.ds(pl.multiple_of(i * width + hp * LANES, LANES), LANES)] = total[:, i * LANES:(i + 1) * LANES]

    def level_q(level, hp):
        if level == red.level2:
            level(last_t + hp, cols_q(hp), held_q(hp))
        else:
            level(last_t + hp, cols_q(hp))

    outermost = table.block[0] == 0

    def pair(hp, carry):
        def put_dq(slot, value):
            dq[slot] = value

        attend_back_pair(hp, table, q, kv, da, lse, delta, put_dq, dk_acc, dv_acc, width)
        lanes = pl.ds(pl.multiple_of(hp * LANES, LANES), LANES)
        for i, half in enumerate(halves):
            dqkv[0, half, lanes] = dq[i]
            outer, inner = (0, 1) if i == 0 else (3, 2)
            for n, sums in enumerate((dk_acc, dv_acc)):
                dqkv[1 + n, half, lanes] = jnp.where(outermost, sums[outer], sums[inner]).astype(BF)
                send[hp, half, n * LANES:(n + 1) * LANES] = jnp.where(outermost, sums[inner], sums[outer]).astype(BF)
        kv_copy(hp).start()

        @pl.when(hp < 5)
        def _():
            red.level2(4 + hp, cols_of(4 + hp))

        red.level3(3 + hp, cols_of(3 + hp))
        red.level4(2 + hp, cols_of(2 + hp))
        done_t(1 + hp)

        @pl.when(hp >= 2)
        def _():
            q_grad(hp - 2)

        for lag, level in ((3, red.level2), (4, red.level3), (5, red.level4)):
            @pl.when(hp >= lag)
            def _():
                level_q(level, hp - lag)
        return carry

    lax.fori_loop(0, PAIRS, pair, 0)
    for i in range(3):
        plain_copy(i, i).wait()
    red.level4(8, cols_of(8))
    done_t(jnp.int32(7))
    q_grad(jnp.int32(4))
    level_q(red.level2, 3)
    level_q(red.level3, 2)
    level_q(red.level4, 1)
    o_out[...] = red.level5(8, cols_of(8))
    done_q(0)
    q_grad(jnp.int32(5))
    level_q(red.level2, 4)
    level_q(red.level3, 3)
    level_q(red.level4, 2)
    done_q(1)
    for i in range(3):
        piece = dot_t(dqkv[i], wub[i].reshape(width, width))
        if i == 0:
            dh2[...] = piece
        else:
            dh2[...] += piece
    level_q(red.level2, 5)
    level_q(red.level3, 4)
    level_q(red.level4, 3)
    for half in halves:
        dy = dh2[half]
        unit, inv = normed(tok[half].astype(F32))
        acc[half] += norm_back(dy, unit, inv, vec[0:1])
        rows[0:1] += jnp.sum(dy * unit, axis=0, keepdims=True)
        rows[1:2] += jnp.sum(dy, axis=0, keepdims=True)
        rows[2:3] += jnp.sum(dqkv[0, half].astype(F32), axis=0, keepdims=True)
        rows[3:4] += jnp.sum(dqkv[2, half].astype(F32), axis=0, keepdims=True)
    for i, half in enumerate(halves):
        gtok[half] = jnp.where(table.turned, acc[halves[1 - i]], acc[half]).astype(BF)
    small = jnp.transpose(rows[...])
    lane = lax.broadcasted_iota(jnp.int32, small.shape, 1)
    tall = jnp.transpose(jnp.broadcast_to(gup[...], (8, 4 * chunk))).reshape(dp, 4, r, 8)
    for j in range(4):
        small = jnp.where(lane == 8 + j, tall[:, j].reshape(width, 8)[:, 0:1], small)
    g[:, :, :, :, held_small] = small.astype(BF).reshape(lines, 2, 2, r, 128)
    red.level1(last_t + 6, cols_small, held_small)
    level_q(red.level3, 5)
    red.level2(last_t + 6, cols_small, held_small)
    level_q(red.level4, 4)
    done_q(2)
    done_q(3)
    red.level3(last_t + 6, cols_small)
    level_q(red.level4, 5)
    red.level4(last_t + 6, cols_small)
    done_q(4)
    done_q(5)
    o_small[...] = red.level5(last_t + 6, cols_small)
    for p in range(last_t):
        red.finish(p, cols_of(p))
    for hp in range(PAIRS):
        red.finish(last_t + hp, cols_q(hp), hp >= 3, held_q(hp))
        kv_copy(hp).wait_send()
    red.finish(last_t + 6, cols_small, True, held_small)


def backward(tbl, tok, att, cot, q, kv, h1t, lse, vec, bup, wall, ctx):
    rows, width = tok.shape
    dp, r, full = wall.shape
    lines, nd = dp // 4, dp // 4
    chunk = 4 * nd * r
    V = pltpu.VMEM
    return pl.pallas_call(
        functools.partial(backward_kernel, dp, ctx),
        out_shape=(shape(rows, width), shape(rows, width), shape(r, 128, dtype=F32), shape(r, 3 * width, dtype=F32),
                   shape(r, width, dtype=F32), shape(r, 4 * chunk, dtype=F32), shape(4 * r, width, dtype=F32)),
        in_specs=[SM] + [VM] * 9 + [ANY], out_specs=(VM,) * 7,
        scratch_shapes=[V((rows, width), F32), V((rows, width), F32), V((rows, width), F32), V((rows, width), BF),
                        V((2, 16, BLK), F32),
                        V((2, BLK, LANES), BF), V((2 * ctx, BLK, LANES), F32), V((2 * ctx, BLK, LANES), F32),
                        V((PAIRS, rows, 2 * LANES), BF), V((PAIRS, rows, 2 * LANES), BF), V((3, rows, width), BF),
                        V((1, 4 * chunk), F32), V((128, width), F32),
                        V((3, dp, r, chunk), BF), V((2, nd, 4, r, width), BF),
                        V((lines, 2, 2, r, 9 * width + 128 + 9 * LANES), BF), V((lines, 2, r, full), BF), V((lines, r, full), BF),
                        V((lines - 1, r, full), BF), V((ctx - 1, r, full), BF),
                        DMA((6, 3)), DMA((PAIRS,)), DMA((PAIRS,)),
                        DMA((16,)), DMA((16,)), DMA((16,)), DMA((16,)), DMA((16, lines - 1)), DMA((16, lines - 1)),
                        DMA((16, ctx - 1)), DMA((16, ctx - 1))],
        compiler_params=pltpu.CompilerParams(vmem_limit_bytes=67043328, collective_id=3, has_side_effects=True),
        name="backward",
    )(tbl, tok, att, cot, q, kv, h1t, lse, vec, bup, wall)


def finish_kernel(count, *refs):
    ins, small, outs = refs[:count], refs[count], refs[count + 1:2 * count + 1]
    vectors, rest = refs[2 * count + 1:2 * count + 10], refs[2 * count + 10:]
    held, fetched, given = rest[:count], rest[count], rest[count + 1]

    def fetch(i):
        return pltpu.make_async_copy(ins[i], held[i], fetched.at[i])

    def give(i):
        return pltpu.make_async_copy(held[i], outs[i], given.at[i])

    for i in range(count):
        fetch(i).start()
    r = small.shape[0]
    total = jnp.transpose(jnp.concatenate([small[...], jnp.zeros((128 - r, 128), F32)], axis=0))
    for i in range(8):
        vectors[i][...] = total[i:i + 1, 0:r].reshape(r)
    vectors[8][...] = jnp.concatenate([total[8 + j:9 + j, 0:r] for j in range(4)], axis=1).reshape(4 * r)
    for i in range(count):
        fetch(i).wait()
        give(i).start()
    for i in range(count):
        give(i).wait()


def finish(results, small):
    count, r = len(results), small.shape[0]
    outs = tuple(jax.ShapeDtypeStruct(a.shape, a.dtype) for a in results)
    return pl.pallas_call(
        functools.partial(finish_kernel, count),
        out_shape=outs + (shape(r, dtype=F32),) * 8 + (shape(4 * r, dtype=F32),),
        in_specs=[HBM] * count + [VM], out_specs=(HBM,) * count + (VM,) * 9,
        scratch_shapes=[pltpu.VMEM(a.shape, a.dtype) for a in results] + [DMA((count,)), DMA((count,))],
        compiler_params=pltpu.CompilerParams(vmem_limit_bytes=67043328), name="finish",
    )(*results, small)


def shards(tokens, block_table, ln1_gain, ln1_bias, w_qkv, bias_query, bias_value, w_out, bias_out,
           ln2_gain, ln2_bias, w_up, bias_up, w_down, bias_down, cotangent):
    dp, ctx = lax.axis_size("dp"), lax.axis_size("ctx")
    width, hidden = tokens.shape[2], w_up.shape[1]
    r = w_qkv.shape[0]
    head = 128 + 3 * width
    third = (width + 2 * hidden) // 3
    off_up = head + width
    off_down = off_up + hidden
    vectors = [ln1_gain, ln1_bias, bias_query, bias_value, bias_out, ln2_gain, ln2_bias, bias_down]
    if ctx == 2 and dp == 16:
        wall, tok, cot, h1, q, kv, att, lse, vec, bup = front(
            block_table, tokens[0], cotangent[0], vectors, bias_up, (w_qkv, w_out, w_up, w_down), dp, ctx)
        out, gtok, g_small, g_qkv, g_out, g_up, g_down = backward(
            block_table, tok, att, cot, q, kv, h1, lse, vec, bup, wall, ctx)
        out, gtok, g_qkv, g_out, g_up, g_down, *rows = finish((out, gtok, g_qkv, g_out, g_up, g_down), g_small)
        return (out[None], gtok[None], rows[0], rows[1], g_qkv, rows[2], rows[3], g_out, rows[4], rows[5], rows[6],
                g_up, rows[8], g_down, rows[7])
    small = jnp.concatenate([jnp.stack(vectors), bias_up.reshape(4, r), jnp.zeros((116, r), BF)]).T
    cat = jnp.concatenate([small, w_qkv, w_out, w_up] + [w_down[j * r:(j + 1) * r] for j in range(4)], axis=1)
    tok_all, wall = gather(tokens[0], cat, dp, ctx, head, third)
    h1, q, kv, att, lse, vec = attend(block_table, tok_all, wall, ctx)
    bup = vec[8:12].reshape(4, dp, r).transpose(1, 0, 2).reshape(1, hidden)
    out, gt, da, dx1, delta, gvec, gup = feed_call(block_table, tokens[0], att, wall, cotangent[0], vec, bup,
                                                   ctx, off_up, off_down, 3 * third)
    dq, dkv = attend_back(block_table, q, kv, da, lse, delta, ctx)
    gvec = gvec.at[8:12].set(gup.reshape(dp, 4, r).transpose(1, 0, 2).reshape(4, width))
    gq, gtok = last_call(block_table, dq, dkv, h1, tokens[0], wall, dx1, vec, gvec, ctx, head)
    total = scatter(gq, gt, dp, ctx, head, third)
    rows = total[:, 0:128].T
    g_down = jnp.concatenate([total[:, off_down + j * width:off_down + (j + 1) * width] for j in range(4)], axis=0)
    return (out[None], gtok[None], rows[0], rows[1], total[:, 128:head], rows[2], rows[3],
            total[:, head:off_up], rows[4], rows[5], rows[6], total[:, off_up:off_down],
            rows[8:12].reshape(4 * r), g_down, rows[7])


def solution(mesh):
    row, mat = P("dp"), P("dp", None)
    act = P("dp", "ctx", None)
    in_specs = (act, P(), row, row, mat, row, row, mat, row, row, row, mat, row, mat, row, act)
    out_specs = (act, act, row, row, mat, row, row, mat, row, row, row, mat, row, mat, row)
    return jax.shard_map(shards, mesh=mesh, in_specs=in_specs, out_specs=out_specs, check_vma=False)
```
